128 devices in a mesh: expert: 16 (over y, z), width: 8 (over x, core).
Axes of the slice: x: 4, y: 4, z: 4, core: 2. Of those that a mesh axis runs over, the one named last changes fastest.
Arguments:
- tokens_in: bfloat16 [6144, 7168], P('expert', 'width'), may hold values from -6 to 6
- out_grad: bfloat16 [6144, 7168], P('expert', 'width'), may hold values from -0.08984375 to 0.08984375
- router_weight: bfloat16 [7168, 256], P('width'), may hold values from -0.0625 to 0.0625
- expert_out: bfloat16 [49152, 7168], P('expert', 'width'), may hold values from -6 to 6
- expert_ids: int32 [6144, 8], P('expert'), may hold values from 0 to 255, as said below
- slot_ids: int32 [6144, 8], P('expert'), may hold values from 0 to 191, as said below
Outputs:
- expert_grad: bfloat16 [49152, 7168], P('expert', 'width')
- router_grad: float32 [7168, 256], P('width', 'expert')
- input_grad: bfloat16 [6144, 7168], P('expert', 'width')
The draws below stay inside these ranges and needn't reach their ends.
Inputs may be any that keep to these rules, and one draw needn't show every extreme that they name: `expert_ids`: expert e lies on device e // 16 of the expert axis; a token's 8 experts lie on 8 different devices. The tokens of each device choose experts of each device of the expert axis exactly 192 times. slot_ids[t, k] is the row, within the block of 192 rows that token t's device sends to the device of expert expert_ids[t, k], of that pair. The pairs of one block fill all its rows, grouped by expert in rising order and by token in rising order within an expert. The values of expert_ids and slot_ids fit in 8 bits each, and both may be sent packed several to a 32-bit word.
All inputs are finite; a program needn't handle non-finite values.
Results may differ from the reference program's by a relative error of at most 0.015.
Values may be sent and summed in bfloat16 or wider, within the bound.
A program may use at most 128 MiB of HBM per device.

```python
import jax
import jax.numpy as jnp

D = 7168
EXP_DEV = 16
TOPK = 8
TOK_DEV = 384
TOKENS = 6144
EXPERTS = 256
CAP = 192
RECV = 49152
N_EXPERT = 16


def make_routes(key):
    base = jax.random.fold_in(key, 7)
    key_dev, key_tok, key_local = jax.random.split(base, 3)
    groups = TOKENS // TOK_DEV
    device_count = EXPERTS // EXP_DEV
    dev_rank = jax.random.randint(key_dev, (groups, device_count), 0, 1048576, dtype=jnp.int32) * device_count + jnp.arange(device_count, dtype=jnp.int32)[None, :]
    dev_perm = jnp.argsort(dev_rank, axis=1).astype(jnp.int32)
    tok_rank = jax.random.randint(key_tok, (groups, TOK_DEV), 0, 1048576, dtype=jnp.int32) * TOK_DEV + jnp.arange(TOK_DEV, dtype=jnp.int32)[None, :]
    tok_perm = jnp.argsort(tok_rank, axis=1).astype(jnp.int32)
    offsets = (tok_perm[:, :, None] + jnp.arange(TOPK, dtype=jnp.int32)[None, None, :]) % device_count
    chosen = jnp.take_along_axis(dev_perm, offsets.reshape(groups, TOK_DEV * TOPK), axis=1).reshape(TOKENS, TOPK)
    local_ids = jax.random.randint(key_local, (TOKENS, TOPK), 0, EXP_DEV, dtype=jnp.int32)
    expert_ids = chosen * EXP_DEV + local_ids
    matches = expert_ids[:, :, None] == jnp.arange(EXPERTS, dtype=jnp.int32)[None, None, :]
    routed = jnp.sum(matches.astype(jnp.int32), axis=1).reshape(groups, TOK_DEV, EXPERTS)
    before = jnp.cumsum(routed, axis=1) - routed
    counts = jnp.sum(routed, axis=1).reshape(groups, device_count, EXP_DEV)
    offset = (jnp.cumsum(counts, axis=2) - counts).reshape(groups, 1, EXPERTS)
    positions = (offset + before).reshape(TOKENS, EXPERTS)
    slot_ids = jnp.take_along_axis(positions, expert_ids, axis=1).astype(jnp.int32)
    return (expert_ids.astype(jnp.int32), slot_ids)


def draw_expert_ids(key, part):
    return make_routes(key)[0]


def draw_slot_ids(key, part):
    return make_routes(key)[1]


def block_scale(stream_key, shape, cuts, smallest, top_value):
    loudness, own = 1.0, jax.random.fold_in(stream_key, 6)
    for axis_at, shards_of in cuts:
        draws = jnp.exp(jax.random.uniform(jax.random.fold_in(own, axis_at), (shards_of,), jnp.float32, smallest / len(cuts), top_value / len(cuts)))
        loudness = loudness * jnp.repeat(draws, shape[axis_at] // shards_of).reshape([-1 if axis == axis_at else 1 for axis in range(len(shape))])
    return loudness


def centred(rng, extent, deviation, most, cuts=(), kind=jnp.bfloat16):
    values = deviation * jax.random.normal(rng, extent, jnp.float32)
    if cuts:
        values = values * block_scale(rng, extent, cuts, -0.22, 0.18)
    return jnp.clip(values, -most, most).astype(kind)


def setup_inputs(seed: int = 0) -> dict:
    key_of = jax.random.split(jax.random.key(seed), 7)
    tokens_in = centred(key_of[0], (TOKENS, D), 1.0, 6.0, ((0, 16), (1, 8)))
    out_grad = centred(key_of[1], (TOKENS, D), 0.015, 0.08984375, ((0, 16), (1, 8)))
    router_weight = centred(key_of[2], (D, EXPERTS), D ** -0.5, 0.0625, ((0, 8),))
    expert_out = centred(key_of[3], (RECV, D), 1.0, 6.0, ((0, 16), (1, 8)))
    expert_ids = draw_expert_ids(jax.random.fold_in(key_of[6], 71), 0)
    slot_ids = draw_slot_ids(jax.random.fold_in(key_of[6], 71), 0)
    return {"tokens_in": tokens_in, "out_grad": out_grad, "router_weight": router_weight, "expert_out": expert_out, "expert_ids": expert_ids, "slot_ids": slot_ids}


route_scale = 2.5


def gate_parts(logits, expert_ids):
    scores = jax.nn.sigmoid(logits)
    picked = jnp.take_along_axis(scores, expert_ids, axis=1)
    totals = jnp.sum(picked, axis=1, keepdims=True)
    return picked, totals


def logit_gradient(gate_grads, picked, totals, expert_ids, expert_count):
    weighted = jnp.sum(gate_grads * picked, axis=1, keepdims=True) / totals
    score_grads = route_scale / totals * (gate_grads - weighted)
    local_grads = score_grads * picked * (1.0 - picked)
    matches = expert_ids[:, :, None] == jnp.arange(expert_count, dtype=jnp.int32)[None, None, :]
    return jnp.sum(jnp.where(matches, local_grads[:, :, None], 0.0), axis=1).astype(jnp.bfloat16)


def reference(tokens_in, out_grad, router_weight, expert_out, expert_ids, slot_ids):
    logits = jnp.dot(tokens_in, router_weight, preferred_element_type=jnp.float32)
    picked, totals = gate_parts(logits, expert_ids)
    gate_weights = (route_scale * picked / totals).astype(jnp.bfloat16)
    source = (jnp.arange(TOKENS, dtype=jnp.int32) // TOK_DEV).astype(jnp.int32)
    row_of = ((expert_ids // EXP_DEV) * (N_EXPERT * CAP) + source[:, None] * CAP + slot_ids).astype(jnp.int32)
    grad_f32 = out_grad.astype(jnp.float32)
    expert_grad = jnp.zeros((RECV, D), jnp.bfloat16)
    columns = []
    for pick in range(TOPK):
        outputs = expert_out[row_of[:, pick]].astype(jnp.float32)
        columns.append(jnp.sum(outputs * grad_f32, axis=1))
        update = (gate_weights[:, pick].astype(jnp.float32)[:, None] * grad_f32).astype(jnp.bfloat16)
        expert_grad = expert_grad.at[row_of[:, pick]].set(update)
    gate_grads = jnp.stack(columns, axis=1)
    logit_grads = logit_gradient(gate_grads, picked, totals, expert_ids, EXPERTS)
    router_grad = jnp.dot(tokens_in.T, logit_grads, preferred_element_type=jnp.float32)
    input_grad = jnp.dot(logit_grads, router_weight.T, preferred_element_type=jnp.float32).astype(jnp.bfloat16)
    return (expert_grad, router_grad, input_grad)
```

```python
import functools

import jax
import jax.numpy as jnp
from jax import lax
from jax.experimental import pallas as pl
from jax.experimental.pallas import tpu as pltpu
from jax.sharding import PartitionSpec as P

MESH = pl.DeviceIdType.MESH
SIDE = 4
PER_DEV = 16
ROUTE_SCALE = 2.5
ROW = 256
BF16, F32, I32 = jnp.bfloat16, jnp.float32, jnp.int32
NT = (((1,), (1,)), ((), ()))


def kernel(
    tok_hbm, grad_hbm, weight_hbm, eo_hbm, ids_ref, slots_ref,
    eg_hbm, rg_ref, ig_ref,
    x0, x1, rs0, rs1, rl0, rl1, tok, weight, eo, egv, oh,
    tb_own, tb_in0, tb_in1, tbf0, tbf1, slot_own, eloc, lsend, win, gsend, gin, dsend, rin, win2,
    ggv, picked_v, lgt32, lgt, rb, rr,
    in_sem, eg_sem,
    xs, xr, tbs, tbr, ws, wr, gs, gr, ss, sr, rls, rlr, rts, rtr, w2s, w2r, rps, rpr,
):
    n = lax.axis_size("expert")
    n_width = lax.axis_size("width")
    me = lax.axis_index("expert")
    mw = lax.axis_index("width")
    top, t_rows = ids_ref.shape
    cap = rs0.shape[1]
    half, t_half = cap // 2, t_rows // 2
    xs_of, rs_of, rl_of = (x0, x1), (rs0, rs1), (rl0, rl1)
    tb_in, tbf = (tb_in0, tb_in1), (tbf0, tbf1)
    c0 = x0.shape[2]
    cols = ((0, c0), (c0, x1.shape[2]))
    core = lax.rem(mw, 2)
    gy, gz = me // SIDE, lax.rem(me, SIDE)

    flip = (core, 1 - core)
    p1 = tuple(gz + f * (gy - gz) for f in flip)
    p2 = tuple(gy + f * (gz - gy) for f in flip)

    def mod(v):
        return lax.rem(v + 2 * SIDE, SIDE)

    def place(g, a1, a2):
        return mod(a1) * (1 + (SIDE - 1) * flip[g]) + mod(a2) * (SIDE - (SIDE - 1) * flip[g])

    def ring1(g, step):
        return place(g, p1[g] + step, p2[g])

    def ring2(g, step):
        return place(g, p1[g], p2[g] + step)

    def to(src, dst, send, recv, e=None, w=None):
        where = {"expert": me if e is None else e, "width": mw if w is None else w}
        return pltpu.make_async_remote_copy(
            src_ref=src, dst_ref=dst, send_sem=send, recv_sem=recv, device_id=where, device_id_type=MESH
        )

    barrier = pltpu.get_barrier_semaphore()

    def greet_expert(o, carry):
        pl.semaphore_signal(
            barrier, inc=1, device_id={"expert": lax.rem(me + o, n), "width": mw}, device_id_type=MESH
        )
        return carry

    def greet_width(o, carry):
        pl.semaphore_signal(
            barrier, inc=1, device_id={"expert": me, "width": lax.rem(mw + o, n_width)}, device_id_type=MESH
        )
        return carry

    lax.fori_loop(1, n, greet_expert, 0)
    lax.fori_loop(1, n_width, greet_width, 0)

    loads = [
        pltpu.make_async_copy(grad_hbm.at[:, pl.ds(cols[g][0], cols[g][1])], xs_of[g].at[0], in_sem.at[g])
        for g in range(2)
    ]
    loads.append(pltpu.make_async_copy(tok_hbm, tok, in_sem.at[2]))
    loads.append(pltpu.make_async_copy(weight_hbm, weight, in_sem.at[3]))
    loads.append(pltpu.make_async_copy(eo_hbm, eo, in_sem.at[4]))
    for load in loads:
        load.start()

    row16 = lax.broadcasted_iota(I32, (n, t_rows), 0)
    slot_tbl = jnp.full((n, t_rows), -1, I32)
    eloc_tbl = jnp.full((n, t_rows), -1, I32)
    for k in range(top):
        ids = ids_ref[k : k + 1, :]
        dev = lax.shift_right_logical(ids, 4)
        hit = row16 == dev
        slot_tbl = jnp.where(hit, slots_ref[k : k + 1, :], slot_tbl)
        eloc_tbl = jnp.where(hit, ids - dev * PER_DEV, eloc_tbl)
    slot_own[...] = slot_tbl
    eloc[...] = eloc_tbl
    slot_f = slot_tbl.astype(F32)
    tbf0[0] = slot_f
    tbf1[0] = slot_f
    tb_own[...] = slot_f.astype(BF16)
    dsend[...] = jnp.zeros_like(dsend)

    pl.semaphore_wait(barrier, n - 1 + n_width - 1)

    def first_copy(g, k):
        step, h = ((1, 0), (1, 1), (-1, 1), (-1, 0))[k]
        rows = pl.ds(h * t_half, t_half)
        return to(
            xs_of[g].at[0, rows], xs_of[g].at[step % SIDE, rows], xs.at[g, k], xr.at[g, k], e=ring1(g, step)
        )

    def onward_copy(g, k):
        step, h = ((1, 0), (-1, 1))[k]
        rows = pl.ds(h * t_half, t_half)
        return to(
            xs_of[g].at[step % SIDE, rows], xs_of[g].at[2, rows], xs.at[g, 4 + k], xr.at[g, 4 + k], e=ring1(g, step)
        )

    def table_copy(g, j):
        return to(tb_own, tb_in[g].at[j], tbs.at[g, j], tbr.at[g, j], e=ring1(g, j))

    for g in range(2):
        loads[g].wait()
        first_copy(g, 0).start()
        first_copy(g, 2).start()
    for g in range(2):
        for j in (1, 3, 2):
            table_copy(g, j).start()
    for g in range(2):
        first_copy(g, 1).start()
        first_copy(g, 3).start()

    loads[2].wait()
    loads[3].wait()
    logits_t = jnp.dot(tok[...], weight[...], preferred_element_type=F32).T
    for d in range(n):
        block = logits_t[d * PER_DEV : (d + 1) * PER_DEV, :]
        hit = row16[:PER_DEV] == eloc_tbl[d : d + 1, :]
        lsend[d : d + 1, :] = jnp.sum(jnp.where(hit, block, 0.0), axis=0, keepdims=True)

    slot_iota = lax.broadcasted_iota(I32, (ROW, t_rows), 0).astype(F32)

    def own_table(d, carry):
        row = tbf0[0, pl.ds(d, 1), :]
        oh[d] = jnp.where(row == slot_iota, 1.0, 0.0).astype(BF16)
        return carry

    lax.fori_loop(0, n, own_table, 0)
    win[mw] = lsend[...]

    def logit_copy(o):
        return to(lsend, win.at[mw], ws.at[o], wr.at[o], w=lax.rem(mw + o, n_width))

    def send_logits(o, carry):
        logit_copy(o).start()
        return carry

    lax.fori_loop(1, n_width, send_logits, 0)

    cap_iota = lax.broadcasted_iota(I32, (cap, t_rows), 0).astype(F32)

    def select(g, j0, step, count):
        def one(i, carry):
            j, m = j0 + step * (i // SIDE), lax.rem(i, SIDE)
            row = tbf[g][j, pl.ds(ring2(g, m), 1), :]
            pick = jnp.where(row == cap_iota, 1.0, 0.0).astype(BF16)
            rows = jnp.dot(pick, xs_of[g][j], preferred_element_type=F32).astype(BF16)
            away = (m + SIDE - 1) // SIDE
            home = place(g, p1[g] - j, p2[g])
            rs_of[g][home * (1 - away) + away * (n + j * SIDE + m)] = rows
            return carry

        lax.fori_loop(0, count * SIDE, one, 0)

    def direct_copy(g, j, kind):
        m = (1, 3)[kind]
        return to(
            rs_of[g].at[n + j * SIDE + m], rs_of[g].at[place(g, p1[g] - j, p2[g])],
            ss.at[g, j, kind], sr.at[g, j, kind], e=ring2(g, (1, -1)[kind]),
        )

    def relay_copy(g, j, h):
        return to(
            rs_of[g].at[n + j * SIDE + 2, pl.ds(h * half, half)], rl_of[g].at[j, h],
            ss.at[g, j, 2 + h], rlr.at[g, j, h], e=ring2(g, (1, -1)[h]),
        )

    def final_copy(g, j, h):
        step = (1, -1)[h]
        return to(
            rl_of[g].at[j, h], rs_of[g].at[place(g, p1[g] - j, p2[g] - step), pl.ds(h * half, half)],
            rls.at[g, j, h], sr.at[g, j, 2 + h], e=ring2(g, step),
        )

    def send_picked(j):
        for g in range(2):
            relay_copy(g, j, 0).start()
            relay_copy(g, j, 1).start()
        for g in range(2):
            direct_copy(g, j, 0).start()
            direct_copy(g, j, 1).start()

    def pass_on(j):
        for g in range(2):
            for h in range(2):
                relay_copy(g, j, h).wait_recv()
                final_copy(g, j, h).start()

    for g in range(2):
        select(g, 0, 0, 1)
    for k in range(2):
        for g in range(2):
            first_copy(g, 2 * k).wait_recv()
            onward_copy(g, k).start()
    send_picked(0)

    def wait_logits(o, carry):
        to(lsend, win.at[lax.rem(mw + n_width - o, n_width)], ws.at[o], wr.at[o], w=mw).wait_recv()
        return carry

    lax.fori_loop(1, n_width, wait_logits, 0)
    total_logits = win[0]
    for w in range(1, win.shape[0]):
        total_logits = total_logits + win[w]
    picked = jnp.where(eloc_tbl >= 0, jax.nn.sigmoid(total_logits), 0.0)
    picked_v[...] = picked
    gates = (ROUTE_SCALE * picked / jnp.sum(picked, axis=0, keepdims=True)).astype(BF16).astype(F32)

    def gate_row(d, acc):
        only = jnp.where(row16 == d, gates, 0.0).astype(BF16)
        return acc + lax.dot_general(only, oh[d], NT, preferred_element_type=F32)

    gate_slots = lax.fori_loop(0, n, gate_row, jnp.zeros((n, ROW), F32))
    for d in range(n):
        gsend[d] = gate_slots[d : d + 1, :]
    gin[me] = gsend[me]

    def gate_copy(o):
        d = lax.rem(me + o, n)
        return to(gsend.at[d], gin.at[me], gs.at[o], gr.at[o], e=d)

    def send_gates(o, carry):
        gate_copy(o).start()
        return carry

    lax.fori_loop(1, n, send_gates, 0)

    def take_tables(js):
        for g in range(2):
            for j in js:
                table_copy(g, j).wait_recv()
                tbf[g][j] = tb_in[g][j].astype(F32)

    take_tables((1, 3))
    for g in range(2):
        first_copy(g, 1).wait_recv()
        first_copy(g, 3).wait_recv()
        select(g, 1, 2, 2)
    send_picked(1)
    send_picked(3)
    take_tables((2,))
    for g in range(2):
        onward_copy(g, 0).wait_recv()
        onward_copy(g, 1).wait_recv()
        select(g, 2, 0, 1)
    send_picked(2)

    loads[4].wait()

    def wait_gates(o, carry):
        to(gsend.at[0], gin.at[lax.rem(me + n - o, n)], gs.at[o], gr.at[o], e=me).wait_recv()
        return carry

    lax.fori_loop(1, n, wait_gates, 0)

    ones = jnp.ones((8, 128), BF16)
    eye = lax.broadcasted_iota(I32, (cap, cap), 0) == lax.broadcasted_iota(I32, (cap, cap), 1)

    def offsets_of(o1, o2):
        return place(0, p1[0] - o1, p2[0] - o2)

    def return_copy(s):
        o = lax.rem(me + n - s, n)
        return to(dsend.at[s], rin.at[me], rts.at[o], rtr.at[o], e=s)

    def out_copy(s):
        return pltpu.make_async_copy(egv.at[s], eg_hbm.at[s], eg_sem.at[s])

    def gate_grads_of(s):
        acc = None
        for g in range(2):
            for at in range(0, cols[g][1], 128):
                a = rs_of[g][s, :, at : at + 128].astype(F32)
                b = eo[s, :, cols[g][0] + at : cols[g][0] + at + 128].astype(F32)
                acc = a * b if acc is None else acc + a * b
        high = acc.astype(BF16)
        low = (acc - high.astype(F32)).astype(BF16)
        dots = lax.dot_general(ones, high, NT, preferred_element_type=F32)
        dots = dots + lax.dot_general(ones, low, NT, preferred_element_type=F32)
        dsend[s, :, :cap] = dots[0:1, :]

    def expert_grad_of(s):
        scale = jnp.where(eye, gin[s][:, :cap], 0.0).astype(BF16)
        for g in range(2):
            value = jnp.dot(scale, rs_of[g][s], preferred_element_type=F32)
            egv[s, :, cols[g][0] : cols[g][0] + cols[g][1]] = value.astype(BF16)
        out_copy(s).start()

    def arrived(o1, o2):
        for g, j, by in ((0, o1, o2), (1, o2, o1)):
            if by == 1:
                direct_copy(g, j, 0).wait_recv()
            elif by == 3:
                direct_copy(g, j, 1).wait_recv()
            elif by == 2:
                final_copy(g, j, 0).wait_recv()
                final_copy(g, j, 1).wait_recv()

    def blocks(count, offset, listed):
        for o1, o2 in listed:
            arrived(o1, o2)

        def one(i, carry):
            s = offsets_of(*offset(i))
            gate_grads_of(s)
            expert_grad_of(s)
            return_copy(s).start()
            return carry

        lax.fori_loop(0, count, one, 0)

    def one_axis(i):
        q, r = i // 2, 1 + 2 * lax.rem(i, 2)
        return q * r, (1 - q) * r

    def both_near(i):
        return 1 + 2 * (i // 2), 1 + 2 * lax.rem(i, 2)

    def one_far(i):
        q, r = i // 2, 1 + 2 * lax.rem(i, 2)
        return 2 * q + (1 - q) * r, q * r + 2 * (1 - q)

    gate_grads_of(me)
    expert_grad_of(me)
    rin[me] = dsend[me]
    blocks(4, one_axis, [(0, 1), (0, 3), (1, 0), (3, 0)])
    pass_on(0)
    pass_on(1)
    blocks(4, both_near, [(1, 1), (1, 3), (3, 1), (3, 3)])
    pass_on(3)
    pass_on(2)
    blocks(2, lambda i: (2 * i, 2 - 2 * i), [(0, 2), (2, 0)])
    blocks(4, one_far, [(1, 2), (3, 2), (2, 1), (2, 3)])
    arrived(2, 2)
    last = offsets_of(2, 2)
    gate_grads_of(last)
    expert_grad_of(last)
    return_copy(last).start()

    def wait_return(o, carry):
        to(dsend.at[0], rin.at[lax.rem(me + o, n)], rts.at[o], rtr.at[o], e=me).wait_recv()
        return carry

    lax.fori_loop(1, n, wait_return, 0)

    def width_copy(o):
        return to(rin, win2.at[mw], w2s.at[o], w2r.at[o], w=lax.rem(mw + o, n_width))

    def send_width(o, carry):
        width_copy(o).start()
        return carry

    lax.fori_loop(1, n_width, send_width, 0)
    win2[mw] = rin[...]

    def wait_width(o, carry):
        to(rin, win2.at[lax.rem(mw + n_width - o, n_width)], w2s.at[o], w2r.at[o], w=mw).wait_recv()
        return carry

    lax.fori_loop(1, n_width, wait_width, 0)
    for d in range(n):
        row = win2[0, d]
        for w in range(1, win2.shape[0]):
            row = row + win2[w, d]
        ggv[d : d + 1, :] = row

    slots = slot_own[...]
    lane = jnp.bitwise_and(slots, 127)
    pieces = []
    for at in range(0, t_rows, 128):
        index = lane[:, at : at + 128]
        low = jnp.take_along_axis(ggv[:, 0:128], index, axis=1)
        high = jnp.take_along_axis(ggv[:, 128:256], index, axis=1)
        pieces.append(jnp.where(slots[:, at : at + 128] < 128, low, high))
    chosen = slots >= 0
    gate_grads = jnp.where(chosen, jnp.concatenate(pieces, axis=1), 0.0)

    picked = picked_v[...]
    totals = jnp.sum(picked, axis=0, keepdims=True)
    weighted = jnp.sum(gate_grads * picked, axis=0, keepdims=True) / totals
    local = jnp.where(chosen, ROUTE_SCALE / totals * (gate_grads - weighted) * picked * (1.0 - picked), 0.0)
    for d in range(n):
        hit = row16[:PER_DEV] == eloc[d : d + 1, :]
        block = jnp.where(hit, local[d : d + 1, :], 0.0)
        lgt32[d * PER_DEV : (d + 1) * PER_DEV, :] = block
        lgt[d * PER_DEV : (d + 1) * PER_DEV, :] = block.astype(BF16)

    part = jnp.dot(lgt[...], tok[...], preferred_element_type=F32)
    rb[...] = part.astype(BF16).reshape(rb.shape)

    def part_copy(o):
        d = lax.rem(me + o, n)
        return to(rb.at[d], rr.at[me], rps.at[o], rpr.at[o], e=d)

    def send_part(o, carry):
        part_copy(o).start()
        return carry

    logit_grads = lgt32[...].T.astype(BF16)
    lax.fori_loop(1, n, send_part, 0)
    rr[me] = rb[me]
    ig_ref[...] = lax.dot_general(logit_grads, weight[...], NT, preferred_element_type=F32).astype(BF16)

    def wait_part(o, carry):
        to(rb.at[0], rr.at[lax.rem(me + n - o, n)], rps.at[o], rpr.at[o], e=me).wait_recv()
        return carry

    lax.fori_loop(1, n, wait_part, 0)
    total = rr[0].astype(F32)
    for d in range(1, n):
        total = total + rr[d].astype(F32)
    rg_ref[...] = total

    for g in range(2):
        for k in range(4):
            first_copy(g, k).wait_send()
        for k in range(2):
            onward_copy(g, k).wait_send()
        for j in range(1, SIDE):
            table_copy(g, j).wait_send()
        for j in range(SIDE):
            for h in range(2):
                direct_copy(g, j, h).wait_send()
                relay_copy(g, j, h).wait_send()
                final_copy(g, j, h).wait_send()

    def width_sent(o, carry):
        logit_copy(o).wait_send()
        width_copy(o).wait_send()
        return carry

    def expert_sent(o, carry):
        gate_copy(o).wait_send()
        part_copy(o).wait_send()
        return_copy(lax.rem(me + n - o, n)).wait_send()
        return carry

    def written(s, carry):
        out_copy(s).wait()
        return carry

    lax.fori_loop(1, n_width, width_sent, 0)
    lax.fori_loop(1, n, expert_sent, 0)
    lax.fori_loop(0, n, written, 0)


def body(tokens_in, out_grad, router_weight, expert_out, expert_ids, slot_ids):
    n = lax.axis_size("expert")
    n_width = lax.axis_size("width")
    t_rows, d_cols = out_grad.shape
    top = expert_ids.shape[1]
    experts = router_weight.shape[1]
    cap = t_rows * top // n
    c0 = (d_cols // 128 + 1) // 2 * 128
    c1 = d_cols - c0
    hbm, vmem = pl.BlockSpec(memory_space=pl.ANY), pl.BlockSpec(memory_space=pltpu.VMEM)
    dma = pltpu.SemaphoreType.DMA
    scratch = [
        pltpu.VMEM((SIDE, t_rows, c0), BF16),
        pltpu.VMEM((SIDE, t_rows, c1), BF16),
        pltpu.VMEM((2 * n, cap, c0), BF16),
        pltpu.VMEM((2 * n, cap, c1), BF16),
        pltpu.VMEM((SIDE, 2, cap // 2, c0), BF16),
        pltpu.VMEM((SIDE, 2, cap // 2, c1), BF16),
        pltpu.VMEM((t_rows, d_cols), BF16),
        pltpu.VMEM((d_cols, experts), BF16),
        pltpu.VMEM((n, cap, d_cols), BF16),
        pltpu.VMEM((n, cap, d_cols), BF16),
        pltpu.VMEM((n, ROW, t_rows), BF16),
        pltpu.VMEM((n, t_rows), BF16),
        pltpu.VMEM((SIDE, n, t_rows), BF16),
        pltpu.VMEM((SIDE, n, t_rows), BF16),
        pltpu.VMEM((SIDE, n, t_rows), F32),
        pltpu.VMEM((SIDE, n, t_rows), F32),
        pltpu.VMEM((n, t_rows), I32),
        pltpu.VMEM((n, t_rows), I32),
        pltpu.VMEM((n, t_rows), F32),
        pltpu.VMEM((n_width, n, t_rows), F32),
        pltpu.VMEM((n, 1, ROW), F32),
        pltpu.VMEM((n, 1, ROW), F32),
        pltpu.VMEM((n, 1, ROW), F32),
        pltpu.VMEM((n, 1, ROW), F32),
        pltpu.VMEM((n_width, n, 1, ROW), F32),
        pltpu.VMEM((n, ROW), F32),
        pltpu.VMEM((n, t_rows), F32),
        pltpu.VMEM((experts, t_rows), F32),
        pltpu.VMEM((experts, t_rows), BF16),
        pltpu.VMEM((n, experts // n, d_cols), BF16),
        pltpu.VMEM((n, experts // n, d_cols), BF16),
        dma((5,)),
        dma((n,)),
        dma((2, 6)), dma((2, 6)),
        dma((2, SIDE)), dma((2, SIDE)),
        dma((n_width,)), dma((n_width,)),
        dma((n,)), dma((n,)),
        dma((2, SIDE, 4)), dma((2, SIDE, 4)),
        dma((2, SIDE, 2)), dma((2, SIDE, 2)),
        dma((n,)), dma((n,)),
        dma((n_width,)), dma((n_width,)),
        dma((n,)), dma((n,)),
    ]
    expert_grad, router_grad, input_grad = pl.pallas_call(
        kernel,
        out_shape=(
            jax.ShapeDtypeStruct((n, cap, d_cols), BF16),
            jax.ShapeDtypeStruct((experts // n, d_cols), F32),
            jax.ShapeDtypeStruct((t_rows, d_cols), BF16),
        ),
        in_specs=[hbm, hbm, hbm, hbm, vmem, vmem],
        out_specs=(hbm, vmem, vmem),
        scratch_shapes=scratch,
        compiler_params=pltpu.CompilerParams(
            collective_id=0, has_side_effects=True, vmem_limit_bytes=60 * 1024 * 1024
        ),
    )(
        tokens_in, out_grad, router_weight, expert_out.reshape(n, cap, d_cols), expert_ids.T, slot_ids.T
    )
    return expert_grad.reshape(n * cap, d_cols), router_grad.T, input_grad


def solution(mesh):
    return jax.shard_map(
        body,
        mesh=mesh,
        in_specs=(
            P("expert", "width"),
            P("expert", "width"),
            P("width", None),
            P("expert", "width"),
            P("expert", None),
            P("expert", None),
        ),
        out_specs=(P("expert", "width"), P("width", "expert"), P("expert", "width")),
        check_vma=False,
    )
```

```python
import functools

import jax
import jax.numpy as jnp
from jax import lax
from jax.experimental import pallas as pl
from jax.experimental.pallas import tpu as pltpu
from jax.sharding import PartitionSpec as P

MESH = pl.DeviceIdType.MESH
SIDE = 4
PER_DEV = 16
ROUTE_SCALE = 2.5
ROW = 256
BF16, F32, I32 = jnp.bfloat16, jnp.float32, jnp.int32
NT = (((1,), (1,)), ((), ()))


SELF = ((0, 0),)
FAR_ONE = ((0, 2), (2, 0))
FAR_BOTH = ((2, 2),)
FAR_NEAR = ((1, 2), (3, 2), (2, 1), (2, 3))
DIAGONAL = ((1, 1), (1, 3), (3, 1), (3, 3))
BESIDE = ((0, 1), (0, 3), (1, 0), (3, 0))
OFFSETS = SELF + FAR_ONE + FAR_BOTH + FAR_NEAR + DIAGONAL + BESIDE
EARLY, MIDDLE, LATE = 8, 4, 4


def kernel(
    tok_hbm, grad_hbm, weight_hbm, eo_hbm, ids_hbm, slots_hbm,
    egv, rg_ref, ig_ref,
    x0, x1, rs0, rs1, tok, weight, eo, ids_ref, slots_ref, oh,
    tb_own, tb_in0, tb_in1, tbf0, tbf1, slot_own, eloc, lsend, win, gsend, gin, dsend, rin, win2,
    ggv, picked_v, lgt32, lgt, rb, rr,
    in_sem, xs, xr, tbs, tbr, ws, wr, gs, gr, ss, sr, rts, rtr, w2s, w2r, rps, rpr,
):
    n = lax.axis_size("expert")
    n_width = lax.axis_size("width")
    me = lax.axis_index("expert")
    mw = lax.axis_index("width")
    top, t_rows = ids_ref.shape
    cap = rs0.shape[1]
    t_half = t_rows // 2
    xs_of, rs_of = (x0, x1), (rs0, rs1)
    tb_in, tbf = (tb_in0, tb_in1), (tbf0, tbf1)
    c0 = x0.shape[2]
    cols = ((0, c0), (c0, x1.shape[2]))
    core = lax.rem(mw, 2)
    gy, gz = me // SIDE, lax.rem(me, SIDE)

    flip = (core, 1 - core)
    p1 = tuple(gz + f * (gy - gz) for f in flip)
    p2 = tuple(gy + f * (gz - gy) for f in flip)

    def mod(v):
        return lax.rem(v + 2 * SIDE, SIDE)

    def place(g, a1, a2):
        return mod(a1) * (1 + (SIDE - 1) * flip[g]) + mod(a2) * (SIDE - (SIDE - 1) * flip[g])

    def ring1(g, step):
        return place(g, p1[g] + step, p2[g])

    def ring2(g, step):
        return place(g, p1[g], p2[g] + step)

    def target(dy, dz):
        return mod(gy + dy) * SIDE + mod(gz + dz)

    def origin(dy, dz):
        return mod(gy - dy) * SIDE + mod(gz - dz)

    def to(src, dst, send, recv, e=None, w=None):
        where = {"expert": me if e is None else e, "width": mw if w is None else w}
        return pltpu.make_async_remote_copy(
            src_ref=src, dst_ref=dst, send_sem=send, recv_sem=recv, device_id=where, device_id_type=MESH
        )

    def await_recv(like, sem):
        to(like, like, sem, sem).wait_recv()

    def await_sent(like, sem):
        to(like, like, sem, sem).wait_send()

    barrier = pltpu.get_barrier_semaphore()

    def greet_expert(o, carry):
        pl.semaphore_signal(
            barrier, inc=1, device_id={"expert": lax.rem(me + o, n), "width": mw}, device_id_type=MESH
        )
        return carry

    def greet_width(o, carry):
        pl.semaphore_signal(
            barrier, inc=1, device_id={"expert": me, "width": lax.rem(mw + o, n_width)}, device_id_type=MESH
        )
        return carry

    def greet_beside(o, carry):
        for dy, dz in BESIDE:
            pl.semaphore_signal(
                barrier, inc=1, device_id={"expert": target(dy, dz), "width": lax.rem(mw + o, n_width)},
                device_id_type=MESH,
            )
        return carry

    lax.fori_loop(1, n, greet_expert, 0)
    lax.fori_loop(1, n_width, greet_width, 0)
    lax.fori_loop(1, n_width, greet_beside, 0)

    loads = [
        pltpu.make_async_copy(src, dst, in_sem.at[i])
        for i, (src, dst) in enumerate((
            (ids_hbm, ids_ref),
            (slots_hbm, slots_ref),
            (grad_hbm.at[:, pl.ds(0, c0)], x0.at[0]),
            (grad_hbm.at[:, pl.ds(c0, cols[1][1])], x1.at[0]),
            (tok_hbm, tok),
            (weight_hbm, weight),
            (eo_hbm, eo),
        ))
    ]
    for load in loads:
        load.start()
    loads[0].wait()
    loads[1].wait()

    row16 = lax.broadcasted_iota(I32, (n, t_rows), 0)
    slot_tbl = jnp.full((n, t_rows), -1, I32)
    eloc_tbl = jnp.full((n, t_rows), -1, I32)
    for k in range(top):
        ids = ids_ref[k : k + 1, :]
        dev = lax.shift_right_logical(ids, 4)
        hit = row16 == dev
        slot_tbl = jnp.where(hit, slots_ref[k : k + 1, :], slot_tbl)
        eloc_tbl = jnp.where(hit, ids - dev * PER_DEV, eloc_tbl)
    slot_own[...] = slot_tbl
    eloc[...] = eloc_tbl
    slot_f = slot_tbl.astype(F32)
    tbf0[0] = slot_f
    tbf1[0] = slot_f
    tb_own[...] = slot_f.astype(BF16)
    dsend[...] = jnp.zeros_like(dsend)

    pl.semaphore_wait(barrier, n - 1 + (1 + len(BESIDE)) * (n_width - 1))

    def first_copy(g, k):
        step, h = ((1, 0), (-1, 1), (1, 1), (-1, 0))[k]
        rows = pl.ds(h * t_half, t_half)
        return to(
            xs_of[g].at[0, rows], xs_of[g].at[step % SIDE, rows], xs.at[g], xr.at[g, min(k, 2)], e=ring1(g, step)
        )

    def onward_copy(g, k):
        step, h = ((1, 0), (-1, 1))[k]
        rows = pl.ds(h * t_half, t_half)
        return to(xs_of[g].at[step % SIDE, rows], xs_of[g].at[2, rows], xs.at[g], xr.at[g, 3], e=ring1(g, step))

    def table_copy(g, j):
        return to(tb_own, tb_in[g].at[j], tbs.at[g], tbr.at[g, j // 2 * (3 - j)], e=ring1(g, j))

    for g in range(2):
        loads[2 + g].wait()
        first_copy(g, 0).start()
        first_copy(g, 1).start()
    for g in range(2):
        for j in (1, 3, 2):
            table_copy(g, j).start()
    for g in range(2):
        first_copy(g, 2).start()
        first_copy(g, 3).start()

    loads[4].wait()
    loads[5].wait()
    logits_t = jnp.dot(tok[...], weight[...], preferred_element_type=F32).T
    for d in range(n):
        block = logits_t[d * PER_DEV : (d + 1) * PER_DEV, :]
        hit = row16[:PER_DEV] == eloc_tbl[d : d + 1, :]
        lsend[d : d + 1, :] = jnp.sum(jnp.where(hit, block, 0.0), axis=0, keepdims=True)

    slot_iota = lax.broadcasted_iota(I32, (ROW, t_rows), 0).astype(F32)

    def own_table(d, carry):
        row = tbf0[0, pl.ds(d, 1), :]
        oh[d] = jnp.where(row == slot_iota, 1.0, 0.0).astype(BF16)
        return carry

    lax.fori_loop(0, n, own_table, 0)
    win[mw] = lsend[...]

    def logit_copy(o):
        return to(lsend, win.at[mw], ws, wr, w=lax.rem(mw + o, n_width))

    def send_logits(o, carry):
        logit_copy(o).start()
        return carry

    lax.fori_loop(1, n_width, send_logits, 0)

    cap_iota = lax.broadcasted_iota(I32, (cap, t_rows), 0).astype(F32)

    def select(g, j0, step, count):
        def one(i, carry):
            j, m = j0 + step * (i // SIDE), lax.rem(i, SIDE)
            row = tbf[g][j, pl.ds(ring2(g, m), 1), :]
            pick = jnp.where(row == cap_iota, 1.0, 0.0).astype(BF16)
            rows = jnp.dot(pick, xs_of[g][j], preferred_element_type=F32).astype(BF16)
            away = (m + SIDE - 1) // SIDE
            home = place(g, p1[g] - j, p2[g])
            rs_of[g][home * (1 - away) + away * (n + j * SIDE + m)] = rows
            return carry

        lax.fori_loop(0, count * SIDE, one, 0)

    def near_copy(g, j, kind):
        step = (1, -1)[kind]
        return to(
            rs_of[g].at[n + j * SIDE + step % SIDE], rs_of[g].at[place(g, p1[g] - j, p2[g])],
            ss.at[g], sr.at[g, (0, 1, 2, 1)[j]], e=ring2(g, step),
        )

    def far_copy(g, j):
        return to(
            rs_of[g].at[n + j * SIDE + 2], rs_of[g].at[place(g, p1[g] - j, p2[g])],
            ss.at[g], sr.at[g, 3 + (0, 1, 2, 1)[j]], e=ring2(g, 2),
        )

    def send_far(j):
        for g in range(2):
            far_copy(g, j).start()

    def send_near(j):
        for g in range(2):
            near_copy(g, j, 0).start()
            near_copy(g, j, 1).start()

    def arrived(index, count):
        for g in range(2):
            await_recv(rs_of[g].at[pl.ds(0, count)], sr.at[g, index])

    for g in range(2):
        select(g, 0, 0, 1)
    for k in range(2):
        for g in range(2):
            await_recv(xs_of[g].at[0, pl.ds(0, t_half)], xr.at[g, k])
            onward_copy(g, k).start()
    send_far(0)

    await_recv(win.at[pl.ds(0, n_width - 1)], wr)
    total_logits = win[0]
    for w in range(1, win.shape[0]):
        total_logits = total_logits + win[w]
    picked = jnp.where(eloc_tbl >= 0, jax.nn.sigmoid(total_logits), 0.0)
    picked_v[...] = picked
    gates = (ROUTE_SCALE * picked / jnp.sum(picked, axis=0, keepdims=True)).astype(BF16).astype(F32)

    def gate_row(d, acc):
        only = jnp.where(row16 == d, gates, 0.0).astype(BF16)
        return acc + lax.dot_general(only, oh[d], NT, preferred_element_type=F32)

    gate_slots = lax.fori_loop(0, n, gate_row, jnp.zeros((n, ROW), F32))
    for d in range(n):
        gsend[d] = gate_slots[d : d + 1, :]
    gin[me] = gsend[me]

    def gate_copy(o):
        d = lax.rem(me + o, n)
        return to(gsend.at[d], gin.at[me], gs, gr, e=d)

    def send_gates(o, carry):
        gate_copy(o).start()
        return carry

    lax.fori_loop(1, n, send_gates, 0)

    def take_tables(js):
        for g in range(2):
            await_recv(tb_in[g].at[pl.ds(0, len(js))], tbr.at[g, len(js) % 2])
            for j in js:
                tbf[g][j] = tb_in[g][j].astype(F32)

    take_tables((1, 3))
    for g in range(2):
        await_recv(xs_of[g].at[0], xr.at[g, 2])
        select(g, 1, 2, 2)
    send_far(1)
    send_far(3)
    send_near(1)
    take_tables((2,))
    for g in range(2):
        await_recv(xs_of[g].at[0], xr.at[g, 3])
        select(g, 2, 0, 1)
    send_far(2)
    send_near(2)
    send_near(3)

    loads[6].wait()
    await_recv(gin.at[pl.ds(0, n - 1)], gr)

    ones = jnp.ones((8, 128), BF16)
    eye = lax.broadcasted_iota(I32, (cap, cap), 0) == lax.broadcasted_iota(I32, (cap, cap), 1)

    def gate_grads_of(s):
        acc = None
        for g in range(2):
            for at in range(0, cols[g][1], 128):
                a = rs_of[g][s, :, at : at + 128].astype(F32)
                b = eo[s, :, cols[g][0] + at : cols[g][0] + at + 128].astype(F32)
                acc = a * b if acc is None else acc + a * b
        high = acc.astype(BF16)
        low = (acc - high.astype(F32)).astype(BF16)
        dots = lax.dot_general(ones, high, NT, preferred_element_type=F32)
        dots = dots + lax.dot_general(ones, low, NT, preferred_element_type=F32)
        dsend[s, :, :cap] = dots[0:1, :]

    def expert_grad_of(s):
        scale = jnp.where(eye, gin[s][:, :cap], 0.0).astype(BF16)
        for g in range(2):
            value = jnp.dot(scale, rs_of[g][s], preferred_element_type=F32)
            egv[s, :, cols[g][0] : cols[g][0] + cols[g][1]] = value.astype(BF16)

    def far_one(i):
        return 2 * i, 2 - 2 * i

    def far_near(i):
        q, r = i // 2, 1 + 2 * lax.rem(i, 2)
        return 2 * q + (1 - q) * r, q * r + 2 * (1 - q)

    def diagonal(i):
        return 1 + 2 * (i // 2), 1 + 2 * lax.rem(i, 2)

    def beside(i):
        q, r = i // 2, 1 + 2 * lax.rem(i, 2)
        return q * r, (1 - q) * r

    def grads_back(count, offset, row, index):
        def one(i, carry):
            s = origin(*offset(i))
            gate_grads_of(s)
            to(dsend.at[s], rin.at[row + i], rts.at[0], rtr.at[index], e=s).start()
            return carry

        lax.fori_loop(0, count, one, 0)

    def scaled(count, offset):
        def one(i, carry):
            expert_grad_of(origin(*offset(i)))
            return carry

        lax.fori_loop(0, count, one, 0)

    def width_copy(o, start, count, index):
        rows = pl.ds(start, count)
        return to(rin.at[rows], win2.at[mw, rows], w2s.at[index], w2r.at[index], w=lax.rem(mw + o, n_width))

    def to_widths(start, count, index):
        def one(o, carry):
            width_copy(o, start, count, index).start()
            return carry

        lax.fori_loop(1, n_width, one, 0)
        rows = pl.ds(start, count)
        win2[mw, rows] = rin[rows]

    gate_grads_of(me)
    rin[0] = dsend[me]
    arrived(3, 1)
    grads_back(2, far_one, 1, 0)
    arrived(5, 1)
    grads_back(1, lambda i: (2, 2), 3, 0)
    scaled(1, lambda i: (0, 0))
    scaled(2, far_one)
    scaled(1, lambda i: (2, 2))
    arrived(2, 2)
    arrived(4, 2)
    grads_back(4, far_near, 4, 0)
    send_near(0)
    scaled(4, far_near)
    arrived(1, 4)
    grads_back(4, diagonal, EARLY, 1)
    scaled(4, diagonal)
    await_recv(dsend.at[pl.ds(0, EARLY - 1)], rtr.at[0])
    to_widths(0, EARLY, 0)
    arrived(0, 2)

    def late_grads(i, carry):
        gate_grads_of(origin(*beside(i)))
        return carry

    def late_copy(i, w):
        s = origin(*beside(i))
        return to(dsend.at[s], win2.at[mw, EARLY + MIDDLE + i], rts.at[1], w2r.at[2], e=s, w=w)

    def late_send(i, carry):
        def one(w, inner):
            late_copy(i, w).start()
            return inner

        return lax.fori_loop(0, n_width, one, carry)

    lax.fori_loop(0, LATE, late_grads, 0)
    lax.fori_loop(0, LATE, late_send, 0)
    await_recv(dsend.at[pl.ds(0, MIDDLE)], rtr.at[1])
    to_widths(EARLY, MIDDLE, 1)
    scaled(4, beside)

    await_recv(win2.at[pl.ds(0, n_width - 1), pl.ds(0, EARLY)], w2r.at[0])
    await_recv(win2.at[pl.ds(0, n_width - 1), pl.ds(0, MIDDLE)], w2r.at[1])
    await_recv(win2.at[pl.ds(0, n_width), pl.ds(0, LATE)], w2r.at[2])
    for i, (dy, dz) in enumerate(OFFSETS):
        row = win2[0, i]
        for w in range(1, win2.shape[0]):
            row = row + win2[w, i]
        ggv[pl.ds(target(dy, dz), 1), :] = row

    slots = slot_own[...]
    lane = jnp.bitwise_and(slots, 127)
    pieces = []
    for at in range(0, t_rows, 128):
        index = lane[:, at : at + 128]
        low = jnp.take_along_axis(ggv[:, 0:128], index, axis=1)
        high = jnp.take_along_axis(ggv[:, 128:256], index, axis=1)
        pieces.append(jnp.where(slots[:, at : at + 128] < 128, low, high))
    chosen = slots >= 0
    gate_grads = jnp.where(chosen, jnp.concatenate(pieces, axis=1), 0.0)

    picked = picked_v[...]
    totals = jnp.sum(picked, axis=0, keepdims=True)
    weighted = jnp.sum(gate_grads * picked, axis=0, keepdims=True) / totals
    local = jnp.where(chosen, ROUTE_SCALE / totals * (gate_grads - weighted) * picked * (1.0 - picked), 0.0)
    for d in range(n):
        hit = row16[:PER_DEV] == eloc[d : d + 1, :]
        block = jnp.where(hit, local[d : d + 1, :], 0.0)
        lgt32[d * PER_DEV : (d + 1) * PER_DEV, :] = block
        lgt[d * PER_DEV : (d + 1) * PER_DEV, :] = block.astype(BF16)

    part = jnp.dot(lgt[...], tok[...], preferred_element_type=F32)
    rb[...] = part.astype(BF16).reshape(rb.shape)

    logit_grads = lgt32[...].T.astype(BF16)
    for dy, dz in FAR_BOTH + FAR_NEAR + FAR_ONE + DIAGONAL + BESIDE:
        d = target(dy, dz)
        to(rb.at[d], rr.at[me], rps, rpr, e=d).start()
    rr[me] = rb[me]
    ig_ref[...] = lax.dot_general(logit_grads, weight[...], NT, preferred_element_type=F32).astype(BF16)
    await_recv(rb.at[pl.ds(0, n - 1)], rpr)
    total = rr[0].astype(F32)
    for d in range(1, n):
        total = total + rr[d].astype(F32)
    rg_ref[...] = total

    for g in range(2):
        await_sent(xs_of[g].at[pl.ds(0, SIDE - 1)], xs.at[g])
        await_sent(tb_in[g].at[pl.ds(0, SIDE - 1)], tbs.at[g])
        await_sent(rs_of[g].at[pl.ds(0, (SIDE - 1) * SIDE)], ss.at[g])
    await_sent(win.at[pl.ds(0, n_width - 1)], ws)
    await_sent(gin.at[pl.ds(0, n - 1)], gs)
    await_sent(dsend.at[pl.ds(0, EARLY + MIDDLE - 1)], rts.at[0])
    await_sent(win2.at[pl.ds(0, n_width), pl.ds(0, LATE)], rts.at[1])
    await_sent(win2.at[pl.ds(0, n_width - 1), pl.ds(0, EARLY)], w2s.at[0])
    await_sent(win2.at[pl.ds(0, n_width - 1), pl.ds(0, MIDDLE)], w2s.at[1])
    await_sent(rb.at[pl.ds(0, n - 1)], rps)


def write_out(eg_in, rg_in, ig_in, eg_out, rg_out, ig_out, sem):
    copies = [
        pltpu.make_async_copy(src, dst, sem.at[i])
        for i, (src, dst) in enumerate(((eg_in, eg_out), (ig_in, ig_out), (rg_in, rg_out)))
    ]
    for copy in copies:
        copy.start()
    for copy in copies:
        copy.wait()


def body(tokens_in, out_grad, router_weight, expert_out, expert_ids, slot_ids):
    n = lax.axis_size("expert")
    n_width = lax.axis_size("width")
    t_rows, d_cols = out_grad.shape
    top = expert_ids.shape[1]
    experts = router_weight.shape[1]
    cap = t_rows * top // n
    c0 = (d_cols // 128 + 1) // 2 * 128
    c1 = d_cols - c0
    hbm, vmem = pl.BlockSpec(memory_space=pltpu.HBM), pl.BlockSpec(memory_space=pltpu.VMEM)
    dma = pltpu.SemaphoreType.DMA
    scratch = [
        pltpu.VMEM((SIDE, t_rows, c0), BF16),
        pltpu.VMEM((SIDE, t_rows, c1), BF16),
        pltpu.VMEM((2 * n, cap, c0), BF16),
        pltpu.VMEM((2 * n, cap, c1), BF16),
        pltpu.VMEM((t_rows, d_cols), BF16),
        pltpu.VMEM((d_cols, experts), BF16),
        pltpu.VMEM((n, cap, d_cols), BF16),
        pltpu.VMEM((top, t_rows), I32),
        pltpu.VMEM((top, t_rows), I32),
        pltpu.VMEM((n, ROW, t_rows), BF16),
        pltpu.VMEM((n, t_rows), BF16),
        pltpu.VMEM((SIDE, n, t_rows), BF16),
        pltpu.VMEM((SIDE, n, t_rows), BF16),
        pltpu.VMEM((SIDE, n, t_rows), F32),
        pltpu.VMEM((SIDE, n, t_rows), F32),
        pltpu.VMEM((n, t_rows), I32),
        pltpu.VMEM((n, t_rows), I32),
        pltpu.VMEM((n, t_rows), F32),
        pltpu.VMEM((n_width, n, t_rows), F32),
        pltpu.VMEM((n, 1, ROW), F32),
        pltpu.VMEM((n, 1, ROW), F32),
        pltpu.VMEM((n, 1, ROW), F32),
        pltpu.VMEM((EARLY + MIDDLE, 1, ROW), F32),
        pltpu.VMEM((n_width, n, 1, ROW), F32),
        pltpu.VMEM((n, ROW), F32),
        pltpu.VMEM((n, t_rows), F32),
        pltpu.VMEM((experts, t_rows), F32),
        pltpu.VMEM((experts, t_rows), BF16),
        pltpu.VMEM((n, experts // n, d_cols), BF16),
        pltpu.VMEM((n, experts // n, d_cols), BF16),
        dma((7,)),
        dma((2,)), dma((2, 4)),
        dma((2,)), dma((2, 2)),
        dma(()), dma(()),
        dma(()), dma(()),
        dma((2,)), dma((2, 6)),
        dma((2,)), dma((2,)),
        dma((2,)), dma((3,)),
        dma(()), dma(()),
    ]
    expert_grad, router_grad, input_grad = pl.pallas_call(
        kernel,
        out_shape=(
            pltpu.VMEM((n, cap, d_cols), BF16),
            pltpu.VMEM((experts // n, d_cols), F32),
            pltpu.VMEM((t_rows, d_cols), BF16),
        ),
        in_specs=[hbm] * 6,
        out_specs=(vmem, vmem, vmem),
        scratch_shapes=scratch,
        compiler_params=pltpu.CompilerParams(
            collective_id=0, has_side_effects=True, vmem_limit_bytes=46 * 1024 * 1024
        ),
    )(*(
        pltpu.with_memory_space_constraint(a, pltpu.HBM)
        for a in (tokens_in, out_grad, router_weight, expert_out.reshape(n, cap, d_cols), expert_ids.T, slot_ids.T)
    ))
    expert_grad, router_grad, input_grad = pl.pallas_call(
        write_out,
        out_shape=(
            jax.ShapeDtypeStruct((n, cap, d_cols), BF16),
            jax.ShapeDtypeStruct((experts // n, d_cols), F32),
            jax.ShapeDtypeStruct((t_rows, d_cols), BF16),
        ),
        in_specs=[vmem, vmem, vmem],
        out_specs=(hbm, hbm, hbm),
        scratch_shapes=[dma((3,))],
        compiler_params=pltpu.CompilerParams(vmem_limit_bytes=2 * 1024 * 1024),
    )(*(pltpu.with_memory_space_constraint(a, pltpu.VMEM) for a in (expert_grad, router_grad, input_grad)))
    return expert_grad.reshape(n * cap, d_cols), router_grad.T, input_grad


def solution(mesh):
    return jax.shard_map(
        body,
        mesh=mesh,
        in_specs=(
            P("expert", "width"),
            P("expert", "width"),
            P("width", None),
            P("expert", "width"),
            P("expert", None),
            P("expert", None),
        ),
        out_specs=(P("expert", "width"), P("width", "expert"), P("expert", "width")),
        check_vma=False,
    )
```

```python
import functools

import jax
import jax.numpy as jnp
from jax import lax
from jax.experimental import pallas as pl
from jax.experimental.pallas import tpu as pltpu
from jax.sharding import PartitionSpec as P

MESH = pl.DeviceIdType.MESH
SIDE = 4
PER_DEV = 16
ROUTE_SCALE = 2.5
ROW = 256
BF16, F32, I32 = jnp.bfloat16, jnp.float32, jnp.int32
NT = (((1,), (1,)), ((), ()))


SELF = ((0, 0),)
FAR_ONE = ((0, 2), (2, 0))
FAR_BOTH = ((2, 2),)
FAR_NEAR = ((1, 2), (3, 2), (2, 1), (2, 3))
DIAGONAL = ((1, 1), (1, 3), (3, 1), (3, 3))
BESIDE = ((0, 1), (0, 3), (1, 0), (3, 0))
OFFSETS = SELF + FAR_ONE + FAR_NEAR + FAR_BOTH + DIAGONAL + BESIDE
LATE_ONES = DIAGONAL + BESIDE
EARLY, LATE = 8, 8
ROUNDS = 4


def kernel(
    tok_hbm, grad_hbm, weight_hbm, eo_hbm, ids_hbm, slots_hbm,
    egv, rg_ref, ig_ref,
    x0, x1, rs0, rs1, rl0, rl1, tok, weight, eo, ids_ref, slots_ref, oh,
    tb_own, tb_in0, tb_in1, tbf0, tbf1, slot_own, eloc, lsend, win, gsend, gin, dsend, rin, win2,
    ggv, picked_v, lgt32, lgt, rb, rr,
    known, in_sem, xs, xr, tbs, tbr, ws, wr, gs, gr, ss, sr, rls, rlr, rts, rtr, w2s, w2r, rps, rpr,
):
    n = lax.axis_size("expert")
    n_width = lax.axis_size("width")
    me = lax.axis_index("expert")
    mw = lax.axis_index("width")
    top, t_rows = ids_ref.shape
    cap = rs0.shape[1]
    t_half = t_rows // 2
    half = cap // 2
    xs_of, rs_of, rl_of = (x0, x1), (rs0, rs1), (rl0, rl1)
    tb_in, tbf = (tb_in0, tb_in1), (tbf0, tbf1)
    c0 = x0.shape[2]
    cols = ((0, c0), (c0, x1.shape[2]))
    core = lax.rem(mw, 2)
    gy, gz = me // SIDE, lax.rem(me, SIDE)

    flip = (core, 1 - core)
    p1 = tuple(gz + f * (gy - gz) for f in flip)
    p2 = tuple(gy + f * (gz - gy) for f in flip)

    def mod(v):
        return lax.rem(v + 2 * SIDE, SIDE)

    def place(g, a1, a2):
        return mod(a1) * (1 + (SIDE - 1) * flip[g]) + mod(a2) * (SIDE - (SIDE - 1) * flip[g])

    def ring1(g, step):
        return place(g, p1[g] + step, p2[g])

    def ring2(g, step):
        return place(g, p1[g], p2[g] + step)

    def target(dy, dz):
        return mod(gy + dy) * SIDE + mod(gz + dz)

    def origin(dy, dz):
        return mod(gy - dy) * SIDE + mod(gz - dz)

    def to(src, dst, send, recv, e=None, w=None):
        where = {"expert": me if e is None else e, "width": mw if w is None else w}
        return pltpu.make_async_remote_copy(
            src_ref=src, dst_ref=dst, send_sem=send, recv_sem=recv, device_id=where, device_id_type=MESH
        )

    def await_recv(like, sem):
        to(like, like, sem, sem).wait_recv()

    def await_sent(like, sem):
        to(like, like, sem, sem).wait_send()

    barrier = pltpu.get_barrier_semaphore()

    x_here = mw // 2
    xs_count = n_width // 2

    def greet(sem):
        for dy, dz in BESIDE:
            pl.semaphore_signal(sem, inc=1, device_id={"expert": target(dy, dz), "width": mw}, device_id_type=MESH)
        for step in (1, xs_count - 1):
            w = lax.rem(x_here + step, xs_count) * 2 + core
            pl.semaphore_signal(sem, inc=1, device_id={"expert": me, "width": w}, device_id_type=MESH)
        pl.semaphore_signal(
            sem, inc=1, device_id={"expert": me, "width": x_here * 2 + 1 - core}, device_id_type=MESH
        )

    def take_round(k):
        pl.semaphore_wait(known.at[k], len(BESIDE) + 3)
        if k + 1 < ROUNDS:
            greet(known.at[k + 1])

    greet(barrier)

    loads = [
        pltpu.make_async_copy(src, dst, in_sem.at[i])
        for i, (src, dst) in enumerate((
            (grad_hbm.at[:, pl.ds(0, c0)], x0.at[0]),
            (grad_hbm.at[:, pl.ds(c0, cols[1][1])], x1.at[0]),
            (ids_hbm, ids_ref),
            (slots_hbm, slots_ref),
            (tok_hbm, tok),
            (weight_hbm, weight),
            (eo_hbm, eo),
        ))
    ]
    for load in loads:
        load.start()

    pl.semaphore_wait(barrier, len(BESIDE) + 3)

    def first_copy(g, k):
        step, h = ((1, 0), (-1, 1), (1, 1), (-1, 0))[k]
        rows = pl.ds(h * t_half, t_half)
        return to(
            xs_of[g].at[0, rows], xs_of[g].at[step % SIDE, rows], xs.at[g], xr.at[g, min(k, 2)], e=ring1(g, step)
        )

    def onward_copy(g, k):
        step, h = ((1, 0), (-1, 1))[k]
        rows = pl.ds(h * t_half, t_half)
        return to(xs_of[g].at[step % SIDE, rows], xs_of[g].at[2, rows], xs.at[g], xr.at[g, 3], e=ring1(g, step))

    def table_copy(g, j):
        return to(tb_own, tb_in[g].at[j], tbs.at[g], tbr.at[g, j // 2 * (3 - j)], e=ring1(g, j))

    for g in range(2):
        loads[g].wait()
        first_copy(g, 0).start()
        first_copy(g, 1).start()
    greet(known.at[0])
    loads[2].wait()
    loads[3].wait()
    row16 = lax.broadcasted_iota(I32, (n, t_rows), 0)
    slot_tbl = jnp.full((n, t_rows), -1, I32)
    eloc_tbl = jnp.full((n, t_rows), -1, I32)
    for k in range(top):
        ids = ids_ref[k : k + 1, :]
        dev = lax.shift_right_logical(ids, 4)
        hit = row16 == dev
        slot_tbl = jnp.where(hit, slots_ref[k : k + 1, :], slot_tbl)
        eloc_tbl = jnp.where(hit, ids - dev * PER_DEV, eloc_tbl)
    slot_own[...] = slot_tbl
    eloc[...] = eloc_tbl
    slot_f = slot_tbl.astype(F32)
    tbf0[0] = slot_f
    tbf1[0] = slot_f
    tb_own[...] = slot_f.astype(BF16)
    dsend[...] = jnp.zeros_like(dsend)

    for g in range(2):
        table_copy(g, 1).start()
        table_copy(g, 3).start()
    for g in range(2):
        first_copy(g, 2).start()
        first_copy(g, 3).start()

    loads[4].wait()
    loads[5].wait()
    logits_t = jnp.dot(tok[...], weight[...], preferred_element_type=F32).T
    for d in range(n):
        block = logits_t[d * PER_DEV : (d + 1) * PER_DEV, :]
        hit = row16[:PER_DEV] == eloc_tbl[d : d + 1, :]
        lsend[d : d + 1, :] = jnp.sum(jnp.where(hit, block, 0.0), axis=0, keepdims=True)

    take_round(0)
    for g in range(2):
        table_copy(g, 2).start()

    slot_iota = lax.broadcasted_iota(I32, (ROW, t_rows), 0).astype(F32)

    def own_table(d, carry):
        row = tbf0[0, pl.ds(d, 1), :]
        oh[d] = jnp.where(row == slot_iota, 1.0, 0.0).astype(BF16)
        return carry

    lax.fori_loop(0, n, own_table, 0)
    win[mw] = lsend[...]

    take_round(1)

    def logit_copy(o):
        return to(lsend, win.at[mw], ws, wr, w=lax.rem(mw + o, n_width))

    def send_logits(o, carry):
        logit_copy(o).start()
        return carry

    lax.fori_loop(1, n_width, send_logits, 0)

    cap_iota = lax.broadcasted_iota(I32, (cap, t_rows), 0).astype(F32)

    def select(g, j0, step, count):
        def one(i, carry):
            j = j0 + step * i
            picks = []
            for m in range(SIDE):
                row = tbf[g][j, pl.ds(ring2(g, m), 1), :]
                picks.append(jnp.where(row == cap_iota, 1.0, 0.0).astype(BF16))
            rows = jnp.dot(jnp.concatenate(picks, axis=0), xs_of[g][j], preferred_element_type=F32).astype(BF16)
            rs_of[g][place(g, p1[g] - j, p2[g])] = rows[:cap]
            for m in range(1, SIDE):
                rs_of[g][n + j * SIDE + m] = rows[m * cap : (m + 1) * cap]
            return carry

        if count == 1:
            one(0, 0)
        else:
            lax.fori_loop(0, count, one, 0)

    def near_copy(g, j, kind, start, rows):
        step = (1, -1)[kind]
        rows = pl.ds(start, rows)
        return to(
            rs_of[g].at[n + j * SIDE + step % SIDE, rows], rs_of[g].at[place(g, p1[g] - j, p2[g]), rows],
            ss.at[g], sr.at[g, (0, 1, 2, 1)[j]], e=ring2(g, step),
        )

    def relay_copy(g, j, h):
        return to(
            rs_of[g].at[n + j * SIDE + 2, pl.ds(h * half, half)], rl_of[g].at[j, h],
            ss.at[g], rlr.at[g, j], e=ring2(g, (1, -1)[h]),
        )

    def final_copy(g, j, h):
        step = (1, -1)[h]
        return to(
            rl_of[g].at[j, h], rs_of[g].at[place(g, p1[g] - j, p2[g] - step), pl.ds(h * half, half)],
            rls.at[g], sr.at[g, 3 + (0, 1, 2, 1)[j]], e=ring2(g, step),
        )

    def send_far(j):
        for g in range(2):
            relay_copy(g, j, 0).start()
            relay_copy(g, j, 1).start()

    def pass_on(j):
        for g in range(2):
            await_recv(rl_of[g].at[j], rlr.at[g, j])
            final_copy(g, j, 0).start()
            final_copy(g, j, 1).start()

    def send_near(j, start=0, rows=cap):
        for g in range(2):
            near_copy(g, j, 0, start, rows).start()
            near_copy(g, j, 1, start, rows).start()

    def arrived(index, count):
        for g in range(2):
            await_recv(rs_of[g].at[pl.ds(0, count)], sr.at[g, index])

    for g in range(2):
        select(g, 0, 0, 1)
    for k in range(2):
        for g in range(2):
            await_recv(xs_of[g].at[0, pl.ds(0, t_half)], xr.at[g, k])
            onward_copy(g, k).start()
    send_far(0)
    send_near(0, 0, half)

    await_recv(win.at[pl.ds(0, n_width - 1)], wr)
    total_logits = win[0]
    for w in range(1, win.shape[0]):
        total_logits = total_logits + win[w]
    picked = jnp.where(eloc_tbl >= 0, jax.nn.sigmoid(total_logits), 0.0)
    picked_v[...] = picked
    gates = (ROUTE_SCALE * picked / jnp.sum(picked, axis=0, keepdims=True)).astype(BF16).astype(F32)

    def gate_row(d, acc):
        only = jnp.where(row16 == d, gates, 0.0).astype(BF16)
        return acc + lax.dot_general(only, oh[d], NT, preferred_element_type=F32)

    gate_slots = lax.fori_loop(0, n, gate_row, jnp.zeros((n, ROW), F32))
    for d in range(n):
        gsend[d] = gate_slots[d : d + 1, :]
    gin[me] = gsend[me]

    take_round(2)

    def gate_copy(o):
        d = lax.rem(me + o, n)
        return to(gsend.at[d], gin.at[me], gs, gr, e=d)

    def send_gates(o, carry):
        gate_copy(o).start()
        return carry

    lax.fori_loop(1, n, send_gates, 0)

    def take_tables(js):
        for g in range(2):
            await_recv(tb_in[g].at[pl.ds(0, len(js))], tbr.at[g, len(js) % 2])
            for j in js:
                tbf[g][j] = tb_in[g][j].astype(F32)

    take_tables((1, 3))
    for g in range(2):
        await_recv(xs_of[g].at[0], xr.at[g, 2])
    for g in range(2):
        select(g, 1, 2, 2)
    send_far(1)
    send_far(3)
    pass_on(0)
    take_tables((2,))
    for g in range(2):
        await_recv(xs_of[g].at[0], xr.at[g, 3])
    for g in range(2):
        select(g, 2, 0, 1)
    send_far(2)
    pass_on(1)
    pass_on(3)
    send_near(2)

    loads[6].wait()
    await_recv(gin.at[pl.ds(0, n - 1)], gr)

    ones = jnp.ones((8, 256), BF16)
    eye = lax.broadcasted_iota(I32, (cap, cap), 0) == lax.broadcasted_iota(I32, (cap, cap), 1)

    def gate_grads_of(blocks):
        found = []
        for s in blocks:
            acc = None
            for g in range(2):
                for at in range(0, cols[g][1], 128):
                    a = rs_of[g][s, :, at : at + 128].astype(F32)
                    b = eo[s, :, cols[g][0] + at : cols[g][0] + at + 128].astype(F32)
                    acc = a * b if acc is None else acc + a * b
            high = acc.astype(BF16)
            low = (acc - high.astype(F32)).astype(BF16)
            both = jnp.concatenate([high, low], axis=1)
            found.append(lax.dot_general(ones, both, NT, preferred_element_type=F32)[0:1, :])
        for s, dots in zip(blocks, found):
            dsend[s, :, :cap] = dots

    def expert_grad_of(s):
        scale = jnp.where(eye, gin[s][:, :cap], 0.0).astype(BF16)
        for g in range(2):
            value = jnp.dot(scale, rs_of[g][s], preferred_element_type=F32)
            egv[s, :, cols[g][0] : cols[g][0] + cols[g][1]] = value.astype(BF16)

    def far_one(i):
        return 2 * i, 2 - 2 * i

    def far_near(i):
        q, r = i // 2, 1 + 2 * lax.rem(i, 2)
        return 2 * q + (1 - q) * r, q * r + 2 * (1 - q)

    def diagonal(i):
        return 1 + 2 * (i // 2), 1 + 2 * lax.rem(i, 2)

    def beside(i):
        q, r = i // 2, 1 + 2 * lax.rem(i, 2)
        return q * r, (1 - q) * r

    def grads_back(offsets, row):
        blocks = [origin(dy, dz) for dy, dz in offsets]
        gate_grads_of(blocks)
        for i, s in enumerate(blocks):
            to(dsend.at[s], rin.at[row + i], rts.at[0], rtr, e=s).start()

    def late_copy(s, row, w):
        return to(dsend.at[s], win2.at[mw, row], rts.at[1], w2r.at[1], e=s, w=w)

    def grads_to_widths(offsets, row):
        blocks = [origin(dy, dz) for dy, dz in offsets]
        gate_grads_of(blocks)

        def one(w, carry):
            for i, s in enumerate(blocks):
                late_copy(s, row + i, w).start()
            return carry

        lax.fori_loop(0, n_width, one, 0)

    def scaled(count, offset):
        def one(i, carry):
            expert_grad_of(origin(*offset(i)))
            return carry

        lax.fori_loop(0, count, one, 0)

    rows = pl.ds(0, EARLY)

    def width_copy(o):
        return to(rin, win2.at[mw, rows], w2s, w2r.at[0], w=lax.rem(mw + o, n_width))

    def send_width(o, carry):
        width_copy(o).start()
        return carry

    gate_grads_of([me])
    rin[0] = dsend[me]
    arrived(3, 1)
    grads_back(FAR_ONE, 1)
    pass_on(2)
    send_near(1)
    scaled(1, lambda i: (0, 0))
    scaled(2, far_one)
    arrived(4, 2)
    arrived(2, 2)
    grads_back(FAR_NEAR, 3)
    arrived(5, 1)
    grads_back(FAR_BOTH, 7)
    send_near(3)
    send_near(0, half, half)
    take_round(3)
    scaled(4, far_near)
    scaled(1, lambda i: (2, 2))
    await_recv(dsend.at[pl.ds(0, EARLY - 1)], rtr)
    lax.fori_loop(1, n_width, send_width, 0)
    win2[mw, rows] = rin[...]
    arrived(1, 4)
    grads_to_widths(DIAGONAL, EARLY)
    arrived(0, 2)
    grads_to_widths(BESIDE, EARLY + len(DIAGONAL))
    scaled(4, diagonal)
    scaled(4, beside)

    await_recv(win2.at[pl.ds(0, n_width - 1), pl.ds(0, EARLY)], w2r.at[0])
    await_recv(win2.at[pl.ds(0, n_width), pl.ds(0, LATE)], w2r.at[1])
    for i, (dy, dz) in enumerate(OFFSETS):
        row = win2[0, i]
        for w in range(1, win2.shape[0]):
            row = row + win2[w, i]
        ggv[pl.ds(target(dy, dz), 1), :] = row

    slots = slot_own[...]
    lane = jnp.bitwise_and(slots, 127)
    pieces = []
    for at in range(0, t_rows, 128):
        index = lane[:, at : at + 128]
        low = jnp.take_along_axis(ggv[:, 0:128], index, axis=1)
        high = jnp.take_along_axis(ggv[:, 128:256], index, axis=1)
        pieces.append(jnp.where(slots[:, at : at + 128] < 128, low, high))
    chosen = slots >= 0
    gate_grads = jnp.where(chosen, jnp.concatenate(pieces, axis=1), 0.0)

    picked = picked_v[...]
    totals = jnp.sum(picked, axis=0, keepdims=True)
    weighted = jnp.sum(gate_grads * picked, axis=0, keepdims=True) / totals
    local = jnp.where(chosen, ROUTE_SCALE / totals * (gate_grads - weighted) * picked * (1.0 - picked), 0.0)
    for d in range(n):
        hit = row16[:PER_DEV] == eloc[d : d + 1, :]
        block = jnp.where(hit, local[d : d + 1, :], 0.0)
        lgt32[d * PER_DEV : (d + 1) * PER_DEV, :] = block
        lgt[d * PER_DEV : (d + 1) * PER_DEV, :] = block.astype(BF16)

    part = jnp.dot(lgt[...], tok[...], preferred_element_type=F32)
    rb[...] = part.astype(BF16).reshape(rb.shape)

    logit_grads = lgt32[...].T.astype(BF16)
    for dy, dz in FAR_BOTH + FAR_NEAR + FAR_ONE + DIAGONAL + BESIDE:
        d = target(dy, dz)
        to(rb.at[d], rr.at[me], rps, rpr, e=d).start()
    rr[me] = rb[me]
    ig_ref[...] = lax.dot_general(logit_grads, weight[...], NT, preferred_element_type=F32).astype(BF16)
    await_recv(rb.at[pl.ds(0, n - 1)], rpr)
    total = rr[0].astype(F32)
    for d in range(1, n):
        total = total + rr[d].astype(F32)
    rg_ref[...] = total

    for g in range(2):
        await_sent(xs_of[g].at[pl.ds(0, SIDE - 1)], xs.at[g])
        await_sent(tb_in[g].at[pl.ds(0, SIDE - 1)], tbs.at[g])
        await_sent(rs_of[g].at[pl.ds(0, (SIDE - 1) * SIDE)], ss.at[g])
        await_sent(rl_of[g], rls.at[g])
    await_sent(win.at[pl.ds(0, n_width - 1)], ws)
    await_sent(gin.at[pl.ds(0, n - 1)], gs)
    await_sent(dsend.at[pl.ds(0, EARLY - 1)], rts.at[0])
    await_sent(win2.at[pl.ds(0, n_width), pl.ds(0, LATE)], rts.at[1])
    await_sent(win2.at[pl.ds(0, n_width - 1), pl.ds(0, EARLY)], w2s)
    await_sent(rb.at[pl.ds(0, n - 1)], rps)


def write_out(eg_in, rg_in, ig_in, eg_out, rg_out, ig_out, sem):
    pieces = 4
    step = eg_in.shape[0] // pieces
    pairs = [(eg_in.at[pl.ds(i * step, step)], eg_out.at[pl.ds(i * step, step)]) for i in range(pieces)]
    pairs += [(ig_in, ig_out), (rg_in, rg_out)]
    copies = [pltpu.make_async_copy(src, dst, sem.at[i]) for i, (src, dst) in enumerate(pairs)]
    for copy in copies:
        copy.start()
    for copy in copies:
        copy.wait()


def body(tokens_in, out_grad, router_weight, expert_out, expert_ids, slot_ids):
    n = lax.axis_size("expert")
    n_width = lax.axis_size("width")
    t_rows, d_cols = out_grad.shape
    top = expert_ids.shape[1]
    experts = router_weight.shape[1]
    cap = t_rows * top // n
    c0 = (d_cols // 128 + 1) // 2 * 128
    c1 = d_cols - c0
    hbm, vmem = pl.BlockSpec(memory_space=pltpu.HBM), pl.BlockSpec(memory_space=pltpu.VMEM)
    dma = pltpu.SemaphoreType.DMA
    scratch = [
        pltpu.VMEM((SIDE, t_rows, c0), BF16),
        pltpu.VMEM((SIDE, t_rows, c1), BF16),
        pltpu.VMEM((2 * n, cap, c0), BF16),
        pltpu.VMEM((2 * n, cap, c1), BF16),
        pltpu.VMEM((SIDE, 2, cap // 2, c0), BF16),
        pltpu.VMEM((SIDE, 2, cap // 2, c1), BF16),
        pltpu.VMEM((t_rows, d_cols), BF16),
        pltpu.VMEM((d_cols, experts), BF16),
        pltpu.VMEM((n, cap, d_cols), BF16),
        pltpu.VMEM((top, t_rows), I32),
        pltpu.VMEM((top, t_rows), I32),
        pltpu.VMEM((n, ROW, t_rows), BF16),
        pltpu.VMEM((n, t_rows), BF16),
        pltpu.VMEM((SIDE, n, t_rows), BF16),
        pltpu.VMEM((SIDE, n, t_rows), BF16),
        pltpu.VMEM((SIDE, n, t_rows), F32),
        pltpu.VMEM((SIDE, n, t_rows), F32),
        pltpu.VMEM((n, t_rows), I32),
        pltpu.VMEM((n, t_rows), I32),
        pltpu.VMEM((n, t_rows), F32),
        pltpu.VMEM((n_width, n, t_rows), F32),
        pltpu.VMEM((n, 1, ROW), F32),
        pltpu.VMEM((n, 1, ROW), F32),
        pltpu.VMEM((n, 1, ROW), F32),
        pltpu.VMEM((EARLY, 1, ROW), F32),
        pltpu.VMEM((n_width, n, 1, ROW), F32),
        pltpu.VMEM((n, ROW), F32),
        pltpu.VMEM((n, t_rows), F32),
        pltpu.VMEM((experts, t_rows), F32),
        pltpu.VMEM((experts, t_rows), BF16),
        pltpu.VMEM((n, experts // n, d_cols), BF16),
        pltpu.VMEM((n, experts // n, d_cols), BF16),
        pltpu.SemaphoreType.REGULAR((ROUNDS,)),
        dma((7,)),
        dma((2,)), dma((2, 4)),
        dma((2,)), dma((2, 2)),
        dma(()), dma(()),
        dma(()), dma(()),
        dma((2,)), dma((2, 6)),
        dma((2,)), dma((2, SIDE)),
        dma((2,)), dma(()),
        dma(()), dma((2,)),
        dma(()), dma(()),
    ]
    expert_grad, router_grad, input_grad = pl.pallas_call(
        kernel,
        out_shape=(
            pltpu.VMEM((n, cap, d_cols), BF16),
            pltpu.VMEM((experts // n, d_cols), F32),
            pltpu.VMEM((t_rows, d_cols), BF16),
        ),
        in_specs=[hbm] * 6,
        out_specs=(vmem, vmem, vmem),
        scratch_shapes=scratch,
        compiler_params=pltpu.CompilerParams(
            collective_id=0, has_side_effects=True, vmem_limit_bytes=46 * 1024 * 1024
        ),
    )(*(
        pltpu.with_memory_space_constraint(a, pltpu.HBM)
        for a in (tokens_in, out_grad, router_weight, expert_out.reshape(n, cap, d_cols), expert_ids.T, slot_ids.T)
    ))
    expert_grad, router_grad, input_grad = pl.pallas_call(
        write_out,
        out_shape=(
            jax.ShapeDtypeStruct((n, cap, d_cols), BF16),
            jax.ShapeDtypeStruct((experts // n, d_cols), F32),
            jax.ShapeDtypeStruct((t_rows, d_cols), BF16),
        ),
        in_specs=[vmem, vmem, vmem],
        out_specs=(hbm, hbm, hbm),
        scratch_shapes=[dma((6,))],
        compiler_params=pltpu.CompilerParams(vmem_limit_bytes=2 * 1024 * 1024),
    )(*(pltpu.with_memory_space_constraint(a, pltpu.VMEM) for a in (expert_grad, router_grad, input_grad)))
    return expert_grad.reshape(n * cap, d_cols), router_grad.T, input_grad


def solution(mesh):
    return jax.shard_map(
        body,
        mesh=mesh,
        in_specs=(
            P("expert", "width"),
            P("expert", "width"),
            P("width", None),
            P("expert", "width"),
            P("expert", None),
            P("expert", None),
        ),
        out_specs=(P("expert", "width"), P("width", "expert"), P("expert", "width")),
        check_vma=False,
    )
```

```python
import functools

import jax
import jax.numpy as jnp
from jax import lax
from jax.experimental import pallas as pl
from jax.experimental.pallas import tpu as pltpu
from jax.sharding import PartitionSpec as P

MESH = pl.DeviceIdType.MESH
SIDE = 4
PER_DEV = 16
ROUTE_SCALE = 2.5
ROW = 256
BF16, F32, I32 = jnp.bfloat16, jnp.float32, jnp.int32
NT = (((1,), (1,)), ((), ()))


SELF = ((0, 0),)
FAR_ONE = ((0, 2), (2, 0))
FAR_BOTH = ((2, 2),)
FAR_NEAR = ((1, 2), (3, 2), (2, 1), (2, 3))
DIAGONAL = ((1, 1), (1, 3), (3, 1), (3, 3))
BESIDE = ((0, 1), (0, 3), (1, 0), (3, 0))
OFFSETS = SELF + FAR_ONE + FAR_NEAR + FAR_BOTH + DIAGONAL + BESIDE
LATE_ONES = DIAGONAL + BESIDE
EARLY, LATE = 8, 8
ROUNDS = 4
JOINED = (((0, 1), (2, 1)), ((0, 3), (2, 3)), ((1, 0), (1, 2)), ((3, 0), (3, 2)))
TERMS = SELF + FAR_ONE + FAR_BOTH + DIAGONAL + BESIDE


def kernel(
    tok_hbm, grad_hbm, weight_hbm, eo_hbm, ids_hbm, slots_hbm,
    egv, rg_ref, ig_ref,
    x0, x1, rs0, rs1, rl0, rl1, tok, weight, eo, ids_ref, slots_ref, oh,
    tb_own0, tb_own1, tb_in0, tb_in1, tbf0, tbf1, slot_f32, slot_own, eloc, lsend, win, gsend, gin, dsend, rin, win2,
    ggv, picked_v, lgt32, lgt, rb, rr, rm,
    known, in_sem, xs, xr, tbs, tbr, ws, wr, gs, gr, ss, sr, rls, rlr, rts, rtr, w2s, w2r, rps, rpr, rms,
):
    n = lax.axis_size("expert")
    n_width = lax.axis_size("width")
    me = lax.axis_index("expert")
    mw = lax.axis_index("width")
    top, t_rows = ids_ref.shape
    cap = rs0.shape[1]
    t_half = t_rows // 2
    half = cap // 2
    xs_of, rs_of, rl_of = (x0, x1), (rs0, rs1), (rl0, rl1)
    tb_own, tb_in, tbf = (tb_own0, tb_own1), (tb_in0, tb_in1), (tbf0, tbf1)
    c0 = x0.shape[2]
    cols = ((0, c0), (c0, x1.shape[2]))
    core = lax.rem(mw, 2)
    gy, gz = me // SIDE, lax.rem(me, SIDE)

    flip = (core, 1 - core)
    p1 = tuple(gz + f * (gy - gz) for f in flip)
    p2 = tuple(gy + f * (gz - gy) for f in flip)

    def mod(v):
        return lax.rem(v + 2 * SIDE, SIDE)

    def place(g, a1, a2):
        return mod(a1) * (1 + (SIDE - 1) * flip[g]) + mod(a2) * (SIDE - (SIDE - 1) * flip[g])

    def ring1(g, step):
        return place(g, p1[g] + step, p2[g])

    def ring2(g, step):
        return place(g, p1[g], p2[g] + step)

    def target(dy, dz):
        return mod(gy + dy) * SIDE + mod(gz + dz)

    def origin(dy, dz):
        return mod(gy - dy) * SIDE + mod(gz - dz)

    def to(src, dst, send, recv, e=None, w=None):
        where = {"expert": me if e is None else e, "width": mw if w is None else w}
        return pltpu.make_async_remote_copy(
            src_ref=src, dst_ref=dst, send_sem=send, recv_sem=recv, device_id=where, device_id_type=MESH
        )

    def await_recv(like, sem):
        to(like, like, sem, sem).wait_recv()

    def await_sent(like, sem):
        to(like, like, sem, sem).wait_send()

    barrier = pltpu.get_barrier_semaphore()

    x_here = mw // 2
    xs_count = n_width // 2

    def greet(sem):
        for dy, dz in BESIDE:
            pl.semaphore_signal(sem, inc=1, device_id={"expert": target(dy, dz), "width": mw}, device_id_type=MESH)
        for step in (1, xs_count - 1):
            w = lax.rem(x_here + step, xs_count) * 2 + core
            pl.semaphore_signal(sem, inc=1, device_id={"expert": me, "width": w}, device_id_type=MESH)
        pl.semaphore_signal(
            sem, inc=1, device_id={"expert": me, "width": x_here * 2 + 1 - core}, device_id_type=MESH
        )

    def take_round(k):
        pl.semaphore_wait(known.at[k], len(BESIDE) + 3)
        if k + 1 < ROUNDS:
            greet(known.at[k + 1])

    loads = [
        pltpu.make_async_copy(src, dst, in_sem.at[i])
        for i, (src, dst) in enumerate((
            (grad_hbm.at[:, pl.ds(0, c0)], x0.at[0]),
            (grad_hbm.at[:, pl.ds(c0, cols[1][1])], x1.at[0]),
            (ids_hbm, ids_ref),
            (slots_hbm, slots_ref),
            (tok_hbm, tok),
            (weight_hbm, weight),
            (eo_hbm, eo),
        ))
    ]
    loads[0].start()
    loads[1].start()
    greet(barrier)
    loads[2].start()
    loads[3].start()
    pl.semaphore_wait(barrier, len(BESIDE) + 3)

    def first_copy(g, k):
        step, h = ((1, 0), (-1, 1), (1, 1), (-1, 0))[k]
        rows = pl.ds(h * t_half, t_half)
        return to(
            xs_of[g].at[0, rows], xs_of[g].at[step % SIDE, rows], xs.at[g], xr.at[g, min(k, 2)], e=ring1(g, step)
        )

    def onward_copy(g, k):
        step, h = ((1, 0), (-1, 1))[k]
        rows = pl.ds(h * t_half, t_half)
        return to(xs_of[g].at[step % SIDE, rows], xs_of[g].at[2, rows], xs.at[g], xr.at[g, 3], e=ring1(g, step))

    def table_copy(g, j):
        return to(
            tb_own[g].at[mod(p1[g] + j)], tb_in[g].at[j], tbs.at[g], tbr.at[g, j // 2 * (3 - j)], e=ring1(g, j)
        )

    for g in range(2):
        loads[g].wait()
        first_copy(g, 0).start()
        first_copy(g, 1).start()
    greet(known.at[0])
    loads[4].start()
    loads[5].start()
    loads[2].wait()
    loads[3].wait()
    row16 = lax.broadcasted_iota(I32, (n, t_rows), 0)
    slot_tbl = jnp.full((n, t_rows), -1, I32)
    eloc_tbl = jnp.full((n, t_rows), -1, I32)
    for k in range(top):
        ids = ids_ref[k : k + 1, :]
        dev = lax.shift_right_logical(ids, 4)
        hit = row16 == dev
        slot_tbl = jnp.where(hit, slots_ref[k : k + 1, :], slot_tbl)
        eloc_tbl = jnp.where(hit, ids - dev * PER_DEV, eloc_tbl)
    slot_own[...] = slot_tbl
    eloc[...] = eloc_tbl
    slot_f = slot_tbl.astype(F32)
    slot_f32[...] = slot_f
    for a1 in range(SIDE):
        by_y = slot_f[a1 * SIDE : (a1 + 1) * SIDE, :]
        by_z = jnp.concatenate([slot_f[a2 * SIDE + a1 : a2 * SIDE + a1 + 1, :] for a2 in range(SIDE)], axis=0)
        for g in range(2):
            rows = by_z + flip[g].astype(F32) * (by_y - by_z)
            tb_own[g][a1] = rows.astype(BF16)
    for g in range(2):
        tbf[g][0] = tb_own[g][p1[g]].astype(F32)
    dsend[...] = jnp.zeros_like(dsend)

    for g in range(2):
        table_copy(g, 1).start()
        table_copy(g, 3).start()
    for g in range(2):
        first_copy(g, 2).start()
        first_copy(g, 3).start()
    loads[6].start()

    loads[4].wait()
    loads[5].wait()
    logits_t = jnp.dot(tok[...], weight[...], preferred_element_type=F32).T
    for d in range(n):
        block = logits_t[d * PER_DEV : (d + 1) * PER_DEV, :]
        hit = row16[:PER_DEV] == eloc_tbl[d : d + 1, :]
        lsend[d : d + 1, :] = jnp.sum(jnp.where(hit, block, 0.0), axis=0, keepdims=True)

    take_round(0)
    for g in range(2):
        table_copy(g, 2).start()

    slot_iota = lax.broadcasted_iota(I32, (ROW, t_rows), 0).astype(F32)

    def own_table(d, carry):
        row = slot_f32[pl.ds(d, 1), :]
        oh[d] = jnp.where(row == slot_iota, 1.0, 0.0).astype(BF16)
        return carry

    lax.fori_loop(0, n, own_table, 0)
    win[mw] = lsend[...]

    take_round(1)

    def logit_copy(o):
        return to(lsend, win.at[mw], ws, wr, w=lax.rem(mw + o, n_width))

    def send_logits(o, carry):
        logit_copy(o).start()
        return carry

    lax.fori_loop(1, n_width, send_logits, 0)

    cap_iota = lax.broadcasted_iota(I32, (cap, t_rows), 0).astype(F32)

    def select(g, j0, step, count):
        def one(i, carry):
            j = j0 + step * i
            picks = []
            for m in range(SIDE):
                row = tbf[g][j, pl.ds(mod(p2[g] + m), 1), :]
                picks.append(jnp.where(row == cap_iota, 1.0, 0.0).astype(BF16))
            rows = jnp.dot(jnp.concatenate(picks, axis=0), xs_of[g][j], preferred_element_type=F32).astype(BF16)
            rs_of[g][place(g, p1[g] - j, p2[g])] = rows[:cap]
            for m in range(1, SIDE):
                rs_of[g][n + j * SIDE + m] = rows[m * cap : (m + 1) * cap]
            return carry

        if count == 1:
            one(0, 0)
        else:
            lax.fori_loop(0, count, one, 0)

    def near_copy(g, j, kind, start, rows):
        step = (1, -1)[kind]
        rows = pl.ds(start, rows)
        return to(
            rs_of[g].at[n + j * SIDE + step % SIDE, rows], rs_of[g].at[place(g, p1[g] - j, p2[g]), rows],
            ss.at[g], sr.at[g, (0, 1, 2, 1)[j]], e=ring2(g, step),
        )

    def relay_copy(g, j, h):
        return to(
            rs_of[g].at[n + j * SIDE + 2, pl.ds(h * half, half)], rl_of[g].at[j, h],
            ss.at[g], rlr.at[g, j], e=ring2(g, (1, -1)[h]),
        )

    def final_copy(g, j, h):
        step = (1, -1)[h]
        return to(
            rl_of[g].at[j, h], rs_of[g].at[place(g, p1[g] - j, p2[g] - step), pl.ds(h * half, half)],
            rls.at[g], sr.at[g, 3 + (0, 1, 2, 1)[j]], e=ring2(g, step),
        )

    def send_far(j):
        for g in range(2):
            relay_copy(g, j, 0).start()
            relay_copy(g, j, 1).start()

    def pass_on(j):
        for g in range(2):
            await_recv(rl_of[g].at[j], rlr.at[g, j])
            final_copy(g, j, 0).start()
            final_copy(g, j, 1).start()

    def send_near(j, start=0, rows=cap):
        for g in range(2):
            near_copy(g, j, 0, start, rows).start()
            near_copy(g, j, 1, start, rows).start()

    def arrived(index, count):
        for g in range(2):
            await_recv(rs_of[g].at[pl.ds(0, count)], sr.at[g, index])

    for g in range(2):
        select(g, 0, 0, 1)
    for k in range(2):
        for g in range(2):
            await_recv(xs_of[g].at[0, pl.ds(0, t_half)], xr.at[g, k])
            onward_copy(g, k).start()
    send_far(0)
    send_near(0, 0, half)

    def take_tables(js):
        for g in range(2):
            await_recv(tb_in[g].at[pl.ds(0, len(js))], tbr.at[g, len(js) % 2])
            for j in js:
                tbf[g][j] = tb_in[g][j].astype(F32)

    take_tables((1, 3))
    for g in range(2):
        await_recv(xs_of[g].at[0], xr.at[g, 2])
    for g in range(2):
        select(g, 1, 2, 2)
    send_far(1)
    send_far(3)
    pass_on(0)

    await_recv(win.at[pl.ds(0, n_width - 1)], wr)
    total_logits = win[0]
    for w in range(1, win.shape[0]):
        total_logits = total_logits + win[w]
    picked = jnp.where(eloc_tbl >= 0, jax.nn.sigmoid(total_logits), 0.0)
    picked_v[...] = picked
    gates = (ROUTE_SCALE * picked / jnp.sum(picked, axis=0, keepdims=True)).astype(BF16).astype(F32)

    gates = gates.astype(BF16)
    for first in range(0, n, 4):
        found = [lax.dot_general(gates, oh[d], NT, preferred_element_type=F32) for d in range(first, first + 4)]
        for i, rows in enumerate(found):
            gsend[first + i] = rows[first + i : first + i + 1, :]
    gin[me] = gsend[me]

    take_round(2)

    def gate_copy(o):
        d = lax.rem(me + o, n)
        return to(gsend.at[d], gin.at[me], gs, gr, e=d)

    def send_gates(o, carry):
        gate_copy(o).start()
        return carry

    lax.fori_loop(1, n, send_gates, 0)

    take_tables((2,))
    for g in range(2):
        await_recv(xs_of[g].at[0], xr.at[g, 3])
    for g in range(2):
        select(g, 2, 0, 1)
    send_far(2)
    pass_on(1)
    pass_on(3)
    send_near(2)

    loads[6].wait()
    await_recv(gin.at[pl.ds(0, n - 1)], gr)

    ones = jnp.ones((8, 256), BF16)
    eye = lax.broadcasted_iota(I32, (cap, cap), 0) == lax.broadcasted_iota(I32, (cap, cap), 1)

    def gate_grads_of(blocks):
        found = []
        for s in blocks:
            acc = None
            for g in range(2):
                for at in range(0, cols[g][1], 128):
                    a = rs_of[g][s, :, at : at + 128].astype(F32)
                    b = eo[s, :, cols[g][0] + at : cols[g][0] + at + 128].astype(F32)
                    acc = a * b if acc is None else acc + a * b
            high = acc.astype(BF16)
            low = (acc - high.astype(F32)).astype(BF16)
            both = jnp.concatenate([high, low], axis=1)
            found.append(lax.dot_general(ones, both, NT, preferred_element_type=F32)[0:1, :])
        for s, dots in zip(blocks, found):
            dsend[s, :, :cap] = dots

    def expert_grad_of(s):
        scale = jnp.where(eye, gin[s][:, :cap], 0.0).astype(BF16)
        for g in range(2):
            value = jnp.dot(scale, rs_of[g][s], preferred_element_type=F32)
            egv[s, :, cols[g][0] : cols[g][0] + cols[g][1]] = value.astype(BF16)

    def far_one(i):
        return 2 * i, 2 - 2 * i

    def far_near(i):
        q, r = i // 2, 1 + 2 * lax.rem(i, 2)
        return 2 * q + (1 - q) * r, q * r + 2 * (1 - q)

    def diagonal(i):
        return 1 + 2 * (i // 2), 1 + 2 * lax.rem(i, 2)

    def beside(i):
        q, r = i // 2, 1 + 2 * lax.rem(i, 2)
        return q * r, (1 - q) * r

    def grads_back(offsets, row):
        blocks = [origin(dy, dz) for dy, dz in offsets]
        gate_grads_of(blocks)
        for i, s in enumerate(blocks):
            to(dsend.at[s], rin.at[row + i], rts.at[0], rtr, e=s).start()

    def late_copy(s, row, w):
        return to(dsend.at[s], win2.at[mw, row], rts.at[1], w2r.at[1], e=s, w=w)

    def grads_to_widths(offsets, row):
        blocks = [origin(dy, dz) for dy, dz in offsets]
        gate_grads_of(blocks)

        def one(w, carry):
            for i, s in enumerate(blocks):
                late_copy(s, row + i, w).start()
            return carry

        lax.fori_loop(0, n_width, one, 0)

    def scaled(count, offset):
        def one(i, carry):
            expert_grad_of(origin(*offset(i)))
            return carry

        lax.fori_loop(0, count, one, 0)

    rows = pl.ds(0, EARLY)

    def width_copy(o):
        return to(rin, win2.at[mw, rows], w2s, w2r.at[0], w=lax.rem(mw + o, n_width))

    def send_width(o, carry):
        width_copy(o).start()
        return carry

    gate_grads_of([me])
    rin[0] = dsend[me]
    arrived(3, 1)
    grads_back(FAR_ONE, 1)
    pass_on(2)
    send_near(1)
    scaled(1, lambda i: (0, 0))
    scaled(2, far_one)
    arrived(4, 2)
    arrived(2, 2)
    grads_back(FAR_NEAR, 3)
    arrived(5, 1)
    grads_back(FAR_BOTH, 7)
    send_near(3)
    send_near(0, half, half)
    take_round(3)
    scaled(4, far_near)
    scaled(1, lambda i: (2, 2))
    await_recv(dsend.at[pl.ds(0, EARLY - 1)], rtr)
    lax.fori_loop(1, n_width, send_width, 0)
    win2[mw, rows] = rin[...]
    arrived(1, 4)
    grads_to_widths(DIAGONAL, EARLY)
    arrived(0, 2)
    grads_to_widths(BESIDE, EARLY + len(DIAGONAL))
    scaled(4, diagonal)
    scaled(4, beside)

    await_recv(win2.at[pl.ds(0, n_width - 1), pl.ds(0, EARLY)], w2r.at[0])
    await_recv(win2.at[pl.ds(0, n_width), pl.ds(0, LATE)], w2r.at[1])
    for i, (dy, dz) in enumerate(OFFSETS):
        row = win2[0, i]
        for w in range(1, win2.shape[0]):
            row = row + win2[w, i]
        ggv[pl.ds(target(dy, dz), 1), :] = row

    slots = slot_own[...]
    lane = jnp.bitwise_and(slots, 127)
    pieces = []
    for at in range(0, t_rows, 128):
        index = lane[:, at : at + 128]
        low = jnp.take_along_axis(ggv[:, 0:128], index, axis=1)
        high = jnp.take_along_axis(ggv[:, 128:256], index, axis=1)
        pieces.append(jnp.where(slots[:, at : at + 128] < 128, low, high))
    chosen = slots >= 0
    gate_grads = jnp.where(chosen, jnp.concatenate(pieces, axis=1), 0.0)

    picked = picked_v[...]
    totals = jnp.sum(picked, axis=0, keepdims=True)
    weighted = jnp.sum(gate_grads * picked, axis=0, keepdims=True) / totals
    local = jnp.where(chosen, ROUTE_SCALE / totals * (gate_grads - weighted) * picked * (1.0 - picked), 0.0)
    for d in range(n):
        hit = row16[:PER_DEV] == eloc[d : d + 1, :]
        block = jnp.where(hit, local[d : d + 1, :], 0.0)
        lgt32[d * PER_DEV : (d + 1) * PER_DEV, :] = block
        lgt[d * PER_DEV : (d + 1) * PER_DEV, :] = block.astype(BF16)

    part = jnp.dot(lgt[...], tok[...], preferred_element_type=F32)
    rb[...] = part.astype(BF16).reshape(rb.shape)
    rr[0] = rb[me]

    def send_terms(offsets):
        for dy, dz in offsets:
            d = target(dy, dz)
            to(rb.at[d], rr.at[TERMS.index((dy, dz))], rps, rpr, e=d).start()

    for k, (step, owner) in enumerate(JOINED):
        to(rb.at[target(*owner)], rm.at[k], rps, rms, e=target(*step)).start()
    send_terms(FAR_BOTH + DIAGONAL + BESIDE)
    logit_grads = lgt32[...].T.astype(BF16)
    ig_ref[...] = lax.dot_general(logit_grads, weight[...], NT, preferred_element_type=F32).astype(BF16)
    await_recv(rm, rms)
    for k, owner in ((0, (2, 0)), (2, (0, 2))):
        d = target(*owner)
        rb[d] = (rb[d].astype(F32) + rm[k].astype(F32) + rm[k + 1].astype(F32)).astype(BF16)
    send_terms(FAR_ONE)
    await_recv(rr.at[pl.ds(0, len(TERMS) - 1)], rpr)
    total = rr[0].astype(F32)
    for d in range(1, len(TERMS)):
        total = total + rr[d].astype(F32)
    rg_ref[...] = total

    for g in range(2):
        await_sent(xs_of[g].at[pl.ds(0, SIDE - 1)], xs.at[g])
        await_sent(tb_in[g].at[pl.ds(0, SIDE - 1)], tbs.at[g])
        await_sent(rs_of[g].at[pl.ds(0, (SIDE - 1) * SIDE)], ss.at[g])
        await_sent(rl_of[g], rls.at[g])
    await_sent(win.at[pl.ds(0, n_width - 1)], ws)
    await_sent(gin.at[pl.ds(0, n - 1)], gs)
    await_sent(dsend.at[pl.ds(0, EARLY - 1)], rts.at[0])
    await_sent(win2.at[pl.ds(0, n_width), pl.ds(0, LATE)], rts.at[1])
    await_sent(win2.at[pl.ds(0, n_width - 1), pl.ds(0, EARLY)], w2s)
    await_sent(rb.at[pl.ds(0, n - 1)], rps)


def write_out(eg_in, rg_in, ig_in, eg_out, rg_out, ig_out, sem):
    pieces = 1
    step = eg_in.shape[0] // pieces
    pairs = [(eg_in.at[pl.ds(i * step, step)], eg_out.at[pl.ds(i * step, step)]) for i in range(pieces)]
    pairs += [(ig_in, ig_out), (rg_in, rg_out)]
    copies = [pltpu.make_async_copy(src, dst, sem.at[i]) for i, (src, dst) in enumerate(pairs)]
    for copy in copies:
        copy.start()
    for copy in copies:
        copy.wait()


def body(tokens_in, out_grad, router_weight, expert_out, expert_ids, slot_ids):
    n = lax.axis_size("expert")
    n_width = lax.axis_size("width")
    t_rows, d_cols = out_grad.shape
    top = expert_ids.shape[1]
    experts = router_weight.shape[1]
    cap = t_rows * top // n
    c0 = (d_cols // 128 + 1) // 2 * 128
    c1 = d_cols - c0
    hbm, vmem = pl.BlockSpec(memory_space=pltpu.HBM), pl.BlockSpec(memory_space=pltpu.VMEM)
    dma = pltpu.SemaphoreType.DMA
    scratch = [
        pltpu.VMEM((SIDE, t_rows, c0), BF16),
        pltpu.VMEM((SIDE, t_rows, c1), BF16),
        pltpu.VMEM((2 * n, cap, c0), BF16),
        pltpu.VMEM((2 * n, cap, c1), BF16),
        pltpu.VMEM((SIDE, 2, cap // 2, c0), BF16),
        pltpu.VMEM((SIDE, 2, cap // 2, c1), BF16),
        pltpu.VMEM((t_rows, d_cols), BF16),
        pltpu.VMEM((d_cols, experts), BF16),
        pltpu.VMEM((n, cap, d_cols), BF16),
        pltpu.VMEM((top, t_rows), I32),
        pltpu.VMEM((top, t_rows), I32),
        pltpu.VMEM((n, ROW, t_rows), BF16),
        pltpu.VMEM((SIDE, SIDE, t_rows), BF16),
        pltpu.VMEM((SIDE, SIDE, t_rows), BF16),
        pltpu.VMEM((SIDE, SIDE, t_rows), BF16),
        pltpu.VMEM((SIDE, SIDE, t_rows), BF16),
        pltpu.VMEM((SIDE, SIDE, t_rows), F32),
        pltpu.VMEM((SIDE, SIDE, t_rows), F32),
        pltpu.VMEM((n, t_rows), F32),
        pltpu.VMEM((n, t_rows), I32),
        pltpu.VMEM((n, t_rows), I32),
        pltpu.VMEM((n, t_rows), F32),
        pltpu.VMEM((n_width, n, t_rows), F32),
        pltpu.VMEM((n, 1, ROW), F32),
        pltpu.VMEM((n, 1, ROW), F32),
        pltpu.VMEM((n, 1, ROW), F32),
        pltpu.VMEM((EARLY, 1, ROW), F32),
        pltpu.VMEM((n_width, n, 1, ROW), F32),
        pltpu.VMEM((n, ROW), F32),
        pltpu.VMEM((n, t_rows), F32),
        pltpu.VMEM((experts, t_rows), F32),
        pltpu.VMEM((experts, t_rows), BF16),
        pltpu.VMEM((n, experts // n, d_cols), BF16),
        pltpu.VMEM((len(TERMS), experts // n, d_cols), BF16),
        pltpu.VMEM((len(JOINED), experts // n, d_cols), BF16),
        pltpu.SemaphoreType.REGULAR((ROUNDS,)),
        dma((7,)),
        dma((2,)), dma((2, 4)),
        dma((2,)), dma((2, 2)),
        dma(()), dma(()),
        dma(()), dma(()),
        dma((2,)), dma((2, 6)),
        dma((2,)), dma((2, SIDE)),
        dma((2,)), dma(()),
        dma(()), dma((2,)),
        dma(()), dma(()), dma(()),
    ]
    expert_grad, router_grad, input_grad = pl.pallas_call(
        kernel,
        out_shape=(
            pltpu.VMEM((n, cap, d_cols), BF16),
            pltpu.VMEM((experts // n, d_cols), F32),
            pltpu.VMEM((t_rows, d_cols), BF16),
        ),
        in_specs=[hbm] * 6,
        out_specs=(vmem, vmem, vmem),
        scratch_shapes=scratch,
        compiler_params=pltpu.CompilerParams(
            collective_id=0, has_side_effects=True, vmem_limit_bytes=46 * 1024 * 1024
        ),
    )(*(
        pltpu.with_memory_space_constraint(a, pltpu.HBM)
        for a in (tokens_in, out_grad, router_weight, expert_out.reshape(n, cap, d_cols), expert_ids.T, slot_ids.T)
    ))
    expert_grad, router_grad, input_grad = pl.pallas_call(
        write_out,
        out_shape=(
            jax.ShapeDtypeStruct((n, cap, d_cols), BF16),
            jax.ShapeDtypeStruct((experts // n, d_cols), F32),
            jax.ShapeDtypeStruct((t_rows, d_cols), BF16),
        ),
        in_specs=[vmem, vmem, vmem],
        out_specs=(hbm, hbm, hbm),
        scratch_shapes=[dma((3,))],
        compiler_params=pltpu.CompilerParams(vmem_limit_bytes=2 * 1024 * 1024),
    )(*(pltpu.with_memory_space_constraint(a, pltpu.VMEM) for a in (expert_grad, router_grad, input_grad)))
    return expert_grad.reshape(n * cap, d_cols), router_grad.T, input_grad


def solution(mesh):
    return jax.shard_map(
        body,
        mesh=mesh,
        in_specs=(
            P("expert", "width"),
            P("expert", "width"),
            P("width", None),
            P("expert", "width"),
            P("expert", None),
            P("expert", None),
        ),
        out_specs=(P("expert", "width"), P("width", "expert"), P("expert", "width")),
        check_vma=False,
    )
```

```python
import functools

import jax
import jax.numpy as jnp
from jax import lax
from jax.experimental import pallas as pl
from jax.experimental.pallas import tpu as pltpu
from jax.sharding import PartitionSpec as P

MESH = pl.DeviceIdType.MESH
SIDE = 4
PER_DEV = 16
ROUTE_SCALE = 2.5
ROW = 256
BF16, F32, I32 = jnp.bfloat16, jnp.float32, jnp.int32
NT = (((1,), (1,)), ((), ()))


SELF = ((0, 0),)
FAR_ONE = ((0, 2), (2, 0))
FAR_BOTH = ((2, 2),)
FAR_NEAR = ((1, 2), (3, 2), (2, 1), (2, 3))
DIAGONAL = ((1, 1), (1, 3), (3, 1), (3, 3))
BESIDE = ((0, 1), (0, 3), (1, 0), (3, 0))
OFFSETS = SELF + FAR_ONE + FAR_NEAR + FAR_BOTH + DIAGONAL + BESIDE
LATE_ONES = DIAGONAL + BESIDE
EARLY, LATE = 8, 8
ROUNDS = 4
JOINED = (((0, 1), (2, 1)), ((0, 3), (2, 3)), ((1, 0), (1, 2)), ((3, 0), (3, 2)))
TERMS = SELF + FAR_ONE + FAR_BOTH + DIAGONAL + BESIDE


def kernel(
    tok_hbm, grad_hbm, weight_hbm, eo_hbm, ids_hbm, slots_hbm,
    egv, rg_ref, ig_ref,
    x0, x1, rs0, rs1, rl0, rl1, tok, weight, eo, ids_ref, slots_ref, oh,
    tb_own0, tb_own1, tb_in, tbf0, tbf1, slot_f32, slot_own, eloc, lsend, win, gsend, gin, dsend, rin, win2,
    ggv, picked_v, lgt32, lgt, rb, rr, rm,
    known, in_sem, xs, xr, tbs, tbr, ws, wr, gs, gr, ss, sr, rlr, rts, rtr, w2s, w2r, rps, rpr, rms,
):
    n = lax.axis_size("expert")
    n_width = lax.axis_size("width")
    me = lax.axis_index("expert")
    mw = lax.axis_index("width")
    top, t_rows = ids_ref.shape
    cap = rs0.shape[1]
    t_half = t_rows // 2
    half = cap // 2
    cut = half
    xs_of, rs_of, rl_of = (x0, x1), (rs0, rs1), (rl0, rl1)
    tb_own, tbf = (tb_own0, tb_own1), (tbf0, tbf1)
    c0 = x0.shape[2]
    cols = ((0, c0), (c0, x1.shape[2]))
    core = lax.rem(mw, 2)
    gy, gz = me // SIDE, lax.rem(me, SIDE)

    flip = (core, 1 - core)
    p1 = tuple(gz + f * (gy - gz) for f in flip)
    p2 = tuple(gy + f * (gz - gy) for f in flip)

    def mod(v):
        return lax.rem(v + 2 * SIDE, SIDE)

    def place(g, a1, a2):
        return mod(a1) * (1 + (SIDE - 1) * flip[g]) + mod(a2) * (SIDE - (SIDE - 1) * flip[g])

    def ring1(g, step):
        return place(g, p1[g] + step, p2[g])

    def ring2(g, step):
        return place(g, p1[g], p2[g] + step)

    def target(dy, dz):
        return mod(gy + dy) * SIDE + mod(gz + dz)

    def origin(dy, dz):
        return mod(gy - dy) * SIDE + mod(gz - dz)

    def to(src, dst, send, recv, e=None, w=None):
        where = {"expert": me if e is None else e, "width": mw if w is None else w}
        return pltpu.make_async_remote_copy(
            src_ref=src, dst_ref=dst, send_sem=send, recv_sem=recv, device_id=where, device_id_type=MESH
        )

    def await_recv(like, sem):
        to(like, like, sem, sem).wait_recv()

    def await_sent(like, sem):
        to(like, like, sem, sem).wait_send()

    barrier = pltpu.get_barrier_semaphore()

    x_here = mw // 2
    xs_count = n_width // 2

    def greet(sem):
        for dy, dz in BESIDE:
            pl.semaphore_signal(sem, inc=1, device_id={"expert": target(dy, dz), "width": mw}, device_id_type=MESH)
        for step in (1, xs_count - 1):
            w = lax.rem(x_here + step, xs_count) * 2 + core
            pl.semaphore_signal(sem, inc=1, device_id={"expert": me, "width": w}, device_id_type=MESH)
        pl.semaphore_signal(
            sem, inc=1, device_id={"expert": me, "width": x_here * 2 + 1 - core}, device_id_type=MESH
        )

    def take_round(k):
        pl.semaphore_wait(known.at[k], len(BESIDE) + 3)
        if k + 1 < ROUNDS:
            greet(known.at[k + 1])

    loads = [
        pltpu.make_async_copy(src, dst, in_sem.at[i])
        for i, (src, dst) in enumerate((
            (grad_hbm.at[:, pl.ds(0, c0)], x0.at[0]),
            (grad_hbm.at[:, pl.ds(c0, cols[1][1])], x1.at[0]),
            (ids_hbm, ids_ref),
            (slots_hbm, slots_ref),
            (tok_hbm, tok),
            (weight_hbm, weight),
            (eo_hbm, eo),
        ))
    ]
    loads[0].start()
    loads[1].start()
    greet(barrier)
    loads[2].start()
    loads[3].start()
    pl.semaphore_wait(barrier, len(BESIDE) + 3)

    def first_copy(g, k):
        step, h = ((1, 0), (-1, 1), (1, 1), (-1, 0))[k]
        rows = pl.ds(h * t_half, t_half)
        return to(
            xs_of[g].at[0, rows], xs_of[g].at[step % SIDE, rows], xs, xr.at[2 * g + k if k < 2 else 4], e=ring1(g, step)
        )

    def onward_copy(g, k):
        step, h = ((1, 0), (-1, 1))[k]
        rows = pl.ds(h * t_half, t_half)
        return to(xs_of[g].at[step % SIDE, rows], xs_of[g].at[2, rows], xs, xr.at[5], e=ring1(g, step))

    def table_copy(g, j):
        return to(
            tb_own[g].at[mod(p1[g] + j)], tb_in.at[g, j], tbs, tbr.at[j // 2 * (3 - j)], e=ring1(g, j)
        )

    for g in range(2):
        loads[g].wait()
        first_copy(g, 0).start()
        first_copy(g, 1).start()
    greet(known.at[0])
    loads[4].start()
    loads[5].start()
    loads[2].wait()
    loads[3].wait()
    row16 = lax.broadcasted_iota(I32, (n, t_rows), 0)
    slot_tbl = jnp.full((n, t_rows), -1, I32)
    eloc_tbl = jnp.full((n, t_rows), -1, I32)
    for k in range(top):
        ids = ids_ref[k : k + 1, :]
        dev = lax.shift_right_logical(ids, 4)
        hit = row16 == dev
        slot_tbl = jnp.where(hit, slots_ref[k : k + 1, :], slot_tbl)
        eloc_tbl = jnp.where(hit, ids - dev * PER_DEV, eloc_tbl)
    slot_own[...] = slot_tbl
    eloc[...] = eloc_tbl
    slot_f = slot_tbl.astype(F32)
    slot_f32[...] = slot_f
    for a1 in range(SIDE):
        by_y = slot_f[a1 * SIDE : (a1 + 1) * SIDE, :]
        by_z = jnp.concatenate([slot_f[a2 * SIDE + a1 : a2 * SIDE + a1 + 1, :] for a2 in range(SIDE)], axis=0)
        for g in range(2):
            rows = by_z + flip[g].astype(F32) * (by_y - by_z)
            tb_own[g][a1] = rows.astype(BF16)
    for g in range(2):
        tbf[g][0] = tb_own[g][p1[g]].astype(F32)
    dsend[...] = jnp.zeros_like(dsend)

    for g in range(2):
        table_copy(g, 1).start()
        table_copy(g, 3).start()
    for g in range(2):
        first_copy(g, 2).start()
        first_copy(g, 3).start()
    loads[6].start()

    loads[4].wait()
    loads[5].wait()
    logits_t = jnp.dot(tok[...], weight[...], preferred_element_type=F32).T
    for d in range(n):
        block = logits_t[d * PER_DEV : (d + 1) * PER_DEV, :]
        hit = row16[:PER_DEV] == eloc_tbl[d : d + 1, :]
        lsend[d : d + 1, :] = jnp.sum(jnp.where(hit, block, 0.0), axis=0, keepdims=True)

    take_round(0)
    for g in range(2):
        table_copy(g, 2).start()

    slot_iota = lax.broadcasted_iota(I32, (ROW, t_rows), 0).astype(F32)

    def own_table(d, carry):
        row = slot_f32[pl.ds(d, 1), :]
        oh[d] = jnp.where(row == slot_iota, 1.0, 0.0).astype(BF16)
        return carry

    lax.fori_loop(0, n, own_table, 0)
    win[mw] = lsend[...]

    take_round(1)

    def logit_copy(o):
        return to(lsend, win.at[mw], ws, wr, w=lax.rem(mw + o, n_width))

    def send_logits(o, carry):
        logit_copy(o).start()
        return carry

    lax.fori_loop(1, n_width, send_logits, 0)

    cap_iota = lax.broadcasted_iota(I32, (cap, t_rows), 0).astype(F32)

    def select(g, j0, step, count):
        def one(i, carry):
            j = j0 + step * i
            picks = []
            for m in range(SIDE):
                row = tbf[g][j, pl.ds(mod(p2[g] + m), 1), :]
                picks.append(jnp.where(row == cap_iota, 1.0, 0.0).astype(BF16))
            rows = jnp.dot(jnp.concatenate(picks, axis=0), xs_of[g][j], preferred_element_type=F32).astype(BF16)
            rs_of[g][place(g, p1[g] - j, p2[g])] = rows[:cap]
            for m in range(1, SIDE):
                rs_of[g][n + j * SIDE + m] = rows[m * cap : (m + 1) * cap]
            return carry

        if count == 1:
            one(0, 0)
        else:
            lax.fori_loop(0, count, one, 0)

    def near_copy(g, j, kind, start, rows):
        step = (1, -1)[kind]
        part = pl.ds(start, rows)
        return to(
            rs_of[g].at[n + j * SIDE + step % SIDE, part], rs_of[g].at[place(g, p1[g] - j, p2[g]), part],
            ss, sr.at[(6 if start == 0 else 0, 1, 2, 1)[j]], e=ring2(g, step),
        )

    def relay_copy(g, j, h):
        return to(
            rs_of[g].at[n + j * SIDE + 2, pl.ds(h * half, half)], rl_of[g].at[j, h],
            ss, rlr.at[j], e=ring2(g, (1, -1)[h]),
        )

    def final_copy(g, j, h):
        step = (1, -1)[h]
        return to(
            rl_of[g].at[j, h], rs_of[g].at[place(g, p1[g] - j, p2[g] - step), pl.ds(h * half, half)],
            ss, sr.at[3 + (0, 1, 2, 1)[j]], e=ring2(g, step),
        )

    def send_far(j):
        for g in range(2):
            relay_copy(g, j, 0).start()
            relay_copy(g, j, 1).start()

    def pass_on(j):
        await_recv(eo.at[0], rlr.at[j])
        for g in range(2):
            final_copy(g, j, 0).start()
            final_copy(g, j, 1).start()

    def send_near(j, start=0, rows=cap):
        for g in range(2):
            near_copy(g, j, 0, start, rows).start()
            near_copy(g, j, 1, start, rows).start()

    def arrived(index, count, rows=cap):
        await_recv(eo.at[pl.ds(0, count), pl.ds(0, rows)], sr.at[index])

    for g in range(2):
        select(g, 0, 0, 1)
    for k in range(2):
        for g in range(2):
            await_recv(xs_of[g].at[0, pl.ds(0, t_half)], xr.at[2 * g + k])
            onward_copy(g, k).start()
    send_far(0)
    send_near(0, 0, cut)

    def take_tables(js):
        await_recv(tb_in.at[:, pl.ds(0, len(js))], tbr.at[len(js) % 2])
        for g in range(2):
            for j in js:
                tbf[g][j] = tb_in[g, j].astype(F32)

    take_tables((1, 3))
    await_recv(tok, xr.at[4])
    for g in range(2):
        select(g, 1, 2, 2)
    send_far(1)
    send_far(3)
    pass_on(0)

    await_recv(win.at[pl.ds(0, n_width - 1)], wr)
    total_logits = win[0]
    for w in range(1, win.shape[0]):
        total_logits = total_logits + win[w]
    picked = jnp.where(eloc_tbl >= 0, jax.nn.sigmoid(total_logits), 0.0)
    picked_v[...] = picked
    gates = (ROUTE_SCALE * picked / jnp.sum(picked, axis=0, keepdims=True)).astype(BF16).astype(F32)

    gates = gates.astype(BF16)
    for first in range(0, n, 4):
        found = [lax.dot_general(gates, oh[d], NT, preferred_element_type=F32) for d in range(first, first + 4)]
        for i, rows in enumerate(found):
            gsend[first + i] = rows[first + i : first + i + 1, :]
    gin[me] = gsend[me]

    take_round(2)

    def gate_copy(o):
        d = lax.rem(me + o, n)
        return to(gsend.at[d], gin.at[me], gs, gr, e=d)

    def send_gates(o, carry):
        gate_copy(o).start()
        return carry

    lax.fori_loop(1, n, send_gates, 0)

    take_tables((2,))
    await_recv(tok, xr.at[5])
    for g in range(2):
        select(g, 2, 0, 1)
    send_far(2)
    pass_on(1)
    pass_on(3)
    send_near(2)

    loads[6].wait()
    await_recv(gin.at[pl.ds(0, n - 1)], gr)

    ones = jnp.ones((8, 256), BF16)
    eye = lax.broadcasted_iota(I32, (cap, cap), 0) == lax.broadcasted_iota(I32, (cap, cap), 1)

    def gate_grads_of(blocks, start=0, stop=cap):
        found = []
        for s in blocks:
            acc = None
            for g in range(2):
                for at in range(0, cols[g][1], 128):
                    a = rs_of[g][s, start:stop, at : at + 128].astype(F32)
                    b = eo[s, start:stop, cols[g][0] + at : cols[g][0] + at + 128].astype(F32)
                    acc = a * b if acc is None else acc + a * b
            high = acc.astype(BF16)
            low = (acc - high.astype(F32)).astype(BF16)
            both = jnp.concatenate([high, low], axis=1)
            found.append(lax.dot_general(ones, both, NT, preferred_element_type=F32)[0:1, :])
        for s, dots in zip(blocks, found):
            dsend[s, :, start:stop] = dots

    def expert_grad_of(s):
        scale = jnp.where(eye, gin[s][:, :cap], 0.0).astype(BF16)
        for g in range(2):
            value = jnp.dot(scale, rs_of[g][s], preferred_element_type=F32)
            egv[s, :, cols[g][0] : cols[g][0] + cols[g][1]] = value.astype(BF16)

    def far_one(i):
        return 2 * i, 2 - 2 * i

    def far_near(i):
        q, r = i // 2, 1 + 2 * lax.rem(i, 2)
        return 2 * q + (1 - q) * r, q * r + 2 * (1 - q)

    def diagonal(i):
        return 1 + 2 * (i // 2), 1 + 2 * lax.rem(i, 2)

    def beside(i):
        q, r = i // 2, 1 + 2 * lax.rem(i, 2)
        return q * r, (1 - q) * r

    def grads_back(offsets, row):
        blocks = [origin(dy, dz) for dy, dz in offsets]
        gate_grads_of(blocks)
        for i, s in enumerate(blocks):
            to(dsend.at[s], rin.at[row + i], rts, rtr, e=s).start()

    def late_copy(s, row, w):
        return to(dsend.at[s], win2.at[mw, row], w2s, w2r.at[1], e=s, w=w)

    def grads_to_widths(offsets, row, start=0):
        blocks = [origin(dy, dz) for dy, dz in offsets]
        gate_grads_of(blocks, start)

        def one(w, carry):
            for i, s in enumerate(blocks):
                late_copy(s, row + i, w).start()
            return carry

        lax.fori_loop(0, n_width, one, 0)

    def scaled(count, offset):
        def one(i, carry):
            expert_grad_of(origin(*offset(i)))
            return carry

        lax.fori_loop(0, count, one, 0)

    rows = pl.ds(0, EARLY)

    def width_copy(o):
        return to(rin, win2.at[mw, rows], w2s, w2r.at[0], w=lax.rem(mw + o, n_width))

    def send_width(o, carry):
        width_copy(o).start()
        return carry

    gate_grads_of([me])
    rin[0] = dsend[me]
    arrived(3, 1)
    grads_back(FAR_ONE, 1)
    pass_on(2)
    send_near(1)
    scaled(1, lambda i: (0, 0))
    scaled(2, far_one)
    arrived(4, 2)
    arrived(2, 2)
    grads_back(FAR_NEAR, 3)
    arrived(5, 1)
    grads_back(FAR_BOTH, 7)
    send_near(3)
    send_near(0, cut, cap - cut)
    take_round(3)
    scaled(4, far_near)
    scaled(1, lambda i: (2, 2))
    arrived(6, 2, cut)
    gate_grads_of([origin(dy, dz) for dy, dz in BESIDE], 0, cut)
    await_recv(dsend.at[pl.ds(0, EARLY - 1)], rtr)
    lax.fori_loop(1, n_width, send_width, 0)
    win2[mw, rows] = rin[...]
    arrived(1, 4)
    grads_to_widths(DIAGONAL, EARLY)
    arrived(0, 2, cap - cut)
    grads_to_widths(BESIDE, EARLY + len(DIAGONAL), cut)
    scaled(4, diagonal)
    scaled(4, beside)

    await_recv(win2.at[pl.ds(0, n_width - 1), pl.ds(0, EARLY)], w2r.at[0])
    await_recv(win2.at[pl.ds(0, n_width), pl.ds(0, LATE)], w2r.at[1])
    for i, (dy, dz) in enumerate(OFFSETS):
        row = win2[0, i]
        for w in range(1, win2.shape[0]):
            row = row + win2[w, i]
        ggv[pl.ds(target(dy, dz), 1), :] = row

    slots = slot_own[...]
    lane = jnp.bitwise_and(slots, 127)
    pieces = []
    for at in range(0, t_rows, 128):
        index = lane[:, at : at + 128]
        low = jnp.take_along_axis(ggv[:, 0:128], index, axis=1)
        high = jnp.take_along_axis(ggv[:, 128:256], index, axis=1)
        pieces.append(jnp.where(slots[:, at : at + 128] < 128, low, high))
    chosen = slots >= 0
    gate_grads = jnp.where(chosen, jnp.concatenate(pieces, axis=1), 0.0)

    picked = picked_v[...]
    totals = jnp.sum(picked, axis=0, keepdims=True)
    weighted = jnp.sum(gate_grads * picked, axis=0, keepdims=True) / totals
    local = jnp.where(chosen, ROUTE_SCALE / totals * (gate_grads - weighted) * picked * (1.0 - picked), 0.0)
    for d in range(n):
        hit = row16[:PER_DEV] == eloc[d : d + 1, :]
        block = jnp.where(hit, local[d : d + 1, :], 0.0)
        lgt32[d * PER_DEV : (d + 1) * PER_DEV, :] = block
        lgt[d * PER_DEV : (d + 1) * PER_DEV, :] = block.astype(BF16)

    part = jnp.dot(lgt[...], tok[...], preferred_element_type=F32)
    rb[...] = part.astype(BF16).reshape(rb.shape)
    rr[0] = rb[me]

    def send_terms(offsets):
        for dy, dz in offsets:
            d = target(dy, dz)
            to(rb.at[d], rr.at[TERMS.index((dy, dz))], rps, rpr, e=d).start()

    for k, (step, owner) in enumerate(JOINED):
        to(rb.at[target(*owner)], rm.at[k], rps, rms, e=target(*step)).start()
    send_terms(FAR_BOTH + DIAGONAL + BESIDE)
    logit_grads = lgt32[...].T.astype(BF16)
    ig_ref[...] = lax.dot_general(logit_grads, weight[...], NT, preferred_element_type=F32).astype(BF16)
    await_recv(rm, rms)
    for k, owner in ((0, (2, 0)), (2, (0, 2))):
        d = target(*owner)
        rb[d] = (rb[d].astype(F32) + rm[k].astype(F32) + rm[k + 1].astype(F32)).astype(BF16)
    send_terms(FAR_ONE)
    await_recv(rr.at[pl.ds(0, len(TERMS) - 1)], rpr)
    total = rr[0].astype(F32)
    for d in range(1, len(TERMS)):
        total = total + rr[d].astype(F32)
    rg_ref[...] = total

    await_sent(eo.at[pl.ds(0, (SIDE - 1) * t_rows // cap)], xs)
    await_sent(tb_in.at[:, pl.ds(0, SIDE - 1)], tbs)
    await_sent(eo, ss)
    await_sent(win.at[pl.ds(0, n_width - 1)], ws)
    await_sent(gin.at[pl.ds(0, n - 1)], gs)
    await_sent(dsend.at[pl.ds(0, EARLY - 1)], rts)
    await_sent(win2.at[pl.ds(0, n_width), pl.ds(0, n - 1)], w2s)
    await_sent(rb.at[pl.ds(0, n - 1)], rps)


def write_out(eg_in, rg_in, ig_in, eg_out, rg_out, ig_out, sem):
    pieces = 1
    step = eg_in.shape[0] // pieces
    pairs = [(eg_in.at[pl.ds(i * step, step)], eg_out.at[pl.ds(i * step, step)]) for i in range(pieces)]
    pairs += [(ig_in, ig_out), (rg_in, rg_out)]
    copies = [pltpu.make_async_copy(src, dst, sem.at[i]) for i, (src, dst) in enumerate(pairs)]
    for copy in copies:
        copy.start()
    for copy in copies:
        copy.wait()


def body(tokens_in, out_grad, router_weight, expert_out, expert_ids, slot_ids):
    n = lax.axis_size("expert")
    n_width = lax.axis_size("width")
    t_rows, d_cols = out_grad.shape
    top = expert_ids.shape[1]
    experts = router_weight.shape[1]
    cap = t_rows * top // n
    c0 = (d_cols // 128 + 1) // 2 * 128
    c1 = d_cols - c0
    hbm, vmem = pl.BlockSpec(memory_space=pltpu.HBM), pl.BlockSpec(memory_space=pltpu.VMEM)
    dma = pltpu.SemaphoreType.DMA
    scratch = [
        pltpu.VMEM((SIDE, t_rows, c0), BF16),
        pltpu.VMEM((SIDE, t_rows, c1), BF16),
        pltpu.VMEM((2 * n, cap, c0), BF16),
        pltpu.VMEM((2 * n, cap, c1), BF16),
        pltpu.VMEM((SIDE, 2, cap // 2, c0), BF16),
        pltpu.VMEM((SIDE, 2, cap // 2, c1), BF16),
        pltpu.VMEM((t_rows, d_cols), BF16),
        pltpu.VMEM((d_cols, experts), BF16),
        pltpu.VMEM((n, cap, d_cols), BF16),
        pltpu.VMEM((top, t_rows), I32),
        pltpu.VMEM((top, t_rows), I32),
        pltpu.VMEM((n, ROW, t_rows), BF16),
        pltpu.VMEM((SIDE, SIDE, t_rows), BF16),
        pltpu.VMEM((SIDE, SIDE, t_rows), BF16),
        pltpu.VMEM((2, SIDE, SIDE, t_rows), BF16),
        pltpu.VMEM((SIDE, SIDE, t_rows), F32),
        pltpu.VMEM((SIDE, SIDE, t_rows), F32),
        pltpu.VMEM((n, t_rows), F32),
        pltpu.VMEM((n, t_rows), I32),
        pltpu.VMEM((n, t_rows), I32),
        pltpu.VMEM((n, t_rows), F32),
        pltpu.VMEM((n_width, n, t_rows), F32),
        pltpu.VMEM((n, 1, ROW), F32),
        pltpu.VMEM((n, 1, ROW), F32),
        pltpu.VMEM((n, 1, ROW), F32),
        pltpu.VMEM((EARLY, 1, ROW), F32),
        pltpu.VMEM((n_width, n, 1, ROW), F32),
        pltpu.VMEM((n, ROW), F32),
        pltpu.VMEM((n, t_rows), F32),
        pltpu.VMEM((experts, t_rows), F32),
        pltpu.VMEM((experts, t_rows), BF16),
        pltpu.VMEM((n, experts // n, d_cols), BF16),
        pltpu.VMEM((len(TERMS), experts // n, d_cols), BF16),
        pltpu.VMEM((len(JOINED), experts // n, d_cols), BF16),
        pltpu.SemaphoreType.REGULAR((ROUNDS,)),
        dma((7,)),
        dma(()), dma((6,)),
        dma(()), dma((2,)),
        dma(()), dma(()),
        dma(()), dma(()),
        dma(()), dma((7,)), dma((SIDE,)),
        dma(()), dma(()),
        dma(()), dma((2,)),
        dma(()), dma(()), dma(()),
    ]
    expert_grad, router_grad, input_grad = pl.pallas_call(
        kernel,
        out_shape=(
            pltpu.VMEM((n, cap, d_cols), BF16),
            pltpu.VMEM((experts // n, d_cols), F32),
            pltpu.VMEM((t_rows, d_cols), BF16),
        ),
        in_specs=[hbm] * 6,
        out_specs=(vmem, vmem, vmem),
        scratch_shapes=scratch,
        compiler_params=pltpu.CompilerParams(
            collective_id=0, has_side_effects=True, vmem_limit_bytes=46 * 1024 * 1024
        ),
    )(*(
        pltpu.with_memory_space_constraint(a, pltpu.HBM)
        for a in (tokens_in, out_grad, router_weight, expert_out.reshape(n, cap, d_cols), expert_ids.T, slot_ids.T)
    ))
    expert_grad, router_grad, input_grad = pl.pallas_call(
        write_out,
        out_shape=(
            jax.ShapeDtypeStruct((n, cap, d_cols), BF16),
            jax.ShapeDtypeStruct((experts // n, d_cols), F32),
            jax.ShapeDtypeStruct((t_rows, d_cols), BF16),
        ),
        in_specs=[vmem, vmem, vmem],
        out_specs=(hbm, hbm, hbm),
        scratch_shapes=[dma((3,))],
        compiler_params=pltpu.CompilerParams(vmem_limit_bytes=2 * 1024 * 1024),
    )(*(pltpu.with_memory_space_constraint(a, pltpu.VMEM) for a in (expert_grad, router_grad, input_grad)))
    return expert_grad.reshape(n * cap, d_cols), router_grad.T, input_grad


def solution(mesh):
    return jax.shard_map(
        body,
        mesh=mesh,
        in_specs=(
            P("expert", "width"),
            P("expert", "width"),
            P("width", None),
            P("expert", "width"),
            P("expert", None),
            P("expert", None),
        ),
        out_specs=(P("expert", "width"), P("width", "expert"), P("expert", "width")),
        check_vma=False,
    )
```

```python
import functools

import jax
import jax.numpy as jnp
from jax import lax
from jax.experimental import pallas as pl
from jax.experimental.pallas import tpu as pltpu
from jax.sharding import PartitionSpec as P

MESH = pl.DeviceIdType.MESH
SIDE = 4
PER_DEV = 16
ROUTE_SCALE = 2.5
ROW = 256
BF16, F32, I32 = jnp.bfloat16, jnp.float32, jnp.int32
NT = (((1,), (1,)), ((), ()))


SELF = ((0, 0),)
FAR_ONE = ((0, 2), (2, 0))
FAR_BOTH = ((2, 2),)
FAR_NEAR = ((1, 2), (3, 2), (2, 1), (2, 3))
DIAGONAL = ((1, 1), (1, 3), (3, 1), (3, 3))
BESIDE = ((0, 1), (0, 3), (1, 0), (3, 0))
OFFSETS = SELF + FAR_ONE + FAR_NEAR + FAR_BOTH + DIAGONAL + BESIDE
LATE_ONES = DIAGONAL + BESIDE
EARLY, LATE = 8, 8
ROUNDS = 4
JOINED = (((0, 1), (2, 1)), ((0, 3), (2, 3)), ((1, 0), (1, 2)), ((3, 0), (3, 2)))
TERMS = SELF + FAR_ONE + FAR_BOTH + DIAGONAL + BESIDE


def kernel(
    tok_hbm, grad_hbm, weight_hbm, eo_hbm, ids_hbm, slots_hbm,
    egv, rg_ref, ig_ref,
    x0, x1, rs0, rs1, rl0, rl1, tok, weight, eo, ids_ref, slots_ref, oh,
    tb_own0, tb_own1, tb_in, tbf0, tbf1, slot_f32, slot_own, eloc, lsend, win, gsend, gin, dsend, rin, win2,
    ggv, picked_v, lgt32, lgt, rb, rr, rm,
    known, in_sem, xs, xr, tbs, tbr, ws, wr, gs, gr, ss, sr, rlr, rts, rtr, w2s, w2r, rps, rpr, rms,
):
    n = lax.axis_size("expert")
    n_width = lax.axis_size("width")
    me = lax.axis_index("expert")
    mw = lax.axis_index("width")
    top, t_rows = ids_ref.shape
    cap = rs0.shape[1]
    t_half = t_rows // 2
    half = cap // 2
    cut = half
    xs_of, rs_of, rl_of = (x0, x1), (rs0, rs1), (rl0, rl1)
    tb_own, tbf = (tb_own0, tb_own1), (tbf0, tbf1)
    c0 = x0.shape[2]
    cols = ((0, c0), (c0, x1.shape[2]))
    core = lax.rem(mw, 2)
    gy, gz = me // SIDE, lax.rem(me, SIDE)

    flip = (core, 1 - core)
    p1 = tuple(gz + f * (gy - gz) for f in flip)
    p2 = tuple(gy + f * (gz - gy) for f in flip)

    def mod(v):
        return lax.rem(v + 2 * SIDE, SIDE)

    def place(g, a1, a2):
        return mod(a1) * (1 + (SIDE - 1) * flip[g]) + mod(a2) * (SIDE - (SIDE - 1) * flip[g])

    def ring1(g, step):
        return place(g, p1[g] + step, p2[g])

    def ring2(g, step):
        return place(g, p1[g], p2[g] + step)

    def target(dy, dz):
        return mod(gy + dy) * SIDE + mod(gz + dz)

    def origin(dy, dz):
        return mod(gy - dy) * SIDE + mod(gz - dz)

    def to(src, dst, send, recv, e=None, w=None):
        where = {"expert": me if e is None else e, "width": mw if w is None else w}
        return pltpu.make_async_remote_copy(
            src_ref=src, dst_ref=dst, send_sem=send, recv_sem=recv, device_id=where, device_id_type=MESH
        )

    def await_recv(like, sem):
        to(like, like, sem, sem).wait_recv()

    def await_sent(like, sem):
        to(like, like, sem, sem).wait_send()

    barrier = pltpu.get_barrier_semaphore()

    x_here = mw // 2
    xs_count = n_width // 2

    def greet(sem):
        for dy, dz in BESIDE:
            pl.semaphore_signal(sem, inc=1, device_id={"expert": target(dy, dz), "width": mw}, device_id_type=MESH)
        for step in (1, xs_count - 1):
            w = lax.rem(x_here + step, xs_count) * 2 + core
            pl.semaphore_signal(sem, inc=1, device_id={"expert": me, "width": w}, device_id_type=MESH)
        pl.semaphore_signal(
            sem, inc=1, device_id={"expert": me, "width": x_here * 2 + 1 - core}, device_id_type=MESH
        )

    def take_round(k):
        pl.semaphore_wait(known.at[k], len(BESIDE) + 3)
        if k + 1 < ROUNDS:
            greet(known.at[k + 1])

    loads = [
        pltpu.make_async_copy(src, dst, in_sem.at[i])
        for i, (src, dst) in enumerate((
            (grad_hbm.at[:, pl.ds(0, c0)], x0.at[0]),
            (grad_hbm.at[:, pl.ds(c0, cols[1][1])], x1.at[0]),
            (ids_hbm, ids_ref),
            (slots_hbm, slots_ref),
            (tok_hbm, tok),
            (weight_hbm, weight),
            (eo_hbm, eo),
        ))
    ]
    loads[0].start()
    loads[1].start()
    greet(barrier)
    loads[2].start()
    loads[3].start()
    pl.semaphore_wait(barrier, len(BESIDE) + 3)

    def first_copy(g, k):
        step, h = ((1, 0), (-1, 1), (1, 1), (-1, 0))[k]
        rows = pl.ds(h * t_half, t_half)
        return to(
            xs_of[g].at[0, rows], xs_of[g].at[step % SIDE, rows], xs, xr.at[2 * g + k if k < 2 else 4], e=ring1(g, step)
        )

    def onward_copy(g, k):
        step, h = ((1, 0), (-1, 1))[k]
        rows = pl.ds(h * t_half, t_half)
        return to(xs_of[g].at[step % SIDE, rows], xs_of[g].at[2, rows], xs, xr.at[5], e=ring1(g, step))

    def table_copy(g, j):
        return to(
            tb_own[g].at[mod(p1[g] + j)], tb_in.at[g, j], tbs, tbr.at[j // 2 * (3 - j)], e=ring1(g, j)
        )

    for g in range(2):
        loads[g].wait()
        first_copy(g, 0).start()
        first_copy(g, 1).start()
    greet(known.at[0])
    loads[4].start()
    loads[5].start()
    loads[2].wait()
    loads[3].wait()
    row16 = lax.broadcasted_iota(I32, (n, t_rows), 0)
    slot_tbl = jnp.full((n, t_rows), -1, I32)
    eloc_tbl = jnp.full((n, t_rows), -1, I32)
    for k in range(top):
        ids = ids_ref[k : k + 1, :]
        dev = lax.shift_right_logical(ids, 4)
        hit = row16 == dev
        slot_tbl = jnp.where(hit, slots_ref[k : k + 1, :], slot_tbl)
        eloc_tbl = jnp.where(hit, ids - dev * PER_DEV, eloc_tbl)
    slot_own[...] = slot_tbl
    eloc[...] = eloc_tbl
    slot_f = slot_tbl.astype(F32)
    slot_f32[...] = slot_f
    for a1 in range(SIDE):
        by_y = slot_f[a1 * SIDE : (a1 + 1) * SIDE, :]
        by_z = jnp.concatenate([slot_f[a2 * SIDE + a1 : a2 * SIDE + a1 + 1, :] for a2 in range(SIDE)], axis=0)
        for g in range(2):
            rows = by_z + flip[g].astype(F32) * (by_y - by_z)
            tb_own[g][a1] = rows.astype(BF16)
    for g in range(2):
        tbf[g][0] = tb_own[g][p1[g]].astype(F32)
    dsend[...] = jnp.zeros_like(dsend)

    for g in range(2):
        table_copy(g, 1).start()
        table_copy(g, 3).start()
    for g in range(2):
        first_copy(g, 2).start()
        first_copy(g, 3).start()
    loads[6].start()

    loads[4].wait()
    loads[5].wait()
    logits_t = jnp.dot(tok[...], weight[...], preferred_element_type=F32).T
    for d in range(n):
        block = logits_t[d * PER_DEV : (d + 1) * PER_DEV, :]
        hit = row16[:PER_DEV] == eloc_tbl[d : d + 1, :]
        lsend[d : d + 1, :] = jnp.sum(jnp.where(hit, block, 0.0), axis=0, keepdims=True)

    take_round(0)
    for g in range(2):
        table_copy(g, 2).start()

    slot_iota = lax.broadcasted_iota(I32, (ROW, t_rows), 0).astype(F32)

    def own_table(d, carry):
        row = slot_f32[pl.ds(d, 1), :]
        oh[d] = jnp.where(row == slot_iota, 1.0, 0.0).astype(BF16)
        return carry

    lax.fori_loop(0, n, own_table, 0)
    win[mw] = lsend[...]

    take_round(1)

    def logit_copy(o):
        return to(lsend, win.at[mw], ws, wr, w=lax.rem(mw + o, n_width))

    def send_logits(o, carry):
        logit_copy(o).start()
        return carry

    lax.fori_loop(1, n_width, send_logits, 0)

    cap_iota = lax.broadcasted_iota(I32, (cap, t_rows), 0).astype(F32)

    def select(g, j0, step, count):
        def one(i, carry):
            j = j0 + step * i
            picks = []
            for m in range(SIDE):
                row = tbf[g][j, pl.ds(mod(p2[g] + m), 1), :]
                picks.append(jnp.where(row == cap_iota, 1.0, 0.0).astype(BF16))
            rows = jnp.dot(jnp.concatenate(picks, axis=0), xs_of[g][j], preferred_element_type=F32).astype(BF16)
            rs_of[g][place(g, p1[g] - j, p2[g])] = rows[:cap]
            for m in range(1, SIDE):
                rs_of[g][n + j * SIDE + m] = rows[m * cap : (m + 1) * cap]
            return carry

        if count == 1:
            one(0, 0)
        else:
            lax.fori_loop(0, count, one, 0)

    def near_copy(g, j, kind, start, rows):
        step = (1, -1)[kind]
        part = pl.ds(start, rows)
        return to(
            rs_of[g].at[n + j * SIDE + step % SIDE, part], rs_of[g].at[place(g, p1[g] - j, p2[g]), part],
            ss, sr.at[(6 if start == 0 else 0, 1, 2, 1)[j]], e=ring2(g, step),
        )

    def relay_copy(g, j, h):
        return to(
            rs_of[g].at[n + j * SIDE + 2, pl.ds(h * half, half)], rl_of[g].at[j, h],
            ss, rlr.at[j], e=ring2(g, (1, -1)[h]),
        )

    def final_copy(g, j, h):
        step = (1, -1)[h]
        return to(
            rl_of[g].at[j, h], rs_of[g].at[place(g, p1[g] - j, p2[g] - step), pl.ds(h * half, half)],
            ss, sr.at[3 + (0, 1, 2, 1)[j]], e=ring2(g, step),
        )

    def send_far(j):
        for g in range(2):
            relay_copy(g, j, 0).start()
            relay_copy(g, j, 1).start()

    def pass_on(j):
        await_recv(eo.at[0], rlr.at[j])
        for g in range(2):
            final_copy(g, j, 0).start()
            final_copy(g, j, 1).start()

    def send_near(j, start=0, rows=cap):
        for g in range(2):
            near_copy(g, j, 0, start, rows).start()
            near_copy(g, j, 1, start, rows).start()

    def arrived(index, count, rows=cap):
        await_recv(eo.at[pl.ds(0, count), pl.ds(0, rows)], sr.at[index])

    for g in range(2):
        select(g, 0, 0, 1)
    for k in range(2):
        for g in range(2):
            await_recv(xs_of[g].at[0, pl.ds(0, t_half)], xr.at[2 * g + k])
            onward_copy(g, k).start()
    send_far(0)
    send_near(0, 0, cut)

    def take_tables(js):
        await_recv(tb_in.at[:, pl.ds(0, len(js))], tbr.at[len(js) % 2])
        for g in range(2):
            for j in js:
                tbf[g][j] = tb_in[g, j].astype(F32)

    take_tables((1, 3))
    await_recv(tok, xr.at[4])
    for g in range(2):
        select(g, 1, 2, 2)
    send_far(1)
    send_far(3)
    pass_on(0)

    await_recv(win.at[pl.ds(0, n_width - 1)], wr)
    total_logits = win[0]
    for w in range(1, win.shape[0]):
        total_logits = total_logits + win[w]
    picked = jnp.where(eloc_tbl >= 0, jax.nn.sigmoid(total_logits), 0.0)
    picked_v[...] = picked
    gates = (ROUTE_SCALE * picked / jnp.sum(picked, axis=0, keepdims=True)).astype(BF16).astype(F32)

    gates = gates.astype(BF16)
    for first in range(0, n, 4):
        found = [lax.dot_general(gates, oh[d], NT, preferred_element_type=F32) for d in range(first, first + 4)]
        for i, rows in enumerate(found):
            gsend[first + i] = rows[first + i : first + i + 1, :]
    gin[me] = gsend[me]

    take_round(2)

    def gate_copy(o):
        d = lax.rem(me + o, n)
        return to(gsend.at[d], gin.at[me], gs, gr, e=d)

    def send_gates(o, carry):
        gate_copy(o).start()
        return carry

    lax.fori_loop(1, n, send_gates, 0)

    take_tables((2,))
    await_recv(tok, xr.at[5])
    for g in range(2):
        select(g, 2, 0, 1)
    send_far(2)
    pass_on(1)
    pass_on(3)
    send_near(2)

    loads[6].wait()
    await_recv(gin.at[pl.ds(0, n - 1)], gr)

    ones = jnp.ones((8, 256), BF16)
    eye = lax.broadcasted_iota(I32, (cap, cap), 0) == lax.broadcasted_iota(I32, (cap, cap), 1)

    def gate_grads_of(blocks, start=0, stop=cap):
        found = []
        for s in blocks:
            acc = None
            for g in range(2):
                for at in range(0, cols[g][1], 128):
                    a = rs_of[g][s, start:stop, at : at + 128].astype(F32)
                    b = eo[s, start:stop, cols[g][0] + at : cols[g][0] + at + 128].astype(F32)
                    acc = a * b if acc is None else acc + a * b
            high = acc.astype(BF16)
            low = (acc - high.astype(F32)).astype(BF16)
            both = jnp.concatenate([high, low], axis=1)
            found.append(lax.dot_general(ones, both, NT, preferred_element_type=F32)[0:1, :])
        for s, dots in zip(blocks, found):
            dsend[s, :, start:stop] = dots

    def expert_grad_of(s):
        scale = jnp.where(eye, gin[s][:, :cap], 0.0).astype(BF16)
        for g in range(2):
            value = jnp.dot(scale, rs_of[g][s], preferred_element_type=F32)
            egv[s, :, cols[g][0] : cols[g][0] + cols[g][1]] = value.astype(BF16)

    def far_one(i):
        return 2 * i, 2 - 2 * i

    def far_near(i):
        q, r = i // 2, 1 + 2 * lax.rem(i, 2)
        return 2 * q + (1 - q) * r, q * r + 2 * (1 - q)

    def diagonal(i):
        return 1 + 2 * (i // 2), 1 + 2 * lax.rem(i, 2)

    def beside(i):
        q, r = i // 2, 1 + 2 * lax.rem(i, 2)
        return q * r, (1 - q) * r

    def grads_back(offsets, row):
        blocks = [origin(dy, dz) for dy, dz in offsets]
        gate_grads_of(blocks)
        for i, s in enumerate(blocks):
            to(dsend.at[s], rin.at[row + i], rts, rtr, e=s).start()

    def late_copy(s, row, w):
        return to(dsend.at[s], win2.at[mw, row], w2s, w2r.at[1], e=s, w=w)

    def grads_to_widths(offsets, row, start=0):
        blocks = [origin(dy, dz) for dy, dz in offsets]
        gate_grads_of(blocks, start)

        def one(w, carry):
            for i, s in enumerate(blocks):
                late_copy(s, row + i, w).start()
            return carry

        lax.fori_loop(0, n_width, one, 0)

    def scaled(count, offset):
        def one(i, carry):
            expert_grad_of(origin(*offset(i)))
            return carry

        lax.fori_loop(0, count, one, 0)

    rows = pl.ds(0, EARLY)

    def width_copy(o):
        return to(rin, win2.at[mw, rows], w2s, w2r.at[0], w=lax.rem(mw + o, n_width))

    def send_width(o, carry):
        width_copy(o).start()
        return carry

    gate_grads_of([me])
    rin[0] = dsend[me]
    arrived(3, 1)
    grads_back(FAR_ONE, 1)
    pass_on(2)
    send_near(1)
    scaled(1, lambda i: (0, 0))
    scaled(2, far_one)
    arrived(4, 2)
    arrived(2, 2)
    grads_back(FAR_NEAR, 3)
    arrived(5, 1)
    grads_back(FAR_BOTH, 7)
    send_near(3)
    send_near(0, cut, cap - cut)
    take_round(3)
    scaled(4, far_near)
    scaled(1, lambda i: (2, 2))
    arrived(6, 2, cut)
    gate_grads_of([origin(dy, dz) for dy, dz in BESIDE], 0, cut)
    await_recv(dsend.at[pl.ds(0, EARLY - 1)], rtr)
    lax.fori_loop(1, n_width, send_width, 0)
    win2[mw, rows] = rin[...]
    arrived(1, 4)
    grads_to_widths(DIAGONAL, EARLY)
    arrived(0, 2, cap - cut)
    grads_to_widths(BESIDE, EARLY + len(DIAGONAL), cut)
    scaled(4, diagonal)
    scaled(4, beside)

    await_recv(win2.at[pl.ds(0, n_width - 1), pl.ds(0, EARLY)], w2r.at[0])
    await_recv(win2.at[pl.ds(0, n_width), pl.ds(0, LATE)], w2r.at[1])
    for i, (dy, dz) in enumerate(OFFSETS):
        row = win2[0, i]
        for w in range(1, win2.shape[0]):
            row = row + win2[w, i]
        ggv[pl.ds(target(dy, dz), 1), :] = row

    slots = slot_own[...]
    lane = jnp.bitwise_and(slots, 127)
    pieces = []
    for at in range(0, t_rows, 128):
        index = lane[:, at : at + 128]
        low = jnp.take_along_axis(ggv[:, 0:128], index, axis=1)
        high = jnp.take_along_axis(ggv[:, 128:256], index, axis=1)
        pieces.append(jnp.where(slots[:, at : at + 128] < 128, low, high))
    chosen = slots >= 0
    gate_grads = jnp.where(chosen, jnp.concatenate(pieces, axis=1), 0.0)

    picked = picked_v[...]
    totals = jnp.sum(picked, axis=0, keepdims=True)
    weighted = jnp.sum(gate_grads * picked, axis=0, keepdims=True) / totals
    local = jnp.where(chosen, ROUTE_SCALE / totals * (gate_grads - weighted) * picked * (1.0 - picked), 0.0)
    for d in range(n):
        hit = row16[:PER_DEV] == eloc[d : d + 1, :]
        block = jnp.where(hit, local[d : d + 1, :], 0.0)
        lgt32[d * PER_DEV : (d + 1) * PER_DEV, :] = block
        lgt[d * PER_DEV : (d + 1) * PER_DEV, :] = block.astype(BF16)

    part = jnp.dot(lgt[...], tok[...], preferred_element_type=F32)
    rb[...] = part.astype(BF16).reshape(rb.shape)
    rr[0] = rb[me]

    def send_terms(offsets):
        for dy, dz in offsets:
            d = target(dy, dz)
            to(rb.at[d], rr.at[TERMS.index((dy, dz))], rps, rpr, e=d).start()

    for k, (step, owner) in enumerate(JOINED):
        to(rb.at[target(*owner)], rm.at[k], rps, rms, e=target(*step)).start()
    send_terms(FAR_BOTH + BESIDE + DIAGONAL)
    logit_grads = lgt32[...].T.astype(BF16)
    ig_ref[...] = lax.dot_general(logit_grads, weight[...], NT, preferred_element_type=F32).astype(BF16)
    await_recv(rm, rms)
    for k, owner in ((0, (2, 0)), (2, (0, 2))):
        d = target(*owner)
        rb[d] = (rb[d].astype(F32) + rm[k].astype(F32) + rm[k + 1].astype(F32)).astype(BF16)
    send_terms(FAR_ONE)
    await_recv(rr.at[pl.ds(0, len(TERMS) - 1)], rpr)
    total = rr[0].astype(F32)
    for d in range(1, len(TERMS)):
        total = total + rr[d].astype(F32)
    rg_ref[...] = total

    await_sent(eo.at[pl.ds(0, (SIDE - 1) * t_rows // cap)], xs)
    await_sent(tb_in.at[:, pl.ds(0, SIDE - 1)], tbs)
    await_sent(eo, ss)
    await_sent(win.at[pl.ds(0, n_width - 1)], ws)
    await_sent(gin.at[pl.ds(0, n - 1)], gs)
    await_sent(dsend.at[pl.ds(0, EARLY - 1)], rts)
    await_sent(win2.at[pl.ds(0, n_width), pl.ds(0, n - 1)], w2s)
    await_sent(rb.at[pl.ds(0, n - 1)], rps)


def write_out(eg_in, rg_in, ig_in, eg_out, rg_out, ig_out, sem):
    pieces = 1
    step = eg_in.shape[0] // pieces
    pairs = [(eg_in.at[pl.ds(i * step, step)], eg_out.at[pl.ds(i * step, step)]) for i in range(pieces)]
    pairs += [(ig_in, ig_out), (rg_in, rg_out)]
    copies = [pltpu.make_async_copy(src, dst, sem.at[i]) for i, (src, dst) in enumerate(pairs)]
    for copy in copies:
        copy.start()
    for copy in copies:
        copy.wait()


def body(tokens_in, out_grad, router_weight, expert_out, expert_ids, slot_ids):
    n = lax.axis_size("expert")
    n_width = lax.axis_size("width")
    t_rows, d_cols = out_grad.shape
    top = expert_ids.shape[1]
    experts = router_weight.shape[1]
    cap = t_rows * top // n
    c0 = (d_cols // 128 + 1) // 2 * 128
    c1 = d_cols - c0
    hbm, vmem = pl.BlockSpec(memory_space=pltpu.HBM), pl.BlockSpec(memory_space=pltpu.VMEM)
    dma = pltpu.SemaphoreType.DMA
    scratch = [
        pltpu.VMEM((SIDE, t_rows, c0), BF16),
        pltpu.VMEM((SIDE, t_rows, c1), BF16),
        pltpu.VMEM((2 * n, cap, c0), BF16),
        pltpu.VMEM((2 * n, cap, c1), BF16),
        pltpu.VMEM((SIDE, 2, cap // 2, c0), BF16),
        pltpu.VMEM((SIDE, 2, cap // 2, c1), BF16),
        pltpu.VMEM((t_rows, d_cols), BF16),
        pltpu.VMEM((d_cols, experts), BF16),
        pltpu.VMEM((n, cap, d_cols), BF16),
        pltpu.VMEM((top, t_rows), I32),
        pltpu.VMEM((top, t_rows), I32),
        pltpu.VMEM((n, ROW, t_rows), BF16),
        pltpu.VMEM((SIDE, SIDE, t_rows), BF16),
        pltpu.VMEM((SIDE, SIDE, t_rows), BF16),
        pltpu.VMEM((2, SIDE, SIDE, t_rows), BF16),
        pltpu.VMEM((SIDE, SIDE, t_rows), F32),
        pltpu.VMEM((SIDE, SIDE, t_rows), F32),
        pltpu.VMEM((n, t_rows), F32),
        pltpu.VMEM((n, t_rows), I32),
        pltpu.VMEM((n, t_rows), I32),
        pltpu.VMEM((n, t_rows), F32),
        pltpu.VMEM((n_width, n, t_rows), F32),
        pltpu.VMEM((n, 1, ROW), F32),
        pltpu.VMEM((n, 1, ROW), F32),
        pltpu.VMEM((n, 1, ROW), F32),
        pltpu.VMEM((EARLY, 1, ROW), F32),
        pltpu.VMEM((n_width, n, 1, ROW), F32),
        pltpu.VMEM((n, ROW), F32),
        pltpu.VMEM((n, t_rows), F32),
        pltpu.VMEM((experts, t_rows), F32),
        pltpu.VMEM((experts, t_rows), BF16),
        pltpu.VMEM((n, experts // n, d_cols), BF16),
        pltpu.VMEM((len(TERMS), experts // n, d_cols), BF16),
        pltpu.VMEM((len(JOINED), experts // n, d_cols), BF16),
        pltpu.SemaphoreType.REGULAR((ROUNDS,)),
        dma((7,)),
        dma(()), dma((6,)),
        dma(()), dma((2,)),
        dma(()), dma(()),
        dma(()), dma(()),
        dma(()), dma((7,)), dma((SIDE,)),
        dma(()), dma(()),
        dma(()), dma((2,)),
        dma(()), dma(()), dma(()),
    ]
    expert_grad, router_grad, input_grad = pl.pallas_call(
        kernel,
        out_shape=(
            pltpu.VMEM((n, cap, d_cols), BF16),
            pltpu.VMEM((experts // n, d_cols), F32),
            pltpu.VMEM((t_rows, d_cols), BF16),
        ),
        in_specs=[hbm] * 6,
        out_specs=(vmem, vmem, vmem),
        scratch_shapes=scratch,
        compiler_params=pltpu.CompilerParams(
            collective_id=0, has_side_effects=True, vmem_limit_bytes=46 * 1024 * 1024
        ),
    )(*(
        pltpu.with_memory_space_constraint(a, pltpu.HBM)
        for a in (tokens_in, out_grad, router_weight, expert_out.reshape(n, cap, d_cols), expert_ids.T, slot_ids.T)
    ))
    expert_grad, router_grad, input_grad = pl.pallas_call(
        write_out,
        out_shape=(
            jax.ShapeDtypeStruct((n, cap, d_cols), BF16),
            jax.ShapeDtypeStruct((experts // n, d_cols), F32),
            jax.ShapeDtypeStruct((t_rows, d_cols), BF16),
        ),
        in_specs=[vmem, vmem, vmem],
        out_specs=(hbm, hbm, hbm),
        scratch_shapes=[dma((3,))],
        compiler_params=pltpu.CompilerParams(vmem_limit_bytes=2 * 1024 * 1024),
    )(*(pltpu.with_memory_space_constraint(a, pltpu.VMEM) for a in (expert_grad, router_grad, input_grad)))
    return expert_grad.reshape(n * cap, d_cols), router_grad.T, input_grad


def solution(mesh):
    return jax.shard_map(
        body,
        mesh=mesh,
        in_specs=(
            P("expert", "width"),
            P("expert", "width"),
            P("width", None),
            P("expert", "width"),
            P("expert", None),
            P("expert", None),
        ),
        out_specs=(P("expert", "width"), P("width", "expert"), P("expert", "width")),
        check_vma=False,
    )
```

```python
import functools

import jax
import jax.numpy as jnp
from jax import lax
from jax.experimental import pallas as pl
from jax.experimental.pallas import tpu as pltpu
from jax.sharding import PartitionSpec as P

MESH = pl.DeviceIdType.MESH
SIDE = 4
PER_DEV = 16
ROUTE_SCALE = 2.5
ROW = 256
BF16, F32, I32 = jnp.bfloat16, jnp.float32, jnp.int32
NT = (((1,), (1,)), ((), ()))


SELF = ((0, 0),)
FAR_ONE = ((0, 2), (2, 0))
FAR_BOTH = ((2, 2),)
FAR_NEAR = ((1, 2), (3, 2), (2, 1), (2, 3))
DIAGONAL = ((1, 1), (1, 3), (3, 1), (3, 3))
BESIDE = ((0, 1), (0, 3), (1, 0), (3, 0))
OFFSETS = SELF + FAR_ONE + FAR_NEAR + FAR_BOTH + DIAGONAL + BESIDE
LATE_ONES = DIAGONAL + BESIDE
EARLY, LATE = 8, 8
ROUNDS = 4
JOINED = (((0, 1), (2, 1)), ((0, 3), (2, 3)), ((1, 0), (1, 2)), ((3, 0), (3, 2)))
TERMS = SELF + FAR_ONE + FAR_BOTH + DIAGONAL + BESIDE


def kernel(
    tok_hbm, grad_hbm, weight_hbm, eo_hbm, ids_hbm, slots_hbm,
    egv, rg_ref, ig_ref,
    x0, x1, rs0, rs1, rl0, rl1, tok, weight, eo, ids_ref, slots_ref, oh,
    tb_own0, tb_own1, tb_in, tbf0, tbf1, slot_f32, slot_own, eloc, lsend, win, gsend, gin, dsend, rin, win2,
    ggv, picked_v, lgt32, lgt, rb, rr, rm,
    known, in_sem, xs, xr, tbs, tbr, ws, wr, gs, gr, ss, sr, rlr, rts, rtr, w2s, w2r, rps, rpr, rms,
):
    n = lax.axis_size("expert")
    n_width = lax.axis_size("width")
    me = lax.axis_index("expert")
    mw = lax.axis_index("width")
    top, t_rows = ids_ref.shape
    cap = rs0.shape[1]
    t_half = t_rows // 2
    half = cap // 2
    cut = half
    xs_of, rs_of, rl_of = (x0, x1), (rs0, rs1), (rl0, rl1)
    tb_own, tbf = (tb_own0, tb_own1), (tbf0, tbf1)
    c0 = x0.shape[2]
    cols = ((0, c0), (c0, x1.shape[2]))
    core = lax.rem(mw, 2)
    gy, gz = me // SIDE, lax.rem(me, SIDE)

    flip = (core, 1 - core)
    p1 = tuple(gz + f * (gy - gz) for f in flip)
    p2 = tuple(gy + f * (gz - gy) for f in flip)

    def mod(v):
        return lax.rem(v + 2 * SIDE, SIDE)

    def place(g, a1, a2):
        return mod(a1) * (1 + (SIDE - 1) * flip[g]) + mod(a2) * (SIDE - (SIDE - 1) * flip[g])

    def ring1(g, step):
        return place(g, p1[g] + step, p2[g])

    def ring2(g, step):
        return place(g, p1[g], p2[g] + step)

    def target(dy, dz):
        return mod(gy + dy) * SIDE + mod(gz + dz)

    def origin(dy, dz):
        return mod(gy - dy) * SIDE + mod(gz - dz)

    def to(src, dst, send, recv, e=None, w=None):
        where = {"expert": me if e is None else e, "width": mw if w is None else w}
        return pltpu.make_async_remote_copy(
            src_ref=src, dst_ref=dst, send_sem=send, recv_sem=recv, device_id=where, device_id_type=MESH
        )

    def await_recv(like, sem):
        to(like, like, sem, sem).wait_recv()

    def await_sent(like, sem):
        to(like, like, sem, sem).wait_send()

    barrier = pltpu.get_barrier_semaphore()

    x_here = mw // 2
    xs_count = n_width // 2

    def greet(sem):
        for dy, dz in BESIDE:
            pl.semaphore_signal(sem, inc=1, device_id={"expert": target(dy, dz), "width": mw}, device_id_type=MESH)
        for step in (1, xs_count - 1):
            w = lax.rem(x_here + step, xs_count) * 2 + core
            pl.semaphore_signal(sem, inc=1, device_id={"expert": me, "width": w}, device_id_type=MESH)
        pl.semaphore_signal(
            sem, inc=1, device_id={"expert": me, "width": x_here * 2 + 1 - core}, device_id_type=MESH
        )

    def take_round(k):
        pl.semaphore_wait(known.at[k], len(BESIDE) + 3)
        if k + 1 < ROUNDS:
            greet(known.at[k + 1])

    loads = [
        pltpu.make_async_copy(src, dst, in_sem.at[i])
        for i, (src, dst) in enumerate((
            (grad_hbm.at[:, pl.ds(0, c0)], x0.at[0]),
            (grad_hbm.at[:, pl.ds(c0, cols[1][1])], x1.at[0]),
            (ids_hbm, ids_ref),
            (slots_hbm, slots_ref),
            (tok_hbm, tok),
            (weight_hbm, weight),
            (eo_hbm, eo),
        ))
    ]
    greet(barrier)
    loads[0].start()
    loads[1].start()
    loads[2].start()
    loads[3].start()
    pl.semaphore_wait(barrier, len(BESIDE) + 3)

    def first_copy(g, k):
        step, h = ((1, 0), (-1, 1), (1, 1), (-1, 0))[k]
        rows = pl.ds(h * t_half, t_half)
        return to(
            xs_of[g].at[0, rows], xs_of[g].at[step % SIDE, rows], xs, xr.at[2 * g + k if k < 2 else 4], e=ring1(g, step)
        )

    def onward_copy(g, k):
        step, h = ((1, 0), (-1, 1))[k]
        rows = pl.ds(h * t_half, t_half)
        return to(xs_of[g].at[step % SIDE, rows], xs_of[g].at[2, rows], xs, xr.at[5], e=ring1(g, step))

    def table_copy(g, j):
        return to(
            tb_own[g].at[mod(p1[g] + j)], tb_in.at[g, j], tbs, tbr.at[j // 2 * (3 - j)], e=ring1(g, j)
        )

    for g in range(2):
        loads[g].wait()
        first_copy(g, 0).start()
        first_copy(g, 1).start()
    greet(known.at[0])
    loads[4].start()
    loads[5].start()
    loads[2].wait()
    loads[3].wait()
    row16 = lax.broadcasted_iota(I32, (n, t_rows), 0)
    slot_tbl = jnp.full((n, t_rows), -1, I32)
    eloc_tbl = jnp.full((n, t_rows), -1, I32)
    for k in range(top):
        ids = ids_ref[k : k + 1, :]
        dev = lax.shift_right_logical(ids, 4)
        hit = row16 == dev
        slot_tbl = jnp.where(hit, slots_ref[k : k + 1, :], slot_tbl)
        eloc_tbl = jnp.where(hit, ids - dev * PER_DEV, eloc_tbl)
    slot_own[...] = slot_tbl
    eloc[...] = eloc_tbl
    slot_f = slot_tbl.astype(F32)
    slot_f32[...] = slot_f
    for a1 in range(SIDE):
        by_y = slot_f[a1 * SIDE : (a1 + 1) * SIDE, :]
        by_z = jnp.concatenate([slot_f[a2 * SIDE + a1 : a2 * SIDE + a1 + 1, :] for a2 in range(SIDE)], axis=0)
        for g in range(2):
            rows = by_z + flip[g].astype(F32) * (by_y - by_z)
            tb_own[g][a1] = rows.astype(BF16)
    for g in range(2):
        tbf[g][0] = tb_own[g][p1[g]].astype(F32)
    dsend[...] = jnp.zeros_like(dsend)

    for g in range(2):
        table_copy(g, 1).start()
        table_copy(g, 3).start()
    for g in range(2):
        first_copy(g, 2).start()
        first_copy(g, 3).start()
    loads[6].start()

    loads[4].wait()
    loads[5].wait()
    logits_t = jnp.dot(tok[...], weight[...], preferred_element_type=F32).T
    for d in range(n):
        block = logits_t[d * PER_DEV : (d + 1) * PER_DEV, :]
        hit = row16[:PER_DEV] == eloc_tbl[d : d + 1, :]
        lsend[d : d + 1, :] = jnp.sum(jnp.where(hit, block, 0.0), axis=0, keepdims=True)

    take_round(0)
    for g in range(2):
        table_copy(g, 2).start()

    slot_iota = lax.broadcasted_iota(I32, (ROW, t_rows), 0).astype(F32)

    def own_table(d, carry):
        row = slot_f32[pl.ds(d, 1), :]
        oh[d] = jnp.where(row == slot_iota, 1.0, 0.0).astype(BF16)
        return carry

    lax.fori_loop(0, n, own_table, 0)
    win[mw] = lsend[...]

    take_round(1)

    def logit_copy(o):
        return to(lsend, win.at[mw], ws, wr, w=lax.rem(mw + o, n_width))

    def send_logits(o, carry):
        logit_copy(o).start()
        return carry

    lax.fori_loop(1, n_width, send_logits, 0)

    cap_iota = lax.broadcasted_iota(I32, (cap, t_rows), 0).astype(F32)

    def select(g, j0, step, count):
        def one(i, carry):
            j = j0 + step * i
            picks = []
            for m in range(SIDE):
                row = tbf[g][j, pl.ds(mod(p2[g] + m), 1), :]
                picks.append(jnp.where(row == cap_iota, 1.0, 0.0).astype(BF16))
            rows = jnp.dot(jnp.concatenate(picks, axis=0), xs_of[g][j], preferred_element_type=F32).astype(BF16)
            rs_of[g][place(g, p1[g] - j, p2[g])] = rows[:cap]
            for m in range(1, SIDE):
                rs_of[g][n + j * SIDE + m] = rows[m * cap : (m + 1) * cap]
            return carry

        if count == 1:
            one(0, 0)
        else:
            lax.fori_loop(0, count, one, 0)

    def near_copy(g, j, kind, start, rows):
        step = (1, -1)[kind]
        part = pl.ds(start, rows)
        return to(
            rs_of[g].at[n + j * SIDE + step % SIDE, part], rs_of[g].at[place(g, p1[g] - j, p2[g]), part],
            ss, sr.at[(6 if start == 0 else 0, 1, 2, 1)[j]], e=ring2(g, step),
        )

    def relay_copy(g, j, h):
        return to(
            rs_of[g].at[n + j * SIDE + 2, pl.ds(h * half, half)], rl_of[g].at[j, h],
            ss, rlr.at[j], e=ring2(g, (1, -1)[h]),
        )

    def final_copy(g, j, h):
        step = (1, -1)[h]
        return to(
            rl_of[g].at[j, h], rs_of[g].at[place(g, p1[g] - j, p2[g] - step), pl.ds(h * half, half)],
            ss, sr.at[3 + (0, 1, 2, 1)[j]], e=ring2(g, step),
        )

    def send_far(j):
        for g in range(2):
            relay_copy(g, j, 0).start()
            relay_copy(g, j, 1).start()

    def pass_on(j):
        await_recv(eo.at[0], rlr.at[j])
        for g in range(2):
            final_copy(g, j, 0).start()
            final_copy(g, j, 1).start()

    def send_near(j, start=0, rows=cap):
        for g in range(2):
            near_copy(g, j, 0, start, rows).start()
            near_copy(g, j, 1, start, rows).start()

    def arrived(index, count, rows=cap):
        await_recv(eo.at[pl.ds(0, count), pl.ds(0, rows)], sr.at[index])

    for g in range(2):
        select(g, 0, 0, 1)
    for k in range(2):
        for g in range(2):
            await_recv(xs_of[g].at[0, pl.ds(0, t_half)], xr.at[2 * g + k])
            onward_copy(g, k).start()
    send_far(0)
    send_near(0, 0, cut)

    def take_tables(js):
        await_recv(tb_in.at[:, pl.ds(0, len(js))], tbr.at[len(js) % 2])
        for g in range(2):
            for j in js:
                tbf[g][j] = tb_in[g, j].astype(F32)

    take_tables((1, 3))
    await_recv(tok, xr.at[4])
    for g in range(2):
        select(g, 1, 2, 2)
    send_far(1)
    send_far(3)
    pass_on(0)

    await_recv(win.at[pl.ds(0, n_width - 1)], wr)
    total_logits = win[0]
    for w in range(1, win.shape[0]):
        total_logits = total_logits + win[w]
    picked = jnp.where(eloc_tbl >= 0, jax.nn.sigmoid(total_logits), 0.0)
    picked_v[...] = picked
    gates = (ROUTE_SCALE * picked / jnp.sum(picked, axis=0, keepdims=True)).astype(BF16).astype(F32)

    gates = gates.astype(BF16)
    for first in range(0, n, 4):
        found = [lax.dot_general(gates, oh[d], NT, preferred_element_type=F32) for d in range(first, first + 4)]
        for i, rows in enumerate(found):
            gsend[first + i] = rows[first + i : first + i + 1, :]
    gin[me] = gsend[me]

    take_round(2)

    def gate_copy(o):
        d = lax.rem(me + o, n)
        return to(gsend.at[d], gin.at[me], gs, gr, e=d)

    def send_gates(o, carry):
        gate_copy(o).start()
        return carry

    lax.fori_loop(1, n, send_gates, 0)

    take_tables((2,))
    await_recv(tok, xr.at[5])
    for g in range(2):
        select(g, 2, 0, 1)
    send_far(2)
    pass_on(1)
    pass_on(3)
    send_near(2)

    loads[6].wait()
    await_recv(gin.at[pl.ds(0, n - 1)], gr)

    ones = jnp.ones((8, 256), BF16)
    eye = lax.broadcasted_iota(I32, (cap, cap), 0) == lax.broadcasted_iota(I32, (cap, cap), 1)

    def gate_grads_of(blocks, start=0, stop=cap):
        found = []
        for s in blocks:
            acc = None
            for g in range(2):
                for at in range(0, cols[g][1], 128):
                    a = rs_of[g][s, start:stop, at : at + 128].astype(F32)
                    b = eo[s, start:stop, cols[g][0] + at : cols[g][0] + at + 128].astype(F32)
                    acc = a * b if acc is None else acc + a * b
            high = acc.astype(BF16)
            low = (acc - high.astype(F32)).astype(BF16)
            both = jnp.concatenate([high, low], axis=1)
            found.append(lax.dot_general(ones, both, NT, preferred_element_type=F32)[0:1, :])
        for s, dots in zip(blocks, found):
            dsend[s, :, start:stop] = dots

    def expert_grad_of(s):
        scale = jnp.where(eye, gin[s][:, :cap], 0.0).astype(BF16)
        for g in range(2):
            value = jnp.dot(scale, rs_of[g][s], preferred_element_type=F32)
            egv[s, :, cols[g][0] : cols[g][0] + cols[g][1]] = value.astype(BF16)

    def far_one(i):
        return 2 * i, 2 - 2 * i

    def far_near(i):
        q, r = i // 2, 1 + 2 * lax.rem(i, 2)
        return 2 * q + (1 - q) * r, q * r + 2 * (1 - q)

    def diagonal(i):
        return 1 + 2 * (i // 2), 1 + 2 * lax.rem(i, 2)

    def beside(i):
        q, r = i // 2, 1 + 2 * lax.rem(i, 2)
        return q * r, (1 - q) * r

    def grads_back(offsets, row):
        blocks = [origin(dy, dz) for dy, dz in offsets]
        gate_grads_of(blocks)
        for i, s in enumerate(blocks):
            to(dsend.at[s], rin.at[row + i], rts, rtr, e=s).start()

    def late_copy(s, row, w):
        return to(dsend.at[s], win2.at[mw, row], w2s, w2r.at[1], e=s, w=w)

    def grads_to_widths(offsets, row, start=0):
        blocks = [origin(dy, dz) for dy, dz in offsets]
        gate_grads_of(blocks, start)

        def one(w, carry):
            for i, s in enumerate(blocks):
                late_copy(s, row + i, w).start()
            return carry

        lax.fori_loop(0, n_width, one, 0)

    def scaled(count, offset):
        def one(i, carry):
            expert_grad_of(origin(*offset(i)))
            return carry

        lax.fori_loop(0, count, one, 0)

    rows = pl.ds(0, EARLY)

    def width_copy(o):
        return to(rin, win2.at[mw, rows], w2s, w2r.at[0], w=lax.rem(mw + o, n_width))

    def send_width(o, carry):
        width_copy(o).start()
        return carry

    gate_grads_of([me])
    rin[0] = dsend[me]
    arrived(3, 1)
    grads_back(FAR_ONE, 1)
    pass_on(2)
    send_near(1)
    scaled(1, lambda i: (0, 0))
    scaled(2, far_one)
    arrived(4, 2)
    arrived(2, 2)
    grads_back(FAR_NEAR, 3)
    arrived(5, 1)
    grads_back(FAR_BOTH, 7)
    send_near(3)
    send_near(0, cut, cap - cut)
    take_round(3)
    scaled(4, far_near)
    scaled(1, lambda i: (2, 2))
    arrived(6, 2, cut)
    gate_grads_of([origin(dy, dz) for dy, dz in BESIDE], 0, cut)
    await_recv(dsend.at[pl.ds(0, EARLY - 1)], rtr)
    lax.fori_loop(1, n_width, send_width, 0)
    win2[mw, rows] = rin[...]
    arrived(1, 4)
    grads_to_widths(DIAGONAL, EARLY)
    arrived(0, 2, cap - cut)
    grads_to_widths(BESIDE, EARLY + len(DIAGONAL), cut)
    scaled(4, diagonal)
    scaled(4, beside)

    await_recv(win2.at[pl.ds(0, n_width - 1), pl.ds(0, EARLY)], w2r.at[0])
    await_recv(win2.at[pl.ds(0, n_width), pl.ds(0, LATE)], w2r.at[1])
    for i, (dy, dz) in enumerate(OFFSETS):
        row = win2[0, i]
        for w in range(1, win2.shape[0]):
            row = row + win2[w, i]
        ggv[pl.ds(target(dy, dz), 1), :] = row

    slots = slot_own[...]
    lane = jnp.bitwise_and(slots, 127)
    pieces = []
    for at in range(0, t_rows, 128):
        index = lane[:, at : at + 128]
        low = jnp.take_along_axis(ggv[:, 0:128], index, axis=1)
        high = jnp.take_along_axis(ggv[:, 128:256], index, axis=1)
        pieces.append(jnp.where(slots[:, at : at + 128] < 128, low, high))
    chosen = slots >= 0
    gate_grads = jnp.where(chosen, jnp.concatenate(pieces, axis=1), 0.0)

    picked = picked_v[...]
    totals = jnp.sum(picked, axis=0, keepdims=True)
    weighted = jnp.sum(gate_grads * picked, axis=0, keepdims=True) / totals
    local = jnp.where(chosen, ROUTE_SCALE / totals * (gate_grads - weighted) * picked * (1.0 - picked), 0.0)
    for d in range(n):
        hit = row16[:PER_DEV] == eloc[d : d + 1, :]
        block = jnp.where(hit, local[d : d + 1, :], 0.0)
        lgt32[d * PER_DEV : (d + 1) * PER_DEV, :] = block
        lgt[d * PER_DEV : (d + 1) * PER_DEV, :] = block.astype(BF16)

    part = jnp.dot(lgt[...], tok[...], preferred_element_type=F32)
    rb[...] = part.astype(BF16).reshape(rb.shape)

    def send_terms(offsets):
        for dy, dz in offsets:
            d = target(dy, dz)
            to(rb.at[d], rr.at[TERMS.index((dy, dz))], rps, rpr, e=d).start()

    for k, (step, owner) in enumerate(JOINED):
        to(rb.at[target(*owner)], rm.at[k], rps, rms, e=target(*step)).start()
    send_terms(FAR_BOTH + DIAGONAL + BESIDE)
    rr[0] = rb[me]
    logit_grads = lgt32[...].T.astype(BF16)
    ig_ref[...] = lax.dot_general(logit_grads, weight[...], NT, preferred_element_type=F32).astype(BF16)
    await_recv(rm, rms)
    for k, owner in ((0, (2, 0)), (2, (0, 2))):
        d = target(*owner)
        rb[d] = (rb[d].astype(F32) + rm[k].astype(F32) + rm[k + 1].astype(F32)).astype(BF16)
    send_terms(FAR_ONE)
    await_recv(rr.at[pl.ds(0, len(TERMS) - 1)], rpr)
    total = rr[0].astype(F32)
    for d in range(1, len(TERMS)):
        total = total + rr[d].astype(F32)
    rg_ref[...] = total

    await_sent(eo.at[pl.ds(0, (SIDE - 1) * t_rows // cap)], xs)
    await_sent(tb_in.at[:, pl.ds(0, SIDE - 1)], tbs)
    await_sent(eo, ss)
    await_sent(win.at[pl.ds(0, n_width - 1)], ws)
    await_sent(gin.at[pl.ds(0, n - 1)], gs)
    await_sent(dsend.at[pl.ds(0, EARLY - 1)], rts)
    await_sent(win2.at[pl.ds(0, n_width), pl.ds(0, n - 1)], w2s)
    await_sent(rb.at[pl.ds(0, n - 1)], rps)


def write_out(eg_in, rg_in, ig_in, eg_out, rg_out, ig_out, sem):
    pieces = 1
    step = eg_in.shape[0] // pieces
    pairs = [(eg_in.at[pl.ds(i * step, step)], eg_out.at[pl.ds(i * step, step)]) for i in range(pieces)]
    pairs += [(ig_in, ig_out), (rg_in, rg_out)]
    copies = [pltpu.make_async_copy(src, dst, sem.at[i]) for i, (src, dst) in enumerate(pairs)]
    for copy in copies:
        copy.start()
    for copy in copies:
        copy.wait()


def body(tokens_in, out_grad, router_weight, expert_out, expert_ids, slot_ids):
    n = lax.axis_size("expert")
    n_width = lax.axis_size("width")
    t_rows, d_cols = out_grad.shape
    top = expert_ids.shape[1]
    experts = router_weight.shape[1]
    cap = t_rows * top // n
    c0 = (d_cols // 128 + 1) // 2 * 128
    c1 = d_cols - c0
    hbm, vmem = pl.BlockSpec(memory_space=pltpu.HBM), pl.BlockSpec(memory_space=pltpu.VMEM)
    dma = pltpu.SemaphoreType.DMA
    scratch = [
        pltpu.VMEM((SIDE, t_rows, c0), BF16),
        pltpu.VMEM((SIDE, t_rows, c1), BF16),
        pltpu.VMEM((2 * n, cap, c0), BF16),
        pltpu.VMEM((2 * n, cap, c1), BF16),
        pltpu.VMEM((SIDE, 2, cap // 2, c0), BF16),
        pltpu.VMEM((SIDE, 2, cap // 2, c1), BF16),
        pltpu.VMEM((t_rows, d_cols), BF16),
        pltpu.VMEM((d_cols, experts), BF16),
        pltpu.VMEM((n, cap, d_cols), BF16),
        pltpu.VMEM((top, t_rows), I32),
        pltpu.VMEM((top, t_rows), I32),
        pltpu.VMEM((n, ROW, t_rows), BF16),
        pltpu.VMEM((SIDE, SIDE, t_rows), BF16),
        pltpu.VMEM((SIDE, SIDE, t_rows), BF16),
        pltpu.VMEM((2, SIDE, SIDE, t_rows), BF16),
        pltpu.VMEM((SIDE, SIDE, t_rows), F32),
        pltpu.VMEM((SIDE, SIDE, t_rows), F32),
        pltpu.VMEM((n, t_rows), F32),
        pltpu.VMEM((n, t_rows), I32),
        pltpu.VMEM((n, t_rows), I32),
        pltpu.VMEM((n, t_rows), F32),
        pltpu.VMEM((n_width, n, t_rows), F32),
        pltpu.VMEM((n, 1, ROW), F32),
        pltpu.VMEM((n, 1, ROW), F32),
        pltpu.VMEM((n, 1, ROW), F32),
        pltpu.VMEM((EARLY, 1, ROW), F32),
        pltpu.VMEM((n_width, n, 1, ROW), F32),
        pltpu.VMEM((n, ROW), F32),
        pltpu.VMEM((n, t_rows), F32),
        pltpu.VMEM((experts, t_rows), F32),
        pltpu.VMEM((experts, t_rows), BF16),
        pltpu.VMEM((n, experts // n, d_cols), BF16),
        pltpu.VMEM((len(TERMS), experts // n, d_cols), BF16),
        pltpu.VMEM((len(JOINED), experts // n, d_cols), BF16),
        pltpu.SemaphoreType.REGULAR((ROUNDS,)),
        dma((7,)),
        dma(()), dma((6,)),
        dma(()), dma((2,)),
        dma(()), dma(()),
        dma(()), dma(()),
        dma(()), dma((7,)), dma((SIDE,)),
        dma(()), dma(()),
        dma(()), dma((2,)),
        dma(()), dma(()), dma(()),
    ]
    expert_grad, router_grad, input_grad = pl.pallas_call(
        kernel,
        out_shape=(
            pltpu.VMEM((n, cap, d_cols), BF16),
            pltpu.VMEM((experts // n, d_cols), F32),
            pltpu.VMEM((t_rows, d_cols), BF16),
        ),
        in_specs=[hbm] * 6,
        out_specs=(vmem, vmem, vmem),
        scratch_shapes=scratch,
        compiler_params=pltpu.CompilerParams(
            collective_id=0, has_side_effects=True, vmem_limit_bytes=46 * 1024 * 1024
        ),
    )(*(
        pltpu.with_memory_space_constraint(a, pltpu.HBM)
        for a in (tokens_in, out_grad, router_weight, expert_out.reshape(n, cap, d_cols), expert_ids.T, slot_ids.T)
    ))
    expert_grad, router_grad, input_grad = pl.pallas_call(
        write_out,
        out_shape=(
            jax.ShapeDtypeStruct((n, cap, d_cols), BF16),
            jax.ShapeDtypeStruct((experts // n, d_cols), F32),
            jax.ShapeDtypeStruct((t_rows, d_cols), BF16),
        ),
        in_specs=[vmem, vmem, vmem],
        out_specs=(hbm, hbm, hbm),
        scratch_shapes=[dma((3,))],
        compiler_params=pltpu.CompilerParams(vmem_limit_bytes=2 * 1024 * 1024),
    )(*(pltpu.with_memory_space_constraint(a, pltpu.VMEM) for a in (expert_grad, router_grad, input_grad)))
    return expert_grad.reshape(n * cap, d_cols), router_grad.T, input_grad


def solution(mesh):
    return jax.shard_map(
        body,
        mesh=mesh,
        in_specs=(
            P("expert", "width"),
            P("expert", "width"),
            P("width", None),
            P("expert", "width"),
            P("expert", None),
            P("expert", None),
        ),
        out_specs=(P("expert", "width"), P("width", "expert"), P("expert", "width")),
        check_vma=False,
    )
```

```python
import functools

import jax
import jax.numpy as jnp
from jax import lax
from jax.experimental import pallas as pl
from jax.experimental.pallas import tpu as pltpu
from jax.sharding import PartitionSpec as P

MESH = pl.DeviceIdType.MESH
SIDE = 4
PER_DEV = 16
ROUTE_SCALE = 2.5
ROW = 256
BF16, F32, I32 = jnp.bfloat16, jnp.float32, jnp.int32
NT = (((1,), (1,)), ((), ()))


SELF = ((0, 0),)
FAR_ONE = ((0, 2), (2, 0))
FAR_BOTH = ((2, 2),)
FAR_NEAR = ((1, 2), (3, 2), (2, 1), (2, 3))
DIAGONAL = ((1, 1), (1, 3), (3, 1), (3, 3))
BESIDE = ((0, 1), (0, 3), (1, 0), (3, 0))
OFFSETS = SELF + FAR_ONE + FAR_NEAR + FAR_BOTH + DIAGONAL + BESIDE
LATE_ONES = DIAGONAL + BESIDE
EARLY, LATE = 8, 8
ROUNDS = 4
JOINED = (((0, 1), (2, 1)), ((0, 3), (2, 3)), ((1, 0), (1, 2)), ((3, 0), (3, 2)))
TERMS = SELF + FAR_ONE + FAR_BOTH + DIAGONAL + BESIDE


def kernel(
    tok_hbm, grad_hbm, weight_hbm, eo_hbm, ids_hbm, slots_hbm,
    egv, rg_ref, ig_ref,
    x0, x1, rs0, rs1, rl0, rl1, tok, weight, eo, ids_ref, slots_ref, oh,
    tb_own0, tb_own1, tb_in, tbf0, tbf1, slot_f32, slot_own, eloc, lsend, win, gsend, gin, dsend, rin, win2,
    ggv, picked_v, lgt32, lgt, rb, rr, rm,
    known, in_sem, xs, xr, tbs, tbr, ws, wr, gs, gr, ss, sr, rlr, rts, rtr, w2s, w2r, rps, rpr, rms,
):
    n = lax.axis_size("expert")
    n_width = lax.axis_size("width")
    me = lax.axis_index("expert")
    mw = lax.axis_index("width")
    top, t_rows = ids_ref.shape
    cap = rs0.shape[1]
    t_half = t_rows // 2
    half = cap // 2
    cut = half
    xs_of, rs_of, rl_of = (x0, x1), (rs0, rs1), (rl0, rl1)
    tb_own, tbf = (tb_own0, tb_own1), (tbf0, tbf1)
    c0 = x0.shape[2]
    cols = ((0, c0), (c0, x1.shape[2]))
    core = lax.rem(mw, 2)
    gy, gz = me // SIDE, lax.rem(me, SIDE)

    flip = (core, 1 - core)
    p1 = tuple(gz + f * (gy - gz) for f in flip)
    p2 = tuple(gy + f * (gz - gy) for f in flip)

    def mod(v):
        return lax.rem(v + 2 * SIDE, SIDE)

    def place(g, a1, a2):
        return mod(a1) * (1 + (SIDE - 1) * flip[g]) + mod(a2) * (SIDE - (SIDE - 1) * flip[g])

    def ring1(g, step):
        return place(g, p1[g] + step, p2[g])

    def ring2(g, step):
        return place(g, p1[g], p2[g] + step)

    def target(dy, dz):
        return mod(gy + dy) * SIDE + mod(gz + dz)

    def origin(dy, dz):
        return mod(gy - dy) * SIDE + mod(gz - dz)

    def to(src, dst, send, recv, e=None, w=None):
        where = {"expert": me if e is None else e, "width": mw if w is None else w}
        return pltpu.make_async_remote_copy(
            src_ref=src, dst_ref=dst, send_sem=send, recv_sem=recv, device_id=where, device_id_type=MESH
        )

    def await_recv(like, sem):
        to(like, like, sem, sem).wait_recv()

    def await_sent(like, sem):
        to(like, like, sem, sem).wait_send()

    barrier = pltpu.get_barrier_semaphore()

    x_here = mw // 2
    xs_count = n_width // 2

    def greet(sem):
        for dy, dz in BESIDE:
            pl.semaphore_signal(sem, inc=1, device_id={"expert": target(dy, dz), "width": mw}, device_id_type=MESH)
        for step in (1, xs_count - 1):
            w = lax.rem(x_here + step, xs_count) * 2 + core
            pl.semaphore_signal(sem, inc=1, device_id={"expert": me, "width": w}, device_id_type=MESH)
        pl.semaphore_signal(
            sem, inc=1, device_id={"expert": me, "width": x_here * 2 + 1 - core}, device_id_type=MESH
        )

    def take_round(k):
        pl.semaphore_wait(known.at[k], len(BESIDE) + 3)
        if k + 1 < ROUNDS:
            greet(known.at[k + 1])

    loads = [
        pltpu.make_async_copy(src, dst, in_sem.at[i])
        for i, (src, dst) in enumerate((
            (grad_hbm.at[:, pl.ds(0, c0)], x0.at[0]),
            (grad_hbm.at[:, pl.ds(c0, cols[1][1])], x1.at[0]),
            (ids_hbm, ids_ref),
            (slots_hbm, slots_ref),
            (tok_hbm, tok),
            (weight_hbm, weight),
            (eo_hbm, eo),
        ))
    ]
    greet(barrier)
    loads[0].start()
    loads[1].start()
    loads[2].start()
    loads[3].start()
    pl.semaphore_wait(barrier, len(BESIDE) + 3)

    def first_copy(g, k):
        step, h = ((1, 0), (-1, 1), (1, 1), (-1, 0))[k]
        rows = pl.ds(h * t_half, t_half)
        return to(
            xs_of[g].at[0, rows], xs_of[g].at[step % SIDE, rows], xs, xr.at[2 * g + k if k < 2 else 4], e=ring1(g, step)
        )

    def onward_copy(g, k):
        step, h = ((1, 0), (-1, 1))[k]
        rows = pl.ds(h * t_half, t_half)
        return to(xs_of[g].at[step % SIDE, rows], xs_of[g].at[2, rows], xs, xr.at[5], e=ring1(g, step))

    def table_copy(g, j):
        return to(
            tb_own[g].at[mod(p1[g] + j)], tb_in.at[g, j], tbs, tbr.at[j // 2 * (3 - j)], e=ring1(g, j)
        )

    for g in range(2):
        loads[g].wait()
        first_copy(g, 0).start()
        first_copy(g, 1).start()
    greet(known.at[0])
    loads[4].start()
    loads[5].start()
    loads[2].wait()
    loads[3].wait()
    row16 = lax.broadcasted_iota(I32, (n, t_rows), 0)
    slot_tbl = jnp.full((n, t_rows), -1, I32)
    eloc_tbl = jnp.full((n, t_rows), -1, I32)
    for k in range(top):
        ids = ids_ref[k : k + 1, :]
        dev = lax.shift_right_logical(ids, 4)
        hit = row16 == dev
        slot_tbl = jnp.where(hit, slots_ref[k : k + 1, :], slot_tbl)
        eloc_tbl = jnp.where(hit, ids - dev * PER_DEV, eloc_tbl)
    slot_own[...] = slot_tbl
    eloc[...] = eloc_tbl
    slot_f = slot_tbl.astype(F32)
    slot_f32[...] = slot_f
    for a1 in range(SIDE):
        by_y = slot_f[a1 * SIDE : (a1 + 1) * SIDE, :]
        by_z = jnp.concatenate([slot_f[a2 * SIDE + a1 : a2 * SIDE + a1 + 1, :] for a2 in range(SIDE)], axis=0)
        for g in range(2):
            rows = by_z + flip[g].astype(F32) * (by_y - by_z)
            tb_own[g][a1] = rows.astype(BF16)
    for g in range(2):
        tbf[g][0] = tb_own[g][p1[g]].astype(F32)
    dsend[...] = jnp.zeros_like(dsend)

    for g in range(2):
        table_copy(g, 1).start()
        table_copy(g, 3).start()
    for g in range(2):
        first_copy(g, 2).start()
        first_copy(g, 3).start()
    loads[6].start()

    loads[4].wait()
    loads[5].wait()
    logits_t = jnp.dot(tok[...], weight[...], preferred_element_type=F32).T
    for d in range(n):
        block = logits_t[d * PER_DEV : (d + 1) * PER_DEV, :]
        hit = row16[:PER_DEV] == eloc_tbl[d : d + 1, :]
        lsend[d : d + 1, :] = jnp.sum(jnp.where(hit, block, 0.0), axis=0, keepdims=True)

    take_round(0)
    for g in range(2):
        table_copy(g, 2).start()

    slot_iota = lax.broadcasted_iota(I32, (ROW, t_rows), 0).astype(F32)

    def own_table(d, carry):
        row = slot_f32[pl.ds(d, 1), :]
        oh[d] = jnp.where(row == slot_iota, 1.0, 0.0).astype(BF16)
        return carry

    lax.fori_loop(0, n, own_table, 0)
    win[mw] = lsend[...]

    take_round(1)

    def logit_copy(o):
        return to(lsend, win.at[mw], ws, wr, w=lax.rem(mw + o, n_width))

    def send_logits(o, carry):
        logit_copy(o).start()
        return carry

    lax.fori_loop(1, n_width, send_logits, 0)

    cap_iota = lax.broadcasted_iota(I32, (cap, t_rows), 0).astype(F32)

    def select(g, j0, step, count):
        def one(i, carry):
            j = j0 + step * i
            picks = []
            for m in range(SIDE):
                row = tbf[g][j, pl.ds(mod(p2[g] + m), 1), :]
                picks.append(jnp.where(row == cap_iota, 1.0, 0.0).astype(BF16))
            rows = jnp.dot(jnp.concatenate(picks, axis=0), xs_of[g][j], preferred_element_type=F32).astype(BF16)
            rs_of[g][place(g, p1[g] - j, p2[g])] = rows[:cap]
            for m in range(1, SIDE):
                rs_of[g][n + j * SIDE + m] = rows[m * cap : (m + 1) * cap]
            return carry

        if count == 1:
            one(0, 0)
        else:
            lax.fori_loop(0, count, one, 0)

    def near_copy(g, j, kind, start, rows):
        step = (1, -1)[kind]
        part = pl.ds(start, rows)
        return to(
            rs_of[g].at[n + j * SIDE + step % SIDE, part], rs_of[g].at[place(g, p1[g] - j, p2[g]), part],
            ss, sr.at[(6 if start == 0 else 0, 7, 2, 1)[j]], e=ring2(g, step),
        )

    def relay_copy(g, j, h):
        return to(
            rs_of[g].at[n + j * SIDE + 2, pl.ds(h * half, half)], rl_of[g].at[j, h],
            ss, rlr.at[j], e=ring2(g, (1, -1)[h]),
        )

    def final_copy(g, j, h):
        step = (1, -1)[h]
        return to(
            rl_of[g].at[j, h], rs_of[g].at[place(g, p1[g] - j, p2[g] - step), pl.ds(h * half, half)],
            ss, sr.at[3 + (0, 1, 2, 1)[j]], e=ring2(g, step),
        )

    def send_far(j):
        for g in range(2):
            relay_copy(g, j, 0).start()
            relay_copy(g, j, 1).start()

    def pass_on(j):
        await_recv(eo.at[0], rlr.at[j])
        for g in range(2):
            final_copy(g, j, 0).start()
            final_copy(g, j, 1).start()

    def send_near(j, start=0, rows=cap):
        for g in range(2):
            near_copy(g, j, 0, start, rows).start()
            near_copy(g, j, 1, start, rows).start()

    def arrived(index, count, rows=cap):
        await_recv(eo.at[pl.ds(0, count), pl.ds(0, rows)], sr.at[index])

    for g in range(2):
        select(g, 0, 0, 1)
    for k in range(2):
        for g in range(2):
            await_recv(xs_of[g].at[0, pl.ds(0, t_half)], xr.at[2 * g + k])
            onward_copy(g, k).start()
    send_far(0)
    send_near(0, 0, cut)

    def take_tables(js):
        await_recv(tb_in.at[:, pl.ds(0, len(js))], tbr.at[len(js) % 2])
        for g in range(2):
            for j in js:
                tbf[g][j] = tb_in[g, j].astype(F32)

    take_tables((1, 3))
    await_recv(tok, xr.at[4])
    for g in range(2):
        select(g, 1, 2, 2)
    send_far(1)
    send_far(3)
    pass_on(0)

    await_recv(win.at[pl.ds(0, n_width - 1)], wr)
    total_logits = win[0]
    for w in range(1, win.shape[0]):
        total_logits = total_logits + win[w]
    picked = jnp.where(eloc_tbl >= 0, jax.nn.sigmoid(total_logits), 0.0)
    picked_v[...] = picked
    gates = (ROUTE_SCALE * picked / jnp.sum(picked, axis=0, keepdims=True)).astype(BF16).astype(F32)

    gates = gates.astype(BF16)
    for first in range(0, n, 4):
        found = [lax.dot_general(gates, oh[d], NT, preferred_element_type=F32) for d in range(first, first + 4)]
        for i, rows in enumerate(found):
            gsend[first + i] = rows[first + i : first + i + 1, :]
    gin[me] = gsend[me]

    take_round(2)

    def gate_copy(o):
        d = lax.rem(me + o, n)
        return to(gsend.at[d], gin.at[me], gs, gr, e=d)

    def send_gates(o, carry):
        gate_copy(o).start()
        return carry

    lax.fori_loop(1, n, send_gates, 0)

    take_tables((2,))
    await_recv(tok, xr.at[5])
    for g in range(2):
        select(g, 2, 0, 1)
    send_far(2)
    pass_on(1)
    pass_on(3)
    send_near(2)

    loads[6].wait()
    await_recv(gin.at[pl.ds(0, n - 1)], gr)

    ones = jnp.ones((8, 256), BF16)
    eye = lax.broadcasted_iota(I32, (cap, cap), 0) == lax.broadcasted_iota(I32, (cap, cap), 1)

    def gate_grads_of(blocks, start=0, stop=cap):
        found = []
        for s in blocks:
            acc = None
            for g in range(2):
                for at in range(0, cols[g][1], 128):
                    a = rs_of[g][s, start:stop, at : at + 128].astype(F32)
                    b = eo[s, start:stop, cols[g][0] + at : cols[g][0] + at + 128].astype(F32)
                    acc = a * b if acc is None else acc + a * b
            high = acc.astype(BF16)
            low = (acc - high.astype(F32)).astype(BF16)
            both = jnp.concatenate([high, low], axis=1)
            found.append(lax.dot_general(ones, both, NT, preferred_element_type=F32)[0:1, :])
        for s, dots in zip(blocks, found):
            dsend[s, :, start:stop] = dots

    def expert_grad_of(s):
        scale = jnp.where(eye, gin[s][:, :cap], 0.0).astype(BF16)
        for g in range(2):
            value = jnp.dot(scale, rs_of[g][s], preferred_element_type=F32)
            egv[s, :, cols[g][0] : cols[g][0] + cols[g][1]] = value.astype(BF16)

    def far_one(i):
        return 2 * i, 2 - 2 * i

    def far_near(i):
        q, r = i // 2, 1 + 2 * lax.rem(i, 2)
        return 2 * q + (1 - q) * r, q * r + 2 * (1 - q)

    def diagonal(i):
        return 1 + 2 * (i // 2), 1 + 2 * lax.rem(i, 2)

    def beside(i):
        q, r = i // 2, 1 + 2 * lax.rem(i, 2)
        return q * r, (1 - q) * r

    def grads_back(offsets, row):
        blocks = [origin(dy, dz) for dy, dz in offsets]
        gate_grads_of(blocks)
        for i, s in enumerate(blocks):
            to(dsend.at[s], rin.at[row + i], rts, rtr, e=s).start()

    def late_copy(s, row, w):
        return to(dsend.at[s], win2.at[mw, row], w2s, w2r.at[1], e=s, w=w)

    def grads_to_widths(offsets, row, start=0):
        blocks = [origin(dy, dz) for dy, dz in offsets]
        gate_grads_of(blocks, start)

        for o in sorted(range(n_width), key=lambda o: -min(o, n_width - o)):
            for i, s in enumerate(blocks):
                late_copy(s, row + i, lax.rem(mw + o, n_width)).start()

    def scaled(count, offset):
        def one(i, carry):
            expert_grad_of(origin(*offset(i)))
            return carry

        lax.fori_loop(0, count, one, 0)

    rows = pl.ds(0, EARLY)

    def width_copy(o):
        return to(rin, win2.at[mw, rows], w2s, w2r.at[0], w=lax.rem(mw + o, n_width))

    def send_width(o, carry):
        width_copy(o).start()
        return carry

    gate_grads_of([me])
    rin[0] = dsend[me]
    arrived(3, 1)
    grads_back(FAR_ONE, 1)
    pass_on(2)
    send_near(1)
    scaled(1, lambda i: (0, 0))
    scaled(2, far_one)
    arrived(4, 2)
    arrived(2, 2)
    grads_back(FAR_NEAR, 3)
    arrived(5, 1)
    grads_back(FAR_BOTH, 7)
    send_near(3)
    send_near(0, cut, cap - cut)
    take_round(3)
    scaled(4, far_near)
    scaled(1, lambda i: (2, 2))
    arrived(6, 2, cut)
    gate_grads_of([origin(dy, dz) for dy, dz in BESIDE], 0, cut)
    arrived(7, 2)
    grads_to_widths(DIAGONAL[:1], EARLY)
    await_recv(dsend.at[pl.ds(0, EARLY - 1)], rtr)
    lax.fori_loop(1, n_width, send_width, 0)
    win2[mw, rows] = rin[...]
    arrived(1, 2)
    grads_to_widths(DIAGONAL[1:], EARLY + 1)
    arrived(0, 2, cap - cut)
    grads_to_widths(BESIDE, EARLY + len(DIAGONAL), cut)
    scaled(4, diagonal)
    scaled(4, beside)

    await_recv(win2.at[pl.ds(0, n_width - 1), pl.ds(0, EARLY)], w2r.at[0])
    await_recv(win2.at[pl.ds(0, n_width), pl.ds(0, LATE)], w2r.at[1])
    for i, (dy, dz) in enumerate(OFFSETS):
        row = win2[0, i]
        for w in range(1, win2.shape[0]):
            row = row + win2[w, i]
        ggv[pl.ds(target(dy, dz), 1), :] = row

    slots = slot_own[...]
    lane = jnp.bitwise_and(slots, 127)
    pieces = []
    for at in range(0, t_rows, 128):
        index = lane[:, at : at + 128]
        low = jnp.take_along_axis(ggv[:, 0:128], index, axis=1)
        high = jnp.take_along_axis(ggv[:, 128:256], index, axis=1)
        pieces.append(jnp.where(slots[:, at : at + 128] < 128, low, high))
    chosen = slots >= 0
    gate_grads = jnp.where(chosen, jnp.concatenate(pieces, axis=1), 0.0)

    picked = picked_v[...]
    totals = jnp.sum(picked, axis=0, keepdims=True)
    weighted = jnp.sum(gate_grads * picked, axis=0, keepdims=True) / totals
    local = jnp.where(chosen, ROUTE_SCALE / totals * (gate_grads - weighted) * picked * (1.0 - picked), 0.0)
    for d in range(n):
        hit = row16[:PER_DEV] == eloc[d : d + 1, :]
        block = jnp.where(hit, local[d : d + 1, :], 0.0)
        lgt32[d * PER_DEV : (d + 1) * PER_DEV, :] = block
        lgt[d * PER_DEV : (d + 1) * PER_DEV, :] = block.astype(BF16)

    part = jnp.dot(lgt[...], tok[...], preferred_element_type=F32)
    rb[...] = part.astype(BF16).reshape(rb.shape)

    def send_terms(offsets):
        for dy, dz in offsets:
            d = target(dy, dz)
            to(rb.at[d], rr.at[TERMS.index((dy, dz))], rps, rpr, e=d).start()

    for k, (step, owner) in enumerate(JOINED):
        to(rb.at[target(*owner)], rm.at[k], rps, rms, e=target(*step)).start()
    send_terms(FAR_BOTH + DIAGONAL + BESIDE)
    rr[0] = rb[me]
    logit_grads = lgt32[...].T.astype(BF16)
    ig_ref[...] = lax.dot_general(logit_grads, weight[...], NT, preferred_element_type=F32).astype(BF16)
    await_recv(rm, rms)
    for k, owner in ((0, (2, 0)), (2, (0, 2))):
        d = target(*owner)
        rb[d] = (rb[d].astype(F32) + rm[k].astype(F32) + rm[k + 1].astype(F32)).astype(BF16)
    send_terms(FAR_ONE)
    await_recv(rr.at[pl.ds(0, len(TERMS) - 1)], rpr)
    total = rr[0].astype(F32)
    for d in range(1, len(TERMS)):
        total = total + rr[d].astype(F32)
    rg_ref[...] = total

    await_sent(eo.at[pl.ds(0, (SIDE - 1) * t_rows // cap)], xs)
    await_sent(tb_in.at[:, pl.ds(0, SIDE - 1)], tbs)
    await_sent(eo, ss)
    await_sent(win.at[pl.ds(0, n_width - 1)], ws)
    await_sent(gin.at[pl.ds(0, n - 1)], gs)
    await_sent(dsend.at[pl.ds(0, EARLY - 1)], rts)
    await_sent(win2.at[pl.ds(0, n_width), pl.ds(0, n - 1)], w2s)
    await_sent(rb.at[pl.ds(0, n - 1)], rps)


def write_out(eg_in, rg_in, ig_in, eg_out, rg_out, ig_out, sem):
    pieces = 1
    step = eg_in.shape[0] // pieces
    pairs = [(eg_in.at[pl.ds(i * step, step)], eg_out.at[pl.ds(i * step, step)]) for i in range(pieces)]
    pairs += [(ig_in, ig_out), (rg_in, rg_out)]
    copies = [pltpu.make_async_copy(src, dst, sem.at[i]) for i, (src, dst) in enumerate(pairs)]
    for copy in copies:
        copy.start()
    for copy in copies:
        copy.wait()


def body(tokens_in, out_grad, router_weight, expert_out, expert_ids, slot_ids):
    n = lax.axis_size("expert")
    n_width = lax.axis_size("width")
    t_rows, d_cols = out_grad.shape
    top = expert_ids.shape[1]
    experts = router_weight.shape[1]
    cap = t_rows * top // n
    c0 = (d_cols // 128 + 1) // 2 * 128
    c1 = d_cols - c0
    hbm, vmem = pl.BlockSpec(memory_space=pltpu.HBM), pl.BlockSpec(memory_space=pltpu.VMEM)
    dma = pltpu.SemaphoreType.DMA
    scratch = [
        pltpu.VMEM((SIDE, t_rows, c0), BF16),
        pltpu.VMEM((SIDE, t_rows, c1), BF16),
        pltpu.VMEM((2 * n, cap, c0), BF16),
        pltpu.VMEM((2 * n, cap, c1), BF16),
        pltpu.VMEM((SIDE, 2, cap // 2, c0), BF16),
        pltpu.VMEM((SIDE, 2, cap // 2, c1), BF16),
        pltpu.VMEM((t_rows, d_cols), BF16),
        pltpu.VMEM((d_cols, experts), BF16),
        pltpu.VMEM((n, cap, d_cols), BF16),
        pltpu.VMEM((top, t_rows), I32),
        pltpu.VMEM((top, t_rows), I32),
        pltpu.VMEM((n, ROW, t_rows), BF16),
        pltpu.VMEM((SIDE, SIDE, t_rows), BF16),
        pltpu.VMEM((SIDE, SIDE, t_rows), BF16),
        pltpu.VMEM((2, SIDE, SIDE, t_rows), BF16),
        pltpu.VMEM((SIDE, SIDE, t_rows), F32),
        pltpu.VMEM((SIDE, SIDE, t_rows), F32),
        pltpu.VMEM((n, t_rows), F32),
        pltpu.VMEM((n, t_rows), I32),
        pltpu.VMEM((n, t_rows), I32),
        pltpu.VMEM((n, t_rows), F32),
        pltpu.VMEM((n_width, n, t_rows), F32),
        pltpu.VMEM((n, 1, ROW), F32),
        pltpu.VMEM((n, 1, ROW), F32),
        pltpu.VMEM((n, 1, ROW), F32),
        pltpu.VMEM((EARLY, 1, ROW), F32),
        pltpu.VMEM((n_width, n, 1, ROW), F32),
        pltpu.VMEM((n, ROW), F32),
        pltpu.VMEM((n, t_rows), F32),
        pltpu.VMEM((experts, t_rows), F32),
        pltpu.VMEM((experts, t_rows), BF16),
        pltpu.VMEM((n, experts // n, d_cols), BF16),
        pltpu.VMEM((len(TERMS), experts // n, d_cols), BF16),
        pltpu.VMEM((len(JOINED), experts // n, d_cols), BF16),
        pltpu.SemaphoreType.REGULAR((ROUNDS,)),
        dma((7,)),
        dma(()), dma((6,)),
        dma(()), dma((2,)),
        dma(()), dma(()),
        dma(()), dma(()),
        dma(()), dma((8,)), dma((SIDE,)),
        dma(()), dma(()),
        dma(()), dma((2,)),
        dma(()), dma(()), dma(()),
    ]
    expert_grad, router_grad, input_grad = pl.pallas_call(
        kernel,
        out_shape=(
            pltpu.VMEM((n, cap, d_cols), BF16),
            pltpu.VMEM((experts // n, d_cols), F32),
            pltpu.VMEM((t_rows, d_cols), BF16),
        ),
        in_specs=[hbm] * 6,
        out_specs=(vmem, vmem, vmem),
        scratch_shapes=scratch,
        compiler_params=pltpu.CompilerParams(
            collective_id=0, has_side_effects=True, vmem_limit_bytes=46 * 1024 * 1024
        ),
    )(*(
        pltpu.with_memory_space_constraint(a, pltpu.HBM)
        for a in (tokens_in, out_grad, router_weight, expert_out.reshape(n, cap, d_cols), expert_ids.T, slot_ids.T)
    ))
    expert_grad, router_grad, input_grad = pl.pallas_call(
        write_out,
        out_shape=(
            jax.ShapeDtypeStruct((n, cap, d_cols), BF16),
            jax.ShapeDtypeStruct((experts // n, d_cols), F32),
            jax.ShapeDtypeStruct((t_rows, d_cols), BF16),
        ),
        in_specs=[vmem, vmem, vmem],
        out_specs=(hbm, hbm, hbm),
        scratch_shapes=[dma((3,))],
        compiler_params=pltpu.CompilerParams(vmem_limit_bytes=2 * 1024 * 1024),
    )(*(pltpu.with_memory_space_constraint(a, pltpu.VMEM) for a in (expert_grad, router_grad, input_grad)))
    return expert_grad.reshape(n * cap, d_cols), router_grad.T, input_grad


def solution(mesh):
    return jax.shard_map(
        body,
        mesh=mesh,
        in_specs=(
            P("expert", "width"),
            P("expert", "width"),
            P("width", None),
            P("expert", "width"),
            P("expert", None),
            P("expert", None),
        ),
        out_specs=(P("expert", "width"), P("width", "expert"), P("expert", "width")),
        check_vma=False,
    )
```
